32 devices in a mesh: samp: 16 (over z, y, core), snp: 2 (over x).
Axes of the slice: x: 2, y: 2, z: 4, core: 2. Of those that a mesh axis runs over, the one named last changes fastest.
Arguments:
- genotypes: float32 [8192, 2048], P('samp', 'snp'), may hold values from 0 to 2, as said below
- observed: int32 [8192, 2048], P('samp', 'snp'), may hold values from 0 to 1
Outputs:
- relation: float32 [16, 2, 256, 8192], P(None, 'snp', None, 'samp')
The draws below stay inside these ranges and needn't reach their ends.
Inputs may be any that keep to these rules, and one draw needn't show every extreme that they name: `genotypes`: dosages are real numbers between 0 and 2.
All inputs are finite; a program needn't handle non-finite values.
Results may differ from the reference program's by a relative error of at most 0.00061.
Values may be sent and summed in bfloat16 or wider, within the bound.
A program may use at most 128 MiB of HBM per device.

```python
import jax
import jax.numpy as jnp
from jax import lax

SAMPLES = 8192
SNPS = 2048
TILE = 256
N_SAMP = 16
N_SNP = 2


def soft_allele(key, threshold, error_top):
    hard_key = jax.random.fold_in(key, 1)
    error_key = jax.random.fold_in(key, 2)
    carried = jax.random.uniform(hard_key, threshold.shape, jnp.float32) < threshold
    error = jax.random.uniform(error_key, threshold.shape, jnp.float32) * error_top
    return jnp.where(carried, 1.0 - error, error)


def draw_genotypes(key, part):
    rate_key = jax.random.fold_in(key, 11)
    first_key = jax.random.fold_in(key, 12)
    second_key = jax.random.fold_in(key, 13)
    base_rate = jax.random.uniform(rate_key, (SNPS,), jnp.float32, 0.005, 0.331)
    position = (jnp.arange(SAMPLES, dtype=jnp.float32) / SAMPLES)[:, None]
    threshold = base_rate[None, :] * (1.0 + 2.0 * position)
    first_allele = soft_allele(first_key, threshold, 0.3)
    second_allele = soft_allele(second_key, threshold, 0.3)
    return jnp.clip(first_allele + second_allele, 0.0, 2.0).astype(jnp.float32)


def draw_observed(key, part):
    shift_key = jax.random.fold_in(key, 21)
    call_key = jax.random.fold_in(key, 22)
    snp_shift = jax.random.randint(shift_key, (SNPS,), 0, 40)
    sample_index = jnp.arange(SAMPLES, dtype=jnp.int32)
    threshold = 500 + 480 * sample_index[:, None] // SAMPLES - snp_shift[None, :]
    call_draw = jax.random.randint(call_key, (SAMPLES, SNPS), 0, 1000)
    return (call_draw < threshold).astype(jnp.int32)


def setup_inputs(seed: int = 0) -> dict:
    key_of = jax.random.split(jax.random.key(seed), 3)
    return {
        "genotypes": draw_genotypes(jax.random.fold_in(key_of[2], 71), 0),
        "observed": draw_observed(jax.random.fold_in(key_of[2], 71), 0),
    }


var_floor = 0.1

def reference(genotypes, observed):
    present = observed.astype(jnp.float32)
    dosage = genotypes.astype(jnp.float32)
    alt_sum = lax.optimization_barrier(jnp.sum(present * dosage, axis=0))
    call_sum = lax.optimization_barrier(jnp.sum(present, axis=0))
    frequency = alt_sum / (2.0 * jnp.maximum(call_sum, 1.0))
    variance = jnp.maximum(2.0 * frequency * (1.0 - frequency), var_floor)
    scaled = (present * (dosage - 2.0 * frequency) * lax.rsqrt(variance)).astype(jnp.bfloat16)
    widened = scaled.astype(jnp.float32)
    grm = jnp.dot(widened, widened.T, precision=lax.Precision.HIGHEST) / SNPS
    return grm.reshape(N_SAMP, N_SNP, TILE, SAMPLES)
```

```python
import functools
import math

import jax
import jax.numpy as jnp
from jax import lax
from jax.experimental import pallas as pl
from jax.experimental.pallas import tpu as pltpu
from jax.sharding import PartitionSpec as P

MESH = pl.DeviceIdType.MESH
var_floor = 0.1
UP, DOWN, SIDE, CORE = 0, 1, 2, 3
STRIP = 64
PIECES = 2
LOADS = 4
VMEM_ALL = 67043328
VMEM_SPARE = 512 * 1024
VMEM_FINISH = 12 * 1024 * 1024
FOLDED_SPARE = 1024 * 1024
FOLDED_FINISH = 8 * 1024 * 1024
CODE_TOP = 32767.0
TINY = 1e-30


def index(at_z, at_y, at_core):
    return at_z * 4 + at_y * 2 + at_core


def source_at(z, depth, i):
    pairs = jnp.minimum(z, depth - 1 - z)
    side = jnp.where(i % 2 == 1, z - (i + 1) // 2, z + i // 2)
    far = jnp.where(z < depth - 1 - z, z + i - pairs, z - i + pairs)
    return jnp.where(i <= 2 * pairs, side, far)


def turned_at(z, depth):
    return jnp.where(z < depth - 1, z + 1, depth - 2)


def product(rows, panel, q, parts):
    pieces, piece_rows, snp_count = rows.shape[2:]
    total = None
    for h in parts:
        block = rows[q, h].reshape(pieces * piece_rows, snp_count)
        term = lax.dot_general(block, panel[h], (((1,), (1,)), ((), ())), preferred_element_type=jnp.float32)
        total = term if total is None else total + term
    return total * (1.0 / (rows.shape[1] * snp_count))


def finish(shards, groups, rows, panel, tiles, out_ref, late, out_sem):
    depth = shards // 4
    me = lax.axis_index("samp")
    z, y = me // 4, (me // 2) % 2
    turned = turned_at(z, depth)
    final = source_at(z, depth, depth - 1)
    final = jnp.where(final == turned, source_at(z, depth, depth - 2), final)
    last_part = lax.rem(lax.axis_index("snp") + groups - 1, groups)

    def is_late(q):
        return ((q // 4 == turned) | (q // 4 == final)) & ((q // 2) % 2 != y)

    def put(q, carry):
        @pl.when(jnp.logical_not(is_late(q)))
        def _():
            pltpu.make_async_copy(tiles.at[q], out_ref.at[q, 0], out_sem.at[q]).start()

        return carry

    lax.fori_loop(0, shards, put, 0)

    def form(i, carry):
        q = index(jnp.where(i // 2 == 0, final, turned), 1 - y, lax.rem(i, 2))
        late[i] = tiles[q] + product(rows, panel, q, [last_part])
        pltpu.make_async_copy(late.at[i], out_ref.at[q, 0], out_sem.at[q]).start()
        return carry

    lax.fori_loop(0, 4, form, 0)

    def flush(q, carry):
        pltpu.make_async_copy(tiles.at[q], out_ref.at[q, 0], out_sem.at[q]).wait()
        return carry

    lax.fori_loop(0, shards, flush, 0)


def kernel(shards, groups, geno_hbm, obs_hbm, panel, rows, tiles, geno_ref, obs_ref, counts, load_sem,
           count_send, count_recv, panel_send, panel_recv, row_send, row_recv):
    row_count, snp_count = geno_ref.shape
    tile_rows = row_count // groups
    piece_rows = tile_rows // PIECES
    depth = shards // 4
    me = lax.axis_index("samp")
    part = lax.axis_index("snp")
    z, y, core = me // 4, (me // 2) % 2, me % 2

    load_rows = row_count // LOADS

    def load(i):
        block = pl.ds(pl.multiple_of(i * load_rows, load_rows), load_rows)
        return (pltpu.make_async_copy(geno_hbm.at[block], geno_ref.at[block], load_sem.at[0, i]),
                pltpu.make_async_copy(obs_hbm.at[block], obs_ref.at[block], load_sem.at[1, i]))

    for i in range(LOADS):
        for copy in load(i):
            copy.start()

    barrier = pltpu.get_barrier_semaphore()
    for step in range(1, shards):
        pl.semaphore_signal(barrier, inc=1, device_id={"samp": lax.rem(me + step, shards)}, device_id_type=MESH)
    for step in range(1, groups):
        pl.semaphore_signal(barrier, inc=1, device_id={"snp": lax.rem(part + step, groups)}, device_id_type=MESH)

    def add_strip(i, total):
        alt, call = total
        strip = pl.ds(pl.multiple_of(i * STRIP, STRIP), STRIP)
        present = obs_ref[strip, :].astype(jnp.float32)
        held = present * geno_ref[strip, :]
        for r in range(0, STRIP, 8):
            alt = alt + held[r:r + 8]
            call = call + present[r:r + 8]
        return alt, call

    zero = jnp.zeros((8, snp_count), jnp.float32)
    alt, call = zero, zero
    strips = load_rows // STRIP
    for i in range(LOADS):
        for copy in load(i):
            copy.wait()
        alt, call = lax.fori_loop(i * strips, (i + 1) * strips, add_strip, (alt, call))
    counts[me, 0:1, :] = jnp.sum(alt, axis=0, keepdims=True)
    counts[me, 1:2, :] = jnp.sum(call, axis=0, keepdims=True)

    pl.semaphore_wait(barrier, shards + groups - 2)

    def count_copy(owner, to):
        return pltpu.make_async_remote_copy(
            src_ref=counts.at[owner], dst_ref=counts.at[owner], send_sem=count_send.at[to],
            recv_sem=count_recv.at[owner], device_id={"samp": to}, device_id_type=MESH)

    for step in range(1, shards):
        count_copy(me, lax.rem(me + step, shards)).start()
    for step in range(1, shards):
        other = lax.rem(me + step, shards)
        count_copy(other, other).wait_recv()
    sums = counts[0]
    for s in range(1, shards):
        sums = sums + counts[s]
    frequency = sums[0:1] / (2.0 * jnp.maximum(sums[1:2], 1.0))
    shift = 2.0 * frequency
    gain = lax.rsqrt(jnp.maximum(shift * (1.0 - frequency), var_floor))

    def piece_of(k, p):
        return pl.ds(pl.multiple_of(k * tile_rows + p * piece_rows, piece_rows), piece_rows)

    def panel_copy(h, k, to, p):
        block = panel.at[h, piece_of(k, p)]
        return pltpu.make_async_remote_copy(
            src_ref=block, dst_ref=block, send_sem=panel_send.at[to, k, p],
            recv_sem=panel_recv.at[h, k, p], device_id={"snp": to}, device_id_type=MESH)

    strip_rows = min(STRIP, piece_rows)

    def scale_piece(k, p):
        def scale_strip(i, carry):
            start = pl.multiple_of(k * tile_rows + p * piece_rows + i * strip_rows, strip_rows)
            strip = pl.ds(start, strip_rows)
            present = obs_ref[strip, :].astype(jnp.float32)
            panel[part, strip, :] = (present * (geno_ref[strip, :] - shift) * gain).astype(jnp.bfloat16)
            return carry

        lax.fori_loop(0, piece_rows // strip_rows, scale_strip, 0)

    def row_copy(q, h, p, way, src=None):
        to = (index(z + 1, y, core), index(z - 1, y, core), index(z, 1 - y, core), index(z, y, 1 - core))[way]
        return pltpu.make_async_remote_copy(
            src_ref=rows.at[q, h, p] if src is None else src, dst_ref=rows.at[q, h, p],
            send_sem=row_send.at[way, q, h, p], recv_sem=row_recv.at[q, h, p],
            device_id={"samp": to}, device_id_type=MESH)

    def arrive(q, h, p):
        row_copy(q, h, p, CORE).wait_recv()

    last_part = lax.rem(part + groups - 1, groups)
    turned = turned_at(z, depth)

    def part_at(i):
        return lax.rem(part + i, groups)

    def send_own(h, p):
        mine = panel.at[h, piece_of(part, p)]
        row_copy(me, h, p, SIDE, mine).start()

        @pl.when(z < depth - 1)
        def _():
            row_copy(me, h, p, UP, mine).start()

        @pl.when(z > 0)
        def _():
            row_copy(me, h, p, DOWN, mine).start()

        row_copy(me, h, p, CORE, mine).start()
        rows[me, h, p] = panel[h, piece_of(part, p), :]

    for p in range(PIECES):
        for step in range(1, groups):
            other = part_at(step)
            scale_piece(other, p)
            panel_copy(part, other, other, p).start()
        scale_piece(part, p)
        send_own(part, p)
    for step in range(1, groups):
        other = part_at(step)
        for k in range(1, groups):
            for p in range(PIECES):
                panel_copy(part, lax.rem(other + k, groups), other, p).start()
    for step in range(1, groups):
        h = part_at(step)
        for p in range(PIECES):
            panel_copy(h, part, h, p).wait_recv()
            send_own(h, p)

    def column_arrival(at_z, h, p, way):
        q = index(at_z, y, core)
        arrive(q, h, p)

        @pl.when(z < depth - 1 if way == UP else z > 0)
        def _():
            row_copy(q, h, p, way).start()

        @pl.when((at_z != turned) | (h != last_part))
        def _():
            row_copy(q, h, p, SIDE).start()

        row_copy(q, h, p, CORE).start()

    def column_arrivals(i):
        def per_piece(t, carry):
            h, p = part_at(t // PIECES), lax.rem(t, PIECES)

            @pl.when(z - i >= 0)
            def _():
                column_arrival(z - i, h, p, UP)

            @pl.when(z + i < depth)
            def _():
                column_arrival(z + i, h, p, DOWN)

            return carry

        lax.fori_loop(0, groups * PIECES, per_piece, 0)

    def arrive_all(q):
        def per_piece(t, carry):
            arrive(q, t // PIECES, lax.rem(t, PIECES))
            return carry

        lax.fori_loop(0, groups * PIECES, per_piece, 0)

    def products(at_z, at_y):
        def per_core(t, carry):
            q = index(at_z, at_y, lax.rem(core + t, 2))

            @pl.when(t == 1)
            def _():
                arrive_all(q)

            tiles[q] = product(rows, panel, q, range(groups))
            return carry

        lax.fori_loop(0, 2, per_core, 0)

    def side_arrival(at_z, h, p):
        q = index(at_z, 1 - y, core)
        arrive(q, h, p)
        row_copy(q, h, p, CORE).start()

    final = source_at(z, depth, depth - 1)
    final = jnp.where(final == turned, source_at(z, depth, depth - 2), final)

    def begin_late():
        def per_tile(t, carry):
            q = index(jnp.where(t % 2 == 0, turned, final), 1 - y, lax.rem(core + t // 2, 2))

            @pl.when(t >= 2)
            def _():
                for step in range(groups - 1):
                    for p in range(PIECES):
                        arrive(q, part_at(step), p)

            tiles[q] = product(rows, panel, q, [part_at(step) for step in range(groups - 1)])
            return carry

        lax.fori_loop(0, 4, per_tile, 0)

    def round_of(i, carry):
        @pl.when(i < depth)
        def _():
            column_arrivals(i)

        @pl.when(i == 1)
        def _():
            for step in range(1, groups):
                h = part_at(step)
                for k in range(1, groups):
                    for p in range(PIECES):
                        panel_copy(h, part_at(k), h, p).wait_recv()

        @pl.when(i == depth - 1)
        def _():
            q = index(z, 1 - y, core)

            @pl.when(z > 0)
            def _():
                for p in range(PIECES):
                    row_copy(q, last_part, p, DOWN).start()

            @pl.when(z == depth - 2)
            def _():
                for p in range(PIECES):
                    row_copy(q, last_part, p, UP).start()

        at_z = source_at(z, depth, i - 1)
        products(at_z, y)

        def per_piece(t, c):
            @pl.when((i == depth) & (t == (groups - 1) * PIECES))
            def _():
                begin_late()

            @pl.when((at_z != turned) | (t // PIECES != groups - 1))
            def _():
                side_arrival(at_z, part_at(t // PIECES), lax.rem(t, PIECES))

            return c

        lax.fori_loop(0, groups * PIECES, per_piece, 0)

        @pl.when((at_z != turned) & (at_z != final))
        def _():
            products(at_z, 1 - y)

        return carry

    lax.fori_loop(1, depth + 1, round_of, 0)
    for p in range(PIECES):
        side_arrival(turned, last_part, p)
    for p in range(PIECES):
        arrive(index(final, 1 - y, 1 - core), last_part, p)
        arrive(index(turned, 1 - y, 1 - core), last_part, p)

    for step in range(1, shards):
        count_copy(me, lax.rem(me + step, shards)).wait_send()
    for step in range(1, groups):
        for k in range(groups):
            for p in range(PIECES):
                panel_copy(part, k, part_at(step), p).wait_send()

    def drain(i, carry):
        at_z, h, p = i // (groups * PIECES), lax.rem(i // PIECES, groups), lax.rem(i, PIECES)
        q = index(at_z, y, core)
        across = index(at_z, 1 - y, core)

        @pl.when((at_z <= z) & (z < depth - 1))
        def _():
            row_copy(q, h, p, UP).wait_send()

        @pl.when((at_z >= z) & (z > 0))
        def _():
            row_copy(q, h, p, DOWN).wait_send()

        @pl.when((at_z != turned) | (h != last_part))
        def _():
            row_copy(q, h, p, SIDE).wait_send()

        row_copy(q, h, p, CORE).wait_send()
        row_copy(across, h, p, CORE).wait_send()

        @pl.when((at_z == z) & (h == last_part) & (z > 0))
        def _():
            row_copy(across, h, p, DOWN).wait_send()

        @pl.when((at_z == z) & (h == last_part) & (z == depth - 2))
        def _():
            row_copy(across, h, p, UP).wait_send()

        return carry

    lax.fori_loop(0, depth * groups * PIECES, drain, 0)


def shape_of_line(depth):
    z = lax.axis_index("samp") // 4
    low = z < depth // 2
    inward = jnp.where(low, z + 1, z - 1)
    outward = jnp.clip(jnp.where(low, z - 1, z + 1), 0, depth - 1)
    is_end = (z == 0) | (z == depth - 1)
    return z, inward, outward, is_end


def folded_finish(shards, groups, rows, panel, tiles, codes, steps, out_ref, late, out_sem):
    depth = shards // 4
    me = lax.axis_index("samp")
    y = (me // 2) % 2
    z, inward, outward, is_end = shape_of_line(depth)
    far_mid, far_end = depth - 1 - inward, depth - 1 - z
    last_part = lax.rem(lax.axis_index("snp") + groups - 1, groups)
    piece_rows = rows.shape[3]
    tile_rows = PIECES * piece_rows

    def is_late(q):
        return is_end & ((q // 4 == far_end) | ((q // 4 == far_mid) & ((q // 2) % 2 != y)))

    def put(q, carry):
        @pl.when(jnp.logical_not(is_late(q)))
        def _():
            pltpu.make_async_copy(tiles.at[q], out_ref.at[q, 0], out_sem.at[0]).start()

        return carry

    lax.fori_loop(0, shards, put, 0)

    @pl.when(is_end)
    def _():
        def decode(t, carry):
            for p in range(PIECES):
                for k in range(groups):
                    unit = (t * PIECES + p) * groups + k
                    late[t, p * piece_rows:(p + 1) * piece_rows, k * tile_rows:(k + 1) * tile_rows] = (
                        codes[unit].astype(jnp.float32) * steps[unit])
            q = index(far_end, jnp.where(t // 2 == 0, y, 1 - y), lax.rem(t, 2))
            pltpu.make_async_copy(late.at[t], out_ref.at[q, 0], out_sem.at[0]).start()
            return carry

        lax.fori_loop(0, 4, decode, 0)

        def form(i, carry):
            q = index(far_mid, 1 - y, i)
            late[4 + i] = tiles[q] + product(rows, panel, q, [last_part])
            pltpu.make_async_copy(late.at[4 + i], out_ref.at[q, 0], out_sem.at[0]).start()
            return carry

        lax.fori_loop(0, 2, form, 0)

    pltpu.make_async_copy(tiles, out_ref.at[:, 0], out_sem.at[0]).wait()


def folded(shards, groups, geno_hbm, obs_hbm, panel, rows, tiles, codes, steps, geno_ref, obs_ref, counts, columns,
           made, made_steps, load_sem, count_sem, across_send, across_recv, line_send, side_send, core_send, row_recv,
           core_recv, code_sem):
    row_count, snp_count = geno_ref.shape
    tile_rows = row_count // groups
    piece_rows = tile_rows // PIECES
    depth = shards // 4
    me = lax.axis_index("samp")
    part = lax.axis_index("snp")
    y, core = (me // 2) % 2, me % 2
    z, inward, outward, is_end = shape_of_line(depth)
    other = lax.rem(part + 1, groups)
    load_rows = row_count // LOADS

    def load(i):
        block = pl.ds(pl.multiple_of(i * load_rows, load_rows), load_rows)
        return (pltpu.make_async_copy(geno_hbm.at[block], geno_ref.at[block], load_sem.at[0, i]),
                pltpu.make_async_copy(obs_hbm.at[block], obs_ref.at[block], load_sem.at[1, i]))

    for i in range(LOADS):
        for copy in load(i):
            copy.start()

    barrier = pltpu.get_barrier_semaphore()
    for step in range(1, shards):
        pl.semaphore_signal(barrier, inc=1, device_id={"samp": lax.rem(me + step, shards)}, device_id_type=MESH)
    pl.semaphore_signal(barrier, inc=1, device_id={"snp": other}, device_id_type=MESH)

    def add_strip(i, total):
        alt, call = total
        strip = pl.ds(pl.multiple_of(i * STRIP, STRIP), STRIP)
        present = obs_ref[strip, :].astype(jnp.float32)
        held = present * geno_ref[strip, :]
        for r in range(0, STRIP, 8):
            alt = alt + held[r:r + 8]
            call = call + present[r:r + 8]
        return alt, call

    zero = jnp.zeros((8, snp_count), jnp.float32)
    alt, call = zero, zero
    strips = load_rows // STRIP
    for i in range(LOADS):
        for copy in load(i):
            copy.wait()
        alt, call = lax.fori_loop(i * strips, (i + 1) * strips, add_strip, (alt, call))
    counts[me, 0:1, :] = jnp.sum(alt, axis=0, keepdims=True)
    counts[me, 1:2, :] = jnp.sum(call, axis=0, keepdims=True)

    pl.semaphore_wait(barrier, shards)

    for step in range(1, shards):
        pltpu.make_async_remote_copy(
            src_ref=counts.at[me], dst_ref=counts.at[me], send_sem=count_sem.at[0], recv_sem=count_sem.at[1],
            device_id={"samp": lax.rem(me + step, shards)}, device_id_type=MESH).start()

    def await_bytes(ref, sem):
        pltpu.make_async_copy(ref, ref, sem).wait()

    others = counts.at[pl.ds(0, shards - 1)]
    await_bytes(others, count_sem.at[1])
    sums = counts[0]
    for s in range(1, shards):
        sums = sums + counts[s]
    frequency = sums[0:1] / (2.0 * jnp.maximum(sums[1:2], 1.0))
    shift = 2.0 * frequency
    gain = lax.rsqrt(jnp.maximum(shift * (1.0 - frequency), var_floor))

    def piece_of(k, p):
        return pl.ds(pl.multiple_of(k * tile_rows + p * piece_rows, piece_rows), piece_rows)

    strip_rows = min(STRIP, piece_rows)

    def scale_piece(k, p):
        def scale_strip(i, carry):
            start = pl.multiple_of(k * tile_rows + p * piece_rows + i * strip_rows, strip_rows)
            strip = pl.ds(start, strip_rows)
            present = obs_ref[strip, :].astype(jnp.float32)
            panel[part, strip, :] = (present * (geno_ref[strip, :] - shift) * gain).astype(jnp.bfloat16)
            return carry

        lax.fori_loop(0, piece_rows // strip_rows, scale_strip, 0)

    def panel_copy(k, p):
        block = panel.at[part, piece_of(k, p)]
        return pltpu.make_async_remote_copy(
            src_ref=block, dst_ref=block, send_sem=across_send.at[0],
            recv_sem=across_recv.at[jnp.where(k == part, PIECES, p)], device_id={"snp": other}, device_id_type=MESH)

    def column_copy(q, h, p):
        return pltpu.make_async_remote_copy(
            src_ref=rows.at[q, h, p], dst_ref=columns.at[part, h, pl.ds(pl.multiple_of(p * piece_rows, piece_rows), piece_rows)],
            send_sem=across_send.at[1], recv_sem=across_recv.at[PIECES + 1], device_id={"snp": other}, device_id_type=MESH)

    def own_copy(q, h, p, to, send_sem, src):
        return pltpu.make_async_remote_copy(
            src_ref=rows.at[q, h, p] if src is None else src, dst_ref=rows.at[q, h, p], send_sem=send_sem,
            recv_sem=row_recv.at[q // 2, h, p], device_id={"samp": to}, device_id_type=MESH)

    def send_in(q, h, p, src=None, extra=0):
        own_copy(q, h, p, index(inward, y, core), line_send.at[extra], src).start()

    def send_out(q, h, p, src=None):
        own_copy(q, h, p, index(outward, y, core), line_send.at[2], src).start()

    def send_side(q, h, p, src=None, extra=0):
        own_copy(q, h, p, index(z, 1 - y, core), side_send.at[extra], src).start()

    def half_of(q, h, p):
        return jnp.where(jnp.logical_not(is_end) & (q // 4 == depth - 1 - outward), p, h)

    def send_core(q, h, p, src=None):
        pltpu.make_async_remote_copy(
            src_ref=rows.at[q, h, p] if src is None else src, dst_ref=rows.at[q, h, p], send_sem=core_send.at[0],
            recv_sem=core_recv.at[q // 2, half_of(q, h, p)], device_id={"samp": index(z, y, 1 - core)},
            device_id_type=MESH).start()

    def arrive(q, h, p):
        await_bytes(rows.at[q, h, p], row_recv.at[q // 2, h, p])

    def arrive_core(q, half):
        await_bytes(rows.at[q, 0], core_recv.at[q // 2, half])

    def part_at(i):
        return lax.rem(part + i, groups)

    def send_own(h, p):
        mine = panel.at[h, piece_of(part, p)]
        send_side(me, h, p, mine)
        send_in(me, h, p, mine)

        @pl.when(jnp.logical_not(is_end))
        def _():
            send_out(me, h, p, mine)

        send_core(me, h, p, mine)
        rows[me, h, p] = panel[h, piece_of(part, p), :]

    for p in range(PIECES):
        scale_piece(other, p)
        panel_copy(other, p).start()
        scale_piece(part, p)
        send_own(part, p)
    for p in range(PIECES):
        panel_copy(part, p).start()
    for p in range(PIECES):
        await_bytes(panel.at[other, piece_of(part, p)], across_recv.at[p])
        send_own(other, p)

    def form(at_z, at_y, parts=None, wait=True):
        def per_core(t, carry):
            q = index(at_z, at_y, lax.rem(core + t, 2))
            if wait:
                @pl.when(t == 1)
                def _():
                    for half in (range(2) if parts is None else parts):
                        arrive_core(q, half)

            tiles[q] = product(rows, panel, q, range(groups) if parts is None else parts)
            return carry

        lax.fori_loop(0, 2, per_core, 0)

    def await_panel():
        await_bytes(panel.at[other, pl.ds(pl.multiple_of(other * tile_rows, tile_rows), tile_rows)], across_recv.at[PIECES])

    def pick(i, values):
        chosen = values[-1]
        for n in range(len(values) - 2, -1, -1):
            chosen = jnp.where(i == n, values[n], chosen)
        return chosen

    count = groups * PIECES

    @pl.when(is_end)
    def _():
        far_mid = depth - 1 - inward

        def first(t, carry):
            h, p = part_at(t // PIECES), lax.rem(t, PIECES)
            near, beside = index(inward, y, core), index(z, 1 - y, core)
            arrive(near, h, p)
            send_side(near, h, p)
            send_core(near, h, p)
            arrive(beside, h, p)
            send_in(beside, h, p)
            send_core(beside, h, p)
            return carry

        lax.fori_loop(0, count, first, 0)
        await_panel()

        def second(t, carry):
            h, p = part_at(t // PIECES), lax.rem(t, PIECES)
            far, cross = index(far_mid, y, core), index(inward, 1 - y, core)
            arrive(far, h, p)
            send_side(far, h, p)
            send_core(far, h, p)
            arrive(cross, h, p)
            send_core(cross, h, p)

            @pl.when(t < 3)
            def _():
                form(pick(t, (z, inward, z)), pick(t, (y, y, 1 - y)))

            return carry

        lax.fori_loop(0, count, second, 0)

        def third(t, carry):
            h, p = part_at(t // PIECES), lax.rem(t, PIECES)
            q = index(far_mid, 1 - y, core)
            arrive(q, h, p)
            send_core(q, h, p)

            @pl.when(t < 2)
            def _():
                form(pick(t, (far_mid, inward)), pick(t, (y, 1 - y)))

            @pl.when(t == 2)
            def _():
                form(far_mid, 1 - y, [part])

            return carry

        lax.fori_loop(0, count, third, 0)
        await_bytes(codes, code_sem.at[1])
        await_bytes(steps, code_sem.at[3])
        arrive_core(index(far_mid, 1 - y, 1 - core), other)
        await_bytes(rows.at[pl.ds(0, 2)], line_send.at[0])
        await_bytes(rows.at[pl.ds(0, 3)], side_send.at[0])
        await_bytes(rows.at[pl.ds(0, 6)], core_send.at[0])

    @pl.when(jnp.logical_not(is_end))
    def _():
        far = depth - 1 - outward

        def first(t, carry):
            h, p = part_at(t // PIECES), lax.rem(t, PIECES)
            end, near, beside = index(outward, y, core), index(inward, y, core), index(z, 1 - y, core)
            arrive(end, h, p)
            send_in(end, h, p)
            send_core(end, h, p)
            column_copy(end, h, p).start()
            arrive(near, h, p)
            send_out(near, h, p)
            send_core(near, h, p)
            arrive(beside, h, p)
            send_core(beside, h, p)
            return carry

        lax.fori_loop(0, count, first, 0)
        for p in range(PIECES):
            send_in(index(z, 1 - y, core), part, p, extra=1)
        for h in range(groups):
            columns[part, h] = rows[index(outward, y, core), h].reshape(tile_rows, snp_count)
        await_panel()

        def make(side, p, k):
            def per_core(t, carry):
                which = lax.rem(core + t, 2)
                q = index(far, jnp.where(side == 0, y, 1 - y), which)
                term = None
                for h in range(groups):
                    one = lax.dot_general(rows[q, h, p], columns[k, h], (((1,), (1,)), ((), ())),
                                          preferred_element_type=jnp.float32)
                    term = one if term is None else term + one
                term = term * (1.0 / (groups * snp_count))
                top = jnp.max(jnp.abs(term), axis=0, keepdims=True)
                unit = ((side * 2 + which) * PIECES + p) * groups + k
                made[unit] = jnp.round(term * (CODE_TOP / jnp.maximum(top, TINY))).astype(jnp.int32).astype(jnp.int16)
                made_steps[unit] = top * (1.0 / CODE_TOP)
                for n, (source, target) in enumerate(((made, codes), (made_steps, steps))):
                    pltpu.make_async_remote_copy(
                        src_ref=source.at[unit], dst_ref=target.at[unit], send_sem=code_sem.at[2 * n],
                        recv_sem=code_sem.at[2 * n + 1], device_id={"samp": index(outward, y, core)},
                        device_id_type=MESH).start()
                return carry

            lax.fori_loop(0, 2, per_core, 0)

        def far_core(side, p):
            arrive_core(index(far, jnp.where(side == 0, y, 1 - y), 1 - core), p)

        def make_list(listed):
            def per_entry(i, carry):
                side, p, away = (pick(i, [entry[n] for entry in listed]) for n in range(3))
                make(side, p, lax.rem(part + away, groups))
                return carry

            lax.fori_loop(0, len(listed), per_entry, 0)

        def second(t, carry):
            h, p = part_at(lax.rem(t, groups)), t // groups
            far_q, cross = index(far, y, core), index(outward, 1 - y, core)

            @pl.when(t == 3)
            def _():
                far_core(0, 0)
                far_core(1, 0)
                make_list([(0, 0, 0), (1, 0, 0)])

            arrive(far_q, h, p)
            send_side(far_q, h, p)
            send_core(far_q, h, p)
            ch, cp = part_at(t // PIECES), lax.rem(t, PIECES)
            arrive(cross, ch, cp)
            send_core(cross, ch, cp)

            @pl.when(t > 0)
            def _():
                q = index(far, 1 - y, core)
                h, p = part_at(lax.rem(t - 1, groups)), (t - 1) // groups
                arrive(q, h, p)
                send_core(q, h, p)

            form(pick(t, (z, outward, inward, z)), pick(t, (y, y, y, 1 - y)))
            return carry

        lax.fori_loop(0, count, second, 0)
        for p in range(PIECES):
            send_side(index(inward, y, core), other, p, extra=1)
        far_core(0, 1)
        make_list([(0, 1, 0)])
        await_bytes(columns.at[other], across_recv.at[PIECES + 1])
        make_list([(0, 0, 1), (0, 1, 1), (1, 0, 1)])
        q = index(far, 1 - y, core)
        arrive(q, other, PIECES - 1)
        send_core(q, other, PIECES - 1)
        far_core(1, 1)
        make_list([(1, 1, 0), (1, 1, 1)])

        def third(t, carry):
            h, p = part_at(t // PIECES), lax.rem(t, PIECES)
            q = index(inward, 1 - y, core)
            arrive(q, h, p)
            send_core(q, h, p)

            @pl.when(t == 0)
            def _():
                form(outward, 1 - y)

            return carry

        lax.fori_loop(0, count, third, 0)
        form(far, y, wait=False)
        form(far, 1 - y, wait=False)
        form(inward, 1 - y)
        await_bytes(rows.at[pl.ds(0, 2)], line_send.at[0])
        await_bytes(rows.at[0, 0], line_send.at[1])
        await_bytes(rows.at[pl.ds(0, 2)], line_send.at[2])
        await_bytes(rows.at[pl.ds(0, 2)], side_send.at[0])
        await_bytes(rows.at[0, 0], side_send.at[1])
        await_bytes(rows.at[pl.ds(0, 8)], core_send.at[0])
        await_bytes(rows.at[0], across_send.at[1])
        await_bytes(made, code_sem.at[0])
        await_bytes(made_steps, code_sem.at[2])

    await_bytes(others, count_sem.at[0])
    await_bytes(rows.at[0], across_send.at[0])


def folded_body(shards, groups, genotypes, observed):
    row_count, snp_count = genotypes.shape
    tile_rows = row_count // groups
    piece_rows = tile_rows // PIECES
    units = 4 * PIECES * groups
    outs = (
        pltpu.VMEM((groups, row_count, snp_count), jnp.bfloat16),
        pltpu.VMEM((shards, groups, PIECES, piece_rows, snp_count), jnp.bfloat16),
        pltpu.VMEM((shards, tile_rows, row_count), jnp.float32),
        pltpu.VMEM((units, piece_rows, tile_rows), jnp.int16),
        pltpu.VMEM((units, 1, tile_rows), jnp.float32),
    )
    kept = sum(math.prod(o.shape) * jnp.dtype(o.dtype).itemsize for o in outs)
    held = pl.pallas_call(
        functools.partial(folded, shards, groups),
        out_shape=outs,
        in_specs=[pl.BlockSpec(memory_space=pltpu.HBM)] * 2,
        out_specs=[pl.BlockSpec(memory_space=pltpu.VMEM)] * 5,
        scratch_shapes=[
            pltpu.VMEM((row_count, snp_count), jnp.float32),
            pltpu.VMEM((row_count, snp_count), jnp.int32),
            pltpu.VMEM((shards, 2, snp_count), jnp.float32),
            pltpu.VMEM((groups, groups, tile_rows, snp_count), jnp.bfloat16),
            pltpu.VMEM((units, piece_rows, tile_rows), jnp.int16),
            pltpu.VMEM((units, 1, tile_rows), jnp.float32),
            pltpu.SemaphoreType.DMA((2, LOADS)),
            pltpu.SemaphoreType.DMA((2,)),
            pltpu.SemaphoreType.DMA((2,)),
            pltpu.SemaphoreType.DMA((PIECES + 2,)),
            pltpu.SemaphoreType.DMA((3,)),
            pltpu.SemaphoreType.DMA((2,)),
            pltpu.SemaphoreType.DMA((1,)),
            pltpu.SemaphoreType.DMA((shards // 2, groups, PIECES)),
            pltpu.SemaphoreType.DMA((shards // 2, 2)),
            pltpu.SemaphoreType.DMA((4,)),
        ],
        compiler_params=pltpu.CompilerParams(
            collective_id=0, has_side_effects=True, vmem_limit_bytes=VMEM_ALL - FOLDED_SPARE - kept),
    )(genotypes, observed)
    panel, rows, tiles, codes, steps = held
    return pl.pallas_call(
        functools.partial(folded_finish, shards, groups),
        out_shape=jax.ShapeDtypeStruct((shards, 1, tile_rows, row_count), jnp.float32),
        in_specs=[pl.BlockSpec(memory_space=pltpu.VMEM)] * 5,
        out_specs=pl.BlockSpec(memory_space=pltpu.HBM),
        scratch_shapes=[
            pltpu.VMEM((6, tile_rows, row_count), jnp.float32),
            pltpu.SemaphoreType.DMA((1,)),
        ],
        compiler_params=pltpu.CompilerParams(vmem_limit_bytes=FOLDED_FINISH),
    )(rows, panel, tiles, codes, steps)


def solution(mesh):
    shards, groups = mesh.shape["samp"], mesh.shape["snp"]

    def body(genotypes, observed):
        if groups == 2 and shards == 16:
            return folded_body(shards, groups, genotypes, observed)
        row_count, snp_count = genotypes.shape
        tile_rows = row_count // groups
        piece_rows = tile_rows // PIECES
        kept = 2 * (groups * row_count * snp_count) * (1 + shards // groups) + 4 * shards * tile_rows * row_count
        panel, rows, tiles = pl.pallas_call(
            functools.partial(kernel, shards, groups),
            out_shape=(
                pltpu.VMEM((groups, row_count, snp_count), jnp.bfloat16),
                pltpu.VMEM((shards, groups, PIECES, piece_rows, snp_count), jnp.bfloat16),
                pltpu.VMEM((shards, tile_rows, row_count), jnp.float32),
            ),
            in_specs=[pl.BlockSpec(memory_space=pltpu.HBM)] * 2,
            out_specs=[pl.BlockSpec(memory_space=pltpu.VMEM)] * 3,
            scratch_shapes=[
                pltpu.VMEM((row_count, snp_count), jnp.float32),
                pltpu.VMEM((row_count, snp_count), jnp.int32),
                pltpu.VMEM((shards, 2, snp_count), jnp.float32),
                pltpu.SemaphoreType.DMA((2, LOADS)),
                pltpu.SemaphoreType.DMA((shards,)),
                pltpu.SemaphoreType.DMA((shards,)),
                pltpu.SemaphoreType.DMA((groups, groups, PIECES)),
                pltpu.SemaphoreType.DMA((groups, groups, PIECES)),
                pltpu.SemaphoreType.DMA((4, shards, groups, PIECES)),
                pltpu.SemaphoreType.DMA((shards, groups, PIECES)),
            ],
            compiler_params=pltpu.CompilerParams(
                collective_id=0, has_side_effects=True, vmem_limit_bytes=VMEM_ALL - VMEM_SPARE - kept),
        )(genotypes, observed)
        return pl.pallas_call(
            functools.partial(finish, shards, groups),
            out_shape=jax.ShapeDtypeStruct((shards, 1, tile_rows, row_count), jnp.float32),
            in_specs=[pl.BlockSpec(memory_space=pltpu.VMEM)] * 3,
            out_specs=pl.BlockSpec(memory_space=pltpu.HBM),
            scratch_shapes=[
                pltpu.VMEM((4, tile_rows, row_count), jnp.float32),
                pltpu.SemaphoreType.DMA((shards,)),
            ],
            compiler_params=pltpu.CompilerParams(vmem_limit_bytes=VMEM_FINISH),
        )(rows, panel, tiles)

    return jax.shard_map(
        body,
        mesh=mesh,
        in_specs=(P("samp", "snp"), P("samp", "snp")),
        out_specs=P(None, "snp", None, "samp"),
        check_vma=False,
    )
```

```python
import functools
import math

import jax
import jax.numpy as jnp
from jax import lax
from jax.experimental import pallas as pl
from jax.experimental.pallas import tpu as pltpu
from jax.sharding import PartitionSpec as P

MESH = pl.DeviceIdType.MESH
var_floor = 0.1
UP, DOWN, SIDE, CORE = 0, 1, 2, 3
STRIP = 64
PIECES = 2
LOADS = 4
VMEM_ALL = 67043328
VMEM_SPARE = 512 * 1024
VMEM_FINISH = 12 * 1024 * 1024
FOLDED_SPARE = 1024 * 1024
FOLDED_FINISH = 8 * 1024 * 1024
CODE_TOP = 32767.0
TINY = 1e-30


def index(at_z, at_y, at_core):
    return at_z * 4 + at_y * 2 + at_core


def source_at(z, depth, i):
    pairs = jnp.minimum(z, depth - 1 - z)
    side = jnp.where(i % 2 == 1, z - (i + 1) // 2, z + i // 2)
    far = jnp.where(z < depth - 1 - z, z + i - pairs, z - i + pairs)
    return jnp.where(i <= 2 * pairs, side, far)


def turned_at(z, depth):
    return jnp.where(z < depth - 1, z + 1, depth - 2)


def product(rows, panel, q, parts):
    pieces, piece_rows, snp_count = rows.shape[2:]
    total = None
    for h in parts:
        block = rows[q, h].reshape(pieces * piece_rows, snp_count)
        term = lax.dot_general(block, panel[h], (((1,), (1,)), ((), ())), preferred_element_type=jnp.float32)
        total = term if total is None else total + term
    return total * (1.0 / (rows.shape[1] * snp_count))


def finish(shards, groups, rows, panel, tiles, out_ref, late, out_sem):
    depth = shards // 4
    me = lax.axis_index("samp")
    z, y = me // 4, (me // 2) % 2
    turned = turned_at(z, depth)
    final = source_at(z, depth, depth - 1)
    final = jnp.where(final == turned, source_at(z, depth, depth - 2), final)
    last_part = lax.rem(lax.axis_index("snp") + groups - 1, groups)

    def is_late(q):
        return ((q // 4 == turned) | (q // 4 == final)) & ((q // 2) % 2 != y)

    def put(q, carry):
        @pl.when(jnp.logical_not(is_late(q)))
        def _():
            pltpu.make_async_copy(tiles.at[q], out_ref.at[q, 0], out_sem.at[q]).start()

        return carry

    lax.fori_loop(0, shards, put, 0)

    def form(i, carry):
        q = index(jnp.where(i // 2 == 0, final, turned), 1 - y, lax.rem(i, 2))
        late[i] = tiles[q] + product(rows, panel, q, [last_part])
        pltpu.make_async_copy(late.at[i], out_ref.at[q, 0], out_sem.at[q]).start()
        return carry

    lax.fori_loop(0, 4, form, 0)

    def flush(q, carry):
        pltpu.make_async_copy(tiles.at[q], out_ref.at[q, 0], out_sem.at[q]).wait()
        return carry

    lax.fori_loop(0, shards, flush, 0)


def kernel(shards, groups, geno_hbm, obs_hbm, panel, rows, tiles, geno_ref, obs_ref, counts, load_sem,
           count_send, count_recv, panel_send, panel_recv, row_send, row_recv):
    row_count, snp_count = geno_ref.shape
    tile_rows = row_count // groups
    piece_rows = tile_rows // PIECES
    depth = shards // 4
    me = lax.axis_index("samp")
    part = lax.axis_index("snp")
    z, y, core = me // 4, (me // 2) % 2, me % 2

    load_rows = row_count // LOADS

    def load(i):
        block = pl.ds(pl.multiple_of(i * load_rows, load_rows), load_rows)
        return (pltpu.make_async_copy(geno_hbm.at[block], geno_ref.at[block], load_sem.at[0, i]),
                pltpu.make_async_copy(obs_hbm.at[block], obs_ref.at[block], load_sem.at[1, i]))

    for i in range(LOADS):
        for copy in load(i):
            copy.start()

    barrier = pltpu.get_barrier_semaphore()
    for step in range(1, shards):
        pl.semaphore_signal(barrier, inc=1, device_id={"samp": lax.rem(me + step, shards)}, device_id_type=MESH)
    for step in range(1, groups):
        pl.semaphore_signal(barrier, inc=1, device_id={"snp": lax.rem(part + step, groups)}, device_id_type=MESH)

    def add_strip(i, total):
        alt, call = total
        strip = pl.ds(pl.multiple_of(i * STRIP, STRIP), STRIP)
        present = obs_ref[strip, :].astype(jnp.float32)
        held = present * geno_ref[strip, :]
        for r in range(0, STRIP, 8):
            alt = alt + held[r:r + 8]
            call = call + present[r:r + 8]
        return alt, call

    zero = jnp.zeros((8, snp_count), jnp.float32)
    alt, call = zero, zero
    strips = load_rows // STRIP
    for i in range(LOADS):
        for copy in load(i):
            copy.wait()
        alt, call = lax.fori_loop(i * strips, (i + 1) * strips, add_strip, (alt, call))
    counts[me, 0:1, :] = jnp.sum(alt, axis=0, keepdims=True)
    counts[me, 1:2, :] = jnp.sum(call, axis=0, keepdims=True)

    pl.semaphore_wait(barrier, shards + groups - 2)

    def count_copy(owner, to):
        return pltpu.make_async_remote_copy(
            src_ref=counts.at[owner], dst_ref=counts.at[owner], send_sem=count_send.at[to],
            recv_sem=count_recv.at[owner], device_id={"samp": to}, device_id_type=MESH)

    for step in range(1, shards):
        count_copy(me, lax.rem(me + step, shards)).start()
    for step in range(1, shards):
        other = lax.rem(me + step, shards)
        count_copy(other, other).wait_recv()
    sums = counts[0]
    for s in range(1, shards):
        sums = sums + counts[s]
    frequency = sums[0:1] / (2.0 * jnp.maximum(sums[1:2], 1.0))
    shift = 2.0 * frequency
    gain = lax.rsqrt(jnp.maximum(shift * (1.0 - frequency), var_floor))

    def piece_of(k, p):
        return pl.ds(pl.multiple_of(k * tile_rows + p * piece_rows, piece_rows), piece_rows)

    def panel_copy(h, k, to, p):
        block = panel.at[h, piece_of(k, p)]
        return pltpu.make_async_remote_copy(
            src_ref=block, dst_ref=block, send_sem=panel_send.at[to, k, p],
            recv_sem=panel_recv.at[h, k, p], device_id={"snp": to}, device_id_type=MESH)

    strip_rows = min(STRIP, piece_rows)

    def scale_piece(k, p):
        def scale_strip(i, carry):
            start = pl.multiple_of(k * tile_rows + p * piece_rows + i * strip_rows, strip_rows)
            strip = pl.ds(start, strip_rows)
            present = obs_ref[strip, :].astype(jnp.float32)
            panel[part, strip, :] = (present * (geno_ref[strip, :] - shift) * gain).astype(jnp.bfloat16)
            return carry

        lax.fori_loop(0, piece_rows // strip_rows, scale_strip, 0)

    def row_copy(q, h, p, way, src=None):
        to = (index(z + 1, y, core), index(z - 1, y, core), index(z, 1 - y, core), index(z, y, 1 - core))[way]
        return pltpu.make_async_remote_copy(
            src_ref=rows.at[q, h, p] if src is None else src, dst_ref=rows.at[q, h, p],
            send_sem=row_send.at[way, q, h, p], recv_sem=row_recv.at[q, h, p],
            device_id={"samp": to}, device_id_type=MESH)

    def arrive(q, h, p):
        row_copy(q, h, p, CORE).wait_recv()

    last_part = lax.rem(part + groups - 1, groups)
    turned = turned_at(z, depth)

    def part_at(i):
        return lax.rem(part + i, groups)

    def send_own(h, p):
        mine = panel.at[h, piece_of(part, p)]
        row_copy(me, h, p, SIDE, mine).start()

        @pl.when(z < depth - 1)
        def _():
            row_copy(me, h, p, UP, mine).start()

        @pl.when(z > 0)
        def _():
            row_copy(me, h, p, DOWN, mine).start()

        row_copy(me, h, p, CORE, mine).start()
        rows[me, h, p] = panel[h, piece_of(part, p), :]

    for p in range(PIECES):
        for step in range(1, groups):
            other = part_at(step)
            scale_piece(other, p)
            panel_copy(part, other, other, p).start()
        scale_piece(part, p)
        send_own(part, p)
    for step in range(1, groups):
        other = part_at(step)
        for k in range(1, groups):
            for p in range(PIECES):
                panel_copy(part, lax.rem(other + k, groups), other, p).start()
    for step in range(1, groups):
        h = part_at(step)
        for p in range(PIECES):
            panel_copy(h, part, h, p).wait_recv()
            send_own(h, p)

    def column_arrival(at_z, h, p, way):
        q = index(at_z, y, core)
        arrive(q, h, p)

        @pl.when(z < depth - 1 if way == UP else z > 0)
        def _():
            row_copy(q, h, p, way).start()

        @pl.when((at_z != turned) | (h != last_part))
        def _():
            row_copy(q, h, p, SIDE).start()

        row_copy(q, h, p, CORE).start()

    def column_arrivals(i):
        def per_piece(t, carry):
            h, p = part_at(t // PIECES), lax.rem(t, PIECES)

            @pl.when(z - i >= 0)
            def _():
                column_arrival(z - i, h, p, UP)

            @pl.when(z + i < depth)
            def _():
                column_arrival(z + i, h, p, DOWN)

            return carry

        lax.fori_loop(0, groups * PIECES, per_piece, 0)

    def arrive_all(q):
        def per_piece(t, carry):
            arrive(q, t // PIECES, lax.rem(t, PIECES))
            return carry

        lax.fori_loop(0, groups * PIECES, per_piece, 0)

    def products(at_z, at_y):
        def per_core(t, carry):
            q = index(at_z, at_y, lax.rem(core + t, 2))

            @pl.when(t == 1)
            def _():
                arrive_all(q)

            tiles[q] = product(rows, panel, q, range(groups))
            return carry

        lax.fori_loop(0, 2, per_core, 0)

    def side_arrival(at_z, h, p):
        q = index(at_z, 1 - y, core)
        arrive(q, h, p)
        row_copy(q, h, p, CORE).start()

    final = source_at(z, depth, depth - 1)
    final = jnp.where(final == turned, source_at(z, depth, depth - 2), final)

    def begin_late():
        def per_tile(t, carry):
            q = index(jnp.where(t % 2 == 0, turned, final), 1 - y, lax.rem(core + t // 2, 2))

            @pl.when(t >= 2)
            def _():
                for step in range(groups - 1):
                    for p in range(PIECES):
                        arrive(q, part_at(step), p)

            tiles[q] = product(rows, panel, q, [part_at(step) for step in range(groups - 1)])
            return carry

        lax.fori_loop(0, 4, per_tile, 0)

    def round_of(i, carry):
        @pl.when(i < depth)
        def _():
            column_arrivals(i)

        @pl.when(i == 1)
        def _():
            for step in range(1, groups):
                h = part_at(step)
                for k in range(1, groups):
                    for p in range(PIECES):
                        panel_copy(h, part_at(k), h, p).wait_recv()

        @pl.when(i == depth - 1)
        def _():
            q = index(z, 1 - y, core)

            @pl.when(z > 0)
            def _():
                for p in range(PIECES):
                    row_copy(q, last_part, p, DOWN).start()

            @pl.when(z == depth - 2)
            def _():
                for p in range(PIECES):
                    row_copy(q, last_part, p, UP).start()

        at_z = source_at(z, depth, i - 1)
        products(at_z, y)

        def per_piece(t, c):
            @pl.when((i == depth) & (t == (groups - 1) * PIECES))
            def _():
                begin_late()

            @pl.when((at_z != turned) | (t // PIECES != groups - 1))
            def _():
                side_arrival(at_z, part_at(t // PIECES), lax.rem(t, PIECES))

            return c

        lax.fori_loop(0, groups * PIECES, per_piece, 0)

        @pl.when((at_z != turned) & (at_z != final))
        def _():
            products(at_z, 1 - y)

        return carry

    lax.fori_loop(1, depth + 1, round_of, 0)
    for p in range(PIECES):
        side_arrival(turned, last_part, p)
    for p in range(PIECES):
        arrive(index(final, 1 - y, 1 - core), last_part, p)
        arrive(index(turned, 1 - y, 1 - core), last_part, p)

    for step in range(1, shards):
        count_copy(me, lax.rem(me + step, shards)).wait_send()
    for step in range(1, groups):
        for k in range(groups):
            for p in range(PIECES):
                panel_copy(part, k, part_at(step), p).wait_send()

    def drain(i, carry):
        at_z, h, p = i // (groups * PIECES), lax.rem(i // PIECES, groups), lax.rem(i, PIECES)
        q = index(at_z, y, core)
        across = index(at_z, 1 - y, core)

        @pl.when((at_z <= z) & (z < depth - 1))
        def _():
            row_copy(q, h, p, UP).wait_send()

        @pl.when((at_z >= z) & (z > 0))
        def _():
            row_copy(q, h, p, DOWN).wait_send()

        @pl.when((at_z != turned) | (h != last_part))
        def _():
            row_copy(q, h, p, SIDE).wait_send()

        row_copy(q, h, p, CORE).wait_send()
        row_copy(across, h, p, CORE).wait_send()

        @pl.when((at_z == z) & (h == last_part) & (z > 0))
        def _():
            row_copy(across, h, p, DOWN).wait_send()

        @pl.when((at_z == z) & (h == last_part) & (z == depth - 2))
        def _():
            row_copy(across, h, p, UP).wait_send()

        return carry

    lax.fori_loop(0, depth * groups * PIECES, drain, 0)


def shape_of_line(depth):
    z = lax.axis_index("samp") // 4
    low = z < depth // 2
    inward = jnp.where(low, z + 1, z - 1)
    outward = jnp.clip(jnp.where(low, z - 1, z + 1), 0, depth - 1)
    is_end = (z == 0) | (z == depth - 1)
    return z, inward, outward, is_end


def folded_finish(shards, groups, rows, panel, tiles, codes, steps, out_ref, late, out_sem):
    depth = shards // 4
    me = lax.axis_index("samp")
    y = (me // 2) % 2
    z, inward, outward, is_end = shape_of_line(depth)
    far_mid, far_end = depth - 1 - inward, depth - 1 - z
    last_part = lax.rem(lax.axis_index("snp") + groups - 1, groups)
    piece_rows = rows.shape[3]
    tile_rows = PIECES * piece_rows

    def is_late(q):
        return is_end & ((q // 4 == far_end) | ((q // 4 == far_mid) & ((q // 2) % 2 != y)))

    def put(q, carry):
        @pl.when(jnp.logical_not(is_late(q)))
        def _():
            pltpu.make_async_copy(tiles.at[q], out_ref.at[q, 0], out_sem.at[0]).start()

        return carry

    lax.fori_loop(0, shards, put, 0)

    @pl.when(is_end)
    def _():
        def decode(t, carry):
            for p in range(PIECES):
                for k in range(groups):
                    unit = (t * PIECES + p) * groups + k
                    late[t, p * piece_rows:(p + 1) * piece_rows, k * tile_rows:(k + 1) * tile_rows] = (
                        codes[unit].astype(jnp.float32) * steps[unit])
            q = index(far_end, jnp.where(t // 2 == 0, y, 1 - y), lax.rem(t, 2))
            pltpu.make_async_copy(late.at[t], out_ref.at[q, 0], out_sem.at[0]).start()
            return carry

        lax.fori_loop(0, 4, decode, 0)

        def form(i, carry):
            q = index(far_mid, 1 - y, i)
            late[4 + i] = tiles[q] + product(rows, panel, q, [last_part])
            pltpu.make_async_copy(late.at[4 + i], out_ref.at[q, 0], out_sem.at[0]).start()
            return carry

        lax.fori_loop(0, 2, form, 0)

    pltpu.make_async_copy(tiles, out_ref.at[:, 0], out_sem.at[0]).wait()


def folded(shards, groups, geno_hbm, obs_hbm, panel, rows, tiles, codes, steps, geno_ref, obs_ref, counts, columns,
           made, made_steps, load_sem, count_sem, across_send, across_recv, line_send, side_send, core_send, row_recv,
           core_recv, code_sem):
    row_count, snp_count = geno_ref.shape
    tile_rows = row_count // groups
    piece_rows = tile_rows // PIECES
    depth = shards // 4
    me = lax.axis_index("samp")
    part = lax.axis_index("snp")
    y, core = (me // 2) % 2, me % 2
    z, inward, outward, is_end = shape_of_line(depth)
    other = lax.rem(part + 1, groups)
    load_rows = row_count // LOADS

    def load(i):
        block = pl.ds(pl.multiple_of(i * load_rows, load_rows), load_rows)
        return (pltpu.make_async_copy(geno_hbm.at[block], geno_ref.at[block], load_sem.at[0, i]),
                pltpu.make_async_copy(obs_hbm.at[block], obs_ref.at[block], load_sem.at[1, i]))

    for i in range(LOADS):
        for copy in load(i):
            copy.start()

    barrier = pltpu.get_barrier_semaphore()
    for step in range(1, shards):
        pl.semaphore_signal(barrier, inc=1, device_id={"samp": lax.rem(me + step, shards)}, device_id_type=MESH)
    pl.semaphore_signal(barrier, inc=1, device_id={"snp": other}, device_id_type=MESH)

    def add_strip(i, total):
        alt, call = total
        strip = pl.ds(pl.multiple_of(i * STRIP, STRIP), STRIP)
        present = obs_ref[strip, :].astype(jnp.float32)
        held = present * geno_ref[strip, :]
        for r in range(0, STRIP, 8):
            alt = alt + held[r:r + 8]
            call = call + present[r:r + 8]
        return alt, call

    zero = jnp.zeros((8, snp_count), jnp.float32)
    alt, call = zero, zero
    strips = load_rows // STRIP
    for i in range(LOADS):
        for copy in load(i):
            copy.wait()
        alt, call = lax.fori_loop(i * strips, (i + 1) * strips, add_strip, (alt, call))
    counts[me, 0:1, :] = jnp.sum(alt, axis=0, keepdims=True)
    counts[me, 1:2, :] = jnp.sum(call, axis=0, keepdims=True)

    pl.semaphore_wait(barrier, shards)

    for step in range(1, shards):
        pltpu.make_async_remote_copy(
            src_ref=counts.at[me], dst_ref=counts.at[me], send_sem=count_sem.at[0], recv_sem=count_sem.at[1],
            device_id={"samp": lax.rem(me + step, shards)}, device_id_type=MESH).start()

    def await_bytes(ref, sem):
        pltpu.make_async_copy(ref, ref, sem).wait()

    others = counts.at[pl.ds(0, shards - 1)]
    await_bytes(others, count_sem.at[1])
    sums = counts[0]
    for s in range(1, shards):
        sums = sums + counts[s]
    frequency = sums[0:1] / (2.0 * jnp.maximum(sums[1:2], 1.0))
    shift = 2.0 * frequency
    gain = lax.rsqrt(jnp.maximum(shift * (1.0 - frequency), var_floor))

    def piece_of(k, p):
        return pl.ds(pl.multiple_of(k * tile_rows + p * piece_rows, piece_rows), piece_rows)

    strip_rows = min(STRIP, piece_rows)

    def scale_piece(k, p):
        def scale_strip(i, carry):
            start = pl.multiple_of(k * tile_rows + p * piece_rows + i * strip_rows, strip_rows)
            strip = pl.ds(start, strip_rows)
            present = obs_ref[strip, :].astype(jnp.float32)
            panel[part, strip, :] = (present * (geno_ref[strip, :] - shift) * gain).astype(jnp.bfloat16)
            return carry

        lax.fori_loop(0, piece_rows // strip_rows, scale_strip, 0)

    def panel_copy(k, p):
        block = panel.at[part, piece_of(k, p)]
        return pltpu.make_async_remote_copy(
            src_ref=block, dst_ref=block, send_sem=across_send.at[0],
            recv_sem=across_recv.at[jnp.where(k == part, PIECES, p)], device_id={"snp": other}, device_id_type=MESH)

    def column_copy(q, h, p):
        return pltpu.make_async_remote_copy(
            src_ref=rows.at[q, h, p], dst_ref=columns.at[part, h, pl.ds(pl.multiple_of(p * piece_rows, piece_rows), piece_rows)],
            send_sem=across_send.at[1], recv_sem=across_recv.at[PIECES + 1], device_id={"snp": other}, device_id_type=MESH)

    def own_copy(q, h, p, to, send_sem, src):
        return pltpu.make_async_remote_copy(
            src_ref=rows.at[q, h, p] if src is None else src, dst_ref=rows.at[q, h, p], send_sem=send_sem,
            recv_sem=row_recv.at[q // 2, h, p], device_id={"samp": to}, device_id_type=MESH)

    def send_in(q, h, p, src=None, extra=0):
        own_copy(q, h, p, index(inward, y, core), line_send.at[extra], src).start()

    def send_out(q, h, p, src=None):
        own_copy(q, h, p, index(outward, y, core), line_send.at[2], src).start()

    def send_side(q, h, p, src=None, extra=0):
        own_copy(q, h, p, index(z, 1 - y, core), side_send.at[extra], src).start()

    def half_of(q, h, p):
        return jnp.where(jnp.logical_not(is_end) & (q // 4 == depth - 1 - outward), p, h)

    def send_core(q, h, p, src=None):
        pltpu.make_async_remote_copy(
            src_ref=rows.at[q, h, p] if src is None else src, dst_ref=rows.at[q, h, p], send_sem=core_send.at[0],
            recv_sem=core_recv.at[q // 2, half_of(q, h, p)], device_id={"samp": index(z, y, 1 - core)},
            device_id_type=MESH).start()

    def arrive(q, h, p):
        await_bytes(rows.at[q, h, p], row_recv.at[q // 2, h, p])

    def arrive_core(q, half):
        await_bytes(rows.at[q, 0], core_recv.at[q // 2, half])

    def part_at(i):
        return lax.rem(part + i, groups)

    def send_own(h, p):
        mine = panel.at[h, piece_of(part, p)]
        send_side(me, h, p, mine)
        send_in(me, h, p, mine)

        @pl.when(jnp.logical_not(is_end))
        def _():
            send_out(me, h, p, mine)

        send_core(me, h, p, mine)
        rows[me, h, p] = panel[h, piece_of(part, p), :]

    for p in range(PIECES):
        scale_piece(other, p)
        panel_copy(other, p).start()
        scale_piece(part, p)
        send_own(part, p)
    for p in range(PIECES):
        panel_copy(part, p).start()
    for p in range(PIECES):
        await_bytes(panel.at[other, piece_of(part, p)], across_recv.at[p])
        send_own(other, p)

    def form(at_z, at_y, parts=None, wait=True):
        def per_core(t, carry):
            q = index(at_z, at_y, lax.rem(core + t, 2))
            if wait:
                @pl.when(t == 1)
                def _():
                    for half in (range(2) if parts is None else parts):
                        arrive_core(q, half)

            tiles[q] = product(rows, panel, q, range(groups) if parts is None else parts)
            return carry

        lax.fori_loop(0, 2, per_core, 0)

    def await_panel():
        await_bytes(panel.at[other, pl.ds(pl.multiple_of(other * tile_rows, tile_rows), tile_rows)], across_recv.at[PIECES])

    def pick(i, values):
        chosen = values[-1]
        for n in range(len(values) - 2, -1, -1):
            chosen = jnp.where(i == n, values[n], chosen)
        return chosen

    count = groups * PIECES

    @pl.when(is_end)
    def _():
        far_mid = depth - 1 - inward

        def first(t, carry):
            h, p = part_at(t // PIECES), lax.rem(t, PIECES)
            near, beside = index(inward, y, core), index(z, 1 - y, core)
            arrive(near, h, p)
            send_side(near, h, p)
            send_core(near, h, p)
            arrive(beside, h, p)
            send_in(beside, h, p)
            send_core(beside, h, p)
            return carry

        lax.fori_loop(0, count, first, 0)
        await_panel()

        def second(t, carry):
            h, p = part_at(t // PIECES), lax.rem(t, PIECES)
            far, cross = index(far_mid, y, core), index(inward, 1 - y, core)
            arrive(far, h, p)
            send_side(far, h, p)
            send_core(far, h, p)
            arrive(cross, h, p)
            send_core(cross, h, p)

            @pl.when(t < 3)
            def _():
                form(pick(t, (z, inward, z)), pick(t, (y, y, 1 - y)))

            return carry

        lax.fori_loop(0, count, second, 0)

        def third(t, carry):
            h, p = part_at(t // PIECES), lax.rem(t, PIECES)
            q = index(far_mid, 1 - y, core)
            arrive(q, h, p)
            send_core(q, h, p)

            @pl.when(t < 2)
            def _():
                form(pick(t, (far_mid, inward)), pick(t, (y, 1 - y)))

            @pl.when(t == 2)
            def _():
                form(far_mid, 1 - y, [part])

            return carry

        lax.fori_loop(0, count, third, 0)
        await_bytes(codes, code_sem.at[1])
        await_bytes(steps, code_sem.at[3])
        arrive_core(index(far_mid, 1 - y, 1 - core), other)
        await_bytes(rows.at[pl.ds(0, 2)], line_send.at[0])
        await_bytes(rows.at[pl.ds(0, 3)], side_send.at[0])
        await_bytes(rows.at[pl.ds(0, 6)], core_send.at[0])

    @pl.when(jnp.logical_not(is_end))
    def _():
        far = depth - 1 - outward

        def first(t, carry):
            h, p = part_at(t // PIECES), lax.rem(t, PIECES)
            end, near, beside = index(outward, y, core), index(inward, y, core), index(z, 1 - y, core)
            arrive(end, h, p)

            @pl.when(p == 0)
            def _():
                send_in(end, h, 0)

            @pl.when(h == other)
            def _():
                send_in(end, jnp.where(p == 0, part, other), 1)

            send_core(end, h, p)
            column_copy(end, h, p).start()
            arrive(near, h, p)
            send_out(near, h, p)
            send_core(near, h, p)
            arrive(beside, h, p)
            send_core(beside, h, p)
            return carry

        lax.fori_loop(0, count, first, 0)
        for p in range(PIECES):
            send_in(index(z, 1 - y, core), part, p, extra=1)
        for h in range(groups):
            columns[part, h] = rows[index(outward, y, core), h].reshape(tile_rows, snp_count)
        await_panel()

        def make(side, p, k):
            def per_core(t, carry):
                which = lax.rem(core + t, 2)
                q = index(far, jnp.where(side == 0, y, 1 - y), which)
                term = None
                for h in range(groups):
                    one = lax.dot_general(rows[q, h, p], columns[k, h], (((1,), (1,)), ((), ())),
                                          preferred_element_type=jnp.float32)
                    term = one if term is None else term + one
                term = term * (1.0 / (groups * snp_count))
                top = jnp.max(jnp.abs(term), axis=0, keepdims=True)
                unit = ((side * 2 + which) * PIECES + p) * groups + k
                made[unit] = jnp.round(term * (CODE_TOP / jnp.maximum(top, TINY))).astype(jnp.int32).astype(jnp.int16)
                made_steps[unit] = top * (1.0 / CODE_TOP)
                for n, (source, target) in enumerate(((made, codes), (made_steps, steps))):
                    pltpu.make_async_remote_copy(
                        src_ref=source.at[unit], dst_ref=target.at[unit], send_sem=code_sem.at[2 * n],
                        recv_sem=code_sem.at[2 * n + 1], device_id={"samp": index(outward, y, core)},
                        device_id_type=MESH).start()
                return carry

            lax.fori_loop(0, 2, per_core, 0)

        def far_core(side, p):
            arrive_core(index(far, jnp.where(side == 0, y, 1 - y), 1 - core), p)

        def make_list(listed):
            def per_entry(i, carry):
                side, p, away = (pick(i, [entry[n] for entry in listed]) for n in range(3))
                make(side, p, lax.rem(part + away, groups))
                return carry

            lax.fori_loop(0, len(listed), per_entry, 0)

        def second(t, carry):
            h, p = part_at(lax.rem(t, groups)), t // groups
            far_q, cross = index(far, y, core), index(outward, 1 - y, core)

            @pl.when(t >= 2)
            def _():
                far_core(t - 2, 0)
                make(t - 2, 0, part)

            arrive(far_q, h, p)
            send_side(far_q, h, p)
            send_core(far_q, h, p)
            ch, cp = part_at(t // PIECES), lax.rem(t, PIECES)
            arrive(cross, ch, cp)
            send_core(cross, ch, cp)

            @pl.when(t > 0)
            def _():
                q = index(far, 1 - y, core)
                h, p = part_at(lax.rem(t - 1, groups)), (t - 1) // groups
                arrive(q, h, p)
                send_core(q, h, p)

            form(pick(t, (z, outward, inward, z)), pick(t, (y, y, y, 1 - y)))
            return carry

        lax.fori_loop(0, count, second, 0)
        for p in range(PIECES):
            send_side(index(inward, y, core), other, p, extra=1)
        far_core(0, 1)
        make_list([(0, 1, 0)])
        await_bytes(columns.at[other], across_recv.at[PIECES + 1])
        make_list([(0, 0, 1), (0, 1, 1), (1, 0, 1)])
        form(outward, 1 - y)
        q = index(far, 1 - y, core)
        arrive(q, other, PIECES - 1)
        send_core(q, other, PIECES - 1)
        far_core(1, 1)
        make_list([(1, 1, 0), (1, 1, 1)])

        def third(t, carry):
            h, p = part_at(t // PIECES), lax.rem(t, PIECES)
            q = index(inward, 1 - y, core)
            arrive(q, h, p)
            send_core(q, h, p)

            @pl.when(t < 2)
            def _():
                form(far, pick(t, (y, 1 - y)), wait=False)

            return carry

        lax.fori_loop(0, count, third, 0)
        form(inward, 1 - y)
        await_bytes(rows.at[pl.ds(0, 2)], line_send.at[0])
        await_bytes(rows.at[0, 0], line_send.at[1])
        await_bytes(rows.at[pl.ds(0, 2)], line_send.at[2])
        await_bytes(rows.at[pl.ds(0, 2)], side_send.at[0])
        await_bytes(rows.at[0, 0], side_send.at[1])
        await_bytes(rows.at[pl.ds(0, 8)], core_send.at[0])
        await_bytes(rows.at[0], across_send.at[1])
        await_bytes(made, code_sem.at[0])
        await_bytes(made_steps, code_sem.at[2])

    await_bytes(others, count_sem.at[0])
    await_bytes(rows.at[0], across_send.at[0])


def folded_body(shards, groups, genotypes, observed):
    row_count, snp_count = genotypes.shape
    tile_rows = row_count // groups
    piece_rows = tile_rows // PIECES
    units = 4 * PIECES * groups
    outs = (
        pltpu.VMEM((groups, row_count, snp_count), jnp.bfloat16),
        pltpu.VMEM((shards, groups, PIECES, piece_rows, snp_count), jnp.bfloat16),
        pltpu.VMEM((shards, tile_rows, row_count), jnp.float32),
        pltpu.VMEM((units, piece_rows, tile_rows), jnp.int16),
        pltpu.VMEM((units, 1, tile_rows), jnp.float32),
    )
    kept = sum(math.prod(o.shape) * jnp.dtype(o.dtype).itemsize for o in outs)
    held = pl.pallas_call(
        functools.partial(folded, shards, groups),
        out_shape=outs,
        in_specs=[pl.BlockSpec(memory_space=pltpu.HBM)] * 2,
        out_specs=[pl.BlockSpec(memory_space=pltpu.VMEM)] * 5,
        scratch_shapes=[
            pltpu.VMEM((row_count, snp_count), jnp.float32),
            pltpu.VMEM((row_count, snp_count), jnp.int32),
            pltpu.VMEM((shards, 2, snp_count), jnp.float32),
            pltpu.VMEM((groups, groups, tile_rows, snp_count), jnp.bfloat16),
            pltpu.VMEM((units, piece_rows, tile_rows), jnp.int16),
            pltpu.VMEM((units, 1, tile_rows), jnp.float32),
            pltpu.SemaphoreType.DMA((2, LOADS)),
            pltpu.SemaphoreType.DMA((2,)),
            pltpu.SemaphoreType.DMA((2,)),
            pltpu.SemaphoreType.DMA((PIECES + 2,)),
            pltpu.SemaphoreType.DMA((3,)),
            pltpu.SemaphoreType.DMA((2,)),
            pltpu.SemaphoreType.DMA((1,)),
            pltpu.SemaphoreType.DMA((shards // 2, groups, PIECES)),
            pltpu.SemaphoreType.DMA((shards // 2, 2)),
            pltpu.SemaphoreType.DMA((4,)),
        ],
        compiler_params=pltpu.CompilerParams(
            collective_id=0, has_side_effects=True, vmem_limit_bytes=VMEM_ALL - FOLDED_SPARE - kept),
    )(genotypes, observed)
    panel, rows, tiles, codes, steps = held
    return pl.pallas_call(
        functools.partial(folded_finish, shards, groups),
        out_shape=jax.ShapeDtypeStruct((shards, 1, tile_rows, row_count), jnp.float32),
        in_specs=[pl.BlockSpec(memory_space=pltpu.VMEM)] * 5,
        out_specs=pl.BlockSpec(memory_space=pltpu.HBM),
        scratch_shapes=[
            pltpu.VMEM((6, tile_rows, row_count), jnp.float32),
            pltpu.SemaphoreType.DMA((1,)),
        ],
        compiler_params=pltpu.CompilerParams(vmem_limit_bytes=FOLDED_FINISH),
    )(rows, panel, tiles, codes, steps)


def solution(mesh):
    shards, groups = mesh.shape["samp"], mesh.shape["snp"]

    def body(genotypes, observed):
        if groups == 2 and shards == 16:
            return folded_body(shards, groups, genotypes, observed)
        row_count, snp_count = genotypes.shape
        tile_rows = row_count // groups
        piece_rows = tile_rows // PIECES
        kept = 2 * (groups * row_count * snp_count) * (1 + shards // groups) + 4 * shards * tile_rows * row_count
        panel, rows, tiles = pl.pallas_call(
            functools.partial(kernel, shards, groups),
            out_shape=(
                pltpu.VMEM((groups, row_count, snp_count), jnp.bfloat16),
                pltpu.VMEM((shards, groups, PIECES, piece_rows, snp_count), jnp.bfloat16),
                pltpu.VMEM((shards, tile_rows, row_count), jnp.float32),
            ),
            in_specs=[pl.BlockSpec(memory_space=pltpu.HBM)] * 2,
            out_specs=[pl.BlockSpec(memory_space=pltpu.VMEM)] * 3,
            scratch_shapes=[
                pltpu.VMEM((row_count, snp_count), jnp.float32),
                pltpu.VMEM((row_count, snp_count), jnp.int32),
                pltpu.VMEM((shards, 2, snp_count), jnp.float32),
                pltpu.SemaphoreType.DMA((2, LOADS)),
                pltpu.SemaphoreType.DMA((shards,)),
                pltpu.SemaphoreType.DMA((shards,)),
                pltpu.SemaphoreType.DMA((groups, groups, PIECES)),
                pltpu.SemaphoreType.DMA((groups, groups, PIECES)),
                pltpu.SemaphoreType.DMA((4, shards, groups, PIECES)),
                pltpu.SemaphoreType.DMA((shards, groups, PIECES)),
            ],
            compiler_params=pltpu.CompilerParams(
                collective_id=0, has_side_effects=True, vmem_limit_bytes=VMEM_ALL - VMEM_SPARE - kept),
        )(genotypes, observed)
        return pl.pallas_call(
            functools.partial(finish, shards, groups),
            out_shape=jax.ShapeDtypeStruct((shards, 1, tile_rows, row_count), jnp.float32),
            in_specs=[pl.BlockSpec(memory_space=pltpu.VMEM)] * 3,
            out_specs=pl.BlockSpec(memory_space=pltpu.HBM),
            scratch_shapes=[
                pltpu.VMEM((4, tile_rows, row_count), jnp.float32),
                pltpu.SemaphoreType.DMA((shards,)),
            ],
            compiler_params=pltpu.CompilerParams(vmem_limit_bytes=VMEM_FINISH),
        )(rows, panel, tiles)

    return jax.shard_map(
        body,
        mesh=mesh,
        in_specs=(P("samp", "snp"), P("samp", "snp")),
        out_specs=P(None, "snp", None, "samp"),
        check_vma=False,
    )
```

```python
import functools
import math

import jax
import jax.numpy as jnp
from jax import lax
from jax.experimental import pallas as pl
from jax.experimental.pallas import tpu as pltpu
from jax.sharding import PartitionSpec as P

MESH = pl.DeviceIdType.MESH
var_floor = 0.1
UP, DOWN, SIDE, CORE = 0, 1, 2, 3
STRIP = 64
PIECES = 2
LOADS = 4
VMEM_ALL = 67043328
VMEM_SPARE = 512 * 1024
VMEM_FINISH = 12 * 1024 * 1024
FOLDED_SPARE = 1024 * 1024
FOLDED_FINISH = 8 * 1024 * 1024
CODE_TOP = 32767.0
TINY = 1e-30


def index(at_z, at_y, at_core):
    return at_z * 4 + at_y * 2 + at_core


def source_at(z, depth, i):
    pairs = jnp.minimum(z, depth - 1 - z)
    side = jnp.where(i % 2 == 1, z - (i + 1) // 2, z + i // 2)
    far = jnp.where(z < depth - 1 - z, z + i - pairs, z - i + pairs)
    return jnp.where(i <= 2 * pairs, side, far)


def turned_at(z, depth):
    return jnp.where(z < depth - 1, z + 1, depth - 2)


def product(rows, panel, q, parts):
    pieces, piece_rows, snp_count = rows.shape[2:]
    total = None
    for h in parts:
        block = rows[q, h].reshape(pieces * piece_rows, snp_count)
        term = lax.dot_general(block, panel[h], (((1,), (1,)), ((), ())), preferred_element_type=jnp.float32)
        total = term if total is None else total + term
    return total * (1.0 / (rows.shape[1] * snp_count))


def finish(shards, groups, rows, panel, tiles, out_ref, late, out_sem):
    depth = shards // 4
    me = lax.axis_index("samp")
    z, y = me // 4, (me // 2) % 2
    turned = turned_at(z, depth)
    final = source_at(z, depth, depth - 1)
    final = jnp.where(final == turned, source_at(z, depth, depth - 2), final)
    last_part = lax.rem(lax.axis_index("snp") + groups - 1, groups)

    def is_late(q):
        return ((q // 4 == turned) | (q // 4 == final)) & ((q // 2) % 2 != y)

    def put(q, carry):
        @pl.when(jnp.logical_not(is_late(q)))
        def _():
            pltpu.make_async_copy(tiles.at[q], out_ref.at[q, 0], out_sem.at[q]).start()

        return carry

    lax.fori_loop(0, shards, put, 0)

    def form(i, carry):
        q = index(jnp.where(i // 2 == 0, final, turned), 1 - y, lax.rem(i, 2))
        late[i] = tiles[q] + product(rows, panel, q, [last_part])
        pltpu.make_async_copy(late.at[i], out_ref.at[q, 0], out_sem.at[q]).start()
        return carry

    lax.fori_loop(0, 4, form, 0)

    def flush(q, carry):
        pltpu.make_async_copy(tiles.at[q], out_ref.at[q, 0], out_sem.at[q]).wait()
        return carry

    lax.fori_loop(0, shards, flush, 0)


def kernel(shards, groups, geno_hbm, obs_hbm, panel, rows, tiles, geno_ref, obs_ref, counts, load_sem,
           count_send, count_recv, panel_send, panel_recv, row_send, row_recv):
    row_count, snp_count = geno_ref.shape
    tile_rows = row_count // groups
    piece_rows = tile_rows // PIECES
    depth = shards // 4
    me = lax.axis_index("samp")
    part = lax.axis_index("snp")
    z, y, core = me // 4, (me // 2) % 2, me % 2

    load_rows = row_count // LOADS

    def load(i):
        block = pl.ds(pl.multiple_of(i * load_rows, load_rows), load_rows)
        return (pltpu.make_async_copy(geno_hbm.at[block], geno_ref.at[block], load_sem.at[0, i]),
                pltpu.make_async_copy(obs_hbm.at[block], obs_ref.at[block], load_sem.at[1, i]))

    for i in range(LOADS):
        for copy in load(i):
            copy.start()

    barrier = pltpu.get_barrier_semaphore()
    for step in range(1, shards):
        pl.semaphore_signal(barrier, inc=1, device_id={"samp": lax.rem(me + step, shards)}, device_id_type=MESH)
    for step in range(1, groups):
        pl.semaphore_signal(barrier, inc=1, device_id={"snp": lax.rem(part + step, groups)}, device_id_type=MESH)

    def add_strip(i, total):
        alt, call = total
        strip = pl.ds(pl.multiple_of(i * STRIP, STRIP), STRIP)
        present = obs_ref[strip, :].astype(jnp.float32)
        held = present * geno_ref[strip, :]
        for r in range(0, STRIP, 8):
            alt = alt + held[r:r + 8]
            call = call + present[r:r + 8]
        return alt, call

    zero = jnp.zeros((8, snp_count), jnp.float32)
    alt, call = zero, zero
    strips = load_rows // STRIP
    for i in range(LOADS):
        for copy in load(i):
            copy.wait()
        alt, call = lax.fori_loop(i * strips, (i + 1) * strips, add_strip, (alt, call))
    counts[me, 0:1, :] = jnp.sum(alt, axis=0, keepdims=True)
    counts[me, 1:2, :] = jnp.sum(call, axis=0, keepdims=True)

    pl.semaphore_wait(barrier, shards + groups - 2)

    def count_copy(owner, to):
        return pltpu.make_async_remote_copy(
            src_ref=counts.at[owner], dst_ref=counts.at[owner], send_sem=count_send.at[to],
            recv_sem=count_recv.at[owner], device_id={"samp": to}, device_id_type=MESH)

    for step in range(1, shards):
        count_copy(me, lax.rem(me + step, shards)).start()
    for step in range(1, shards):
        other = lax.rem(me + step, shards)
        count_copy(other, other).wait_recv()
    sums = counts[0]
    for s in range(1, shards):
        sums = sums + counts[s]
    frequency = sums[0:1] / (2.0 * jnp.maximum(sums[1:2], 1.0))
    shift = 2.0 * frequency
    gain = lax.rsqrt(jnp.maximum(shift * (1.0 - frequency), var_floor))

    def piece_of(k, p):
        return pl.ds(pl.multiple_of(k * tile_rows + p * piece_rows, piece_rows), piece_rows)

    def panel_copy(h, k, to, p):
        block = panel.at[h, piece_of(k, p)]
        return pltpu.make_async_remote_copy(
            src_ref=block, dst_ref=block, send_sem=panel_send.at[to, k, p],
            recv_sem=panel_recv.at[h, k, p], device_id={"snp": to}, device_id_type=MESH)

    strip_rows = min(STRIP, piece_rows)

    def scale_piece(k, p):
        def scale_strip(i, carry):
            start = pl.multiple_of(k * tile_rows + p * piece_rows + i * strip_rows, strip_rows)
            strip = pl.ds(start, strip_rows)
            present = obs_ref[strip, :].astype(jnp.float32)
            panel[part, strip, :] = (present * (geno_ref[strip, :] - shift) * gain).astype(jnp.bfloat16)
            return carry

        lax.fori_loop(0, piece_rows // strip_rows, scale_strip, 0)

    def row_copy(q, h, p, way, src=None):
        to = (index(z + 1, y, core), index(z - 1, y, core), index(z, 1 - y, core), index(z, y, 1 - core))[way]
        return pltpu.make_async_remote_copy(
            src_ref=rows.at[q, h, p] if src is None else src, dst_ref=rows.at[q, h, p],
            send_sem=row_send.at[way, q, h, p], recv_sem=row_recv.at[q, h, p],
            device_id={"samp": to}, device_id_type=MESH)

    def arrive(q, h, p):
        row_copy(q, h, p, CORE).wait_recv()

    last_part = lax.rem(part + groups - 1, groups)
    turned = turned_at(z, depth)

    def part_at(i):
        return lax.rem(part + i, groups)

    def send_own(h, p):
        mine = panel.at[h, piece_of(part, p)]
        row_copy(me, h, p, SIDE, mine).start()

        @pl.when(z < depth - 1)
        def _():
            row_copy(me, h, p, UP, mine).start()

        @pl.when(z > 0)
        def _():
            row_copy(me, h, p, DOWN, mine).start()

        row_copy(me, h, p, CORE, mine).start()
        rows[me, h, p] = panel[h, piece_of(part, p), :]

    for p in range(PIECES):
        for step in range(1, groups):
            other = part_at(step)
            scale_piece(other, p)
            panel_copy(part, other, other, p).start()
        scale_piece(part, p)
        send_own(part, p)
    for step in range(1, groups):
        other = part_at(step)
        for k in range(1, groups):
            for p in range(PIECES):
                panel_copy(part, lax.rem(other + k, groups), other, p).start()
    for step in range(1, groups):
        h = part_at(step)
        for p in range(PIECES):
            panel_copy(h, part, h, p).wait_recv()
            send_own(h, p)

    def column_arrival(at_z, h, p, way):
        q = index(at_z, y, core)
        arrive(q, h, p)

        @pl.when(z < depth - 1 if way == UP else z > 0)
        def _():
            row_copy(q, h, p, way).start()

        @pl.when((at_z != turned) | (h != last_part))
        def _():
            row_copy(q, h, p, SIDE).start()

        row_copy(q, h, p, CORE).start()

    def column_arrivals(i):
        def per_piece(t, carry):
            h, p = part_at(t // PIECES), lax.rem(t, PIECES)

            @pl.when(z - i >= 0)
            def _():
                column_arrival(z - i, h, p, UP)

            @pl.when(z + i < depth)
            def _():
                column_arrival(z + i, h, p, DOWN)

            return carry

        lax.fori_loop(0, groups * PIECES, per_piece, 0)

    def arrive_all(q):
        def per_piece(t, carry):
            arrive(q, t // PIECES, lax.rem(t, PIECES))
            return carry

        lax.fori_loop(0, groups * PIECES, per_piece, 0)

    def products(at_z, at_y):
        def per_core(t, carry):
            q = index(at_z, at_y, lax.rem(core + t, 2))

            @pl.when(t == 1)
            def _():
                arrive_all(q)

            tiles[q] = product(rows, panel, q, range(groups))
            return carry

        lax.fori_loop(0, 2, per_core, 0)

    def side_arrival(at_z, h, p):
        q = index(at_z, 1 - y, core)
        arrive(q, h, p)
        row_copy(q, h, p, CORE).start()

    final = source_at(z, depth, depth - 1)
    final = jnp.where(final == turned, source_at(z, depth, depth - 2), final)

    def begin_late():
        def per_tile(t, carry):
            q = index(jnp.where(t % 2 == 0, turned, final), 1 - y, lax.rem(core + t // 2, 2))

            @pl.when(t >= 2)
            def _():
                for step in range(groups - 1):
                    for p in range(PIECES):
                        arrive(q, part_at(step), p)

            tiles[q] = product(rows, panel, q, [part_at(step) for step in range(groups - 1)])
            return carry

        lax.fori_loop(0, 4, per_tile, 0)

    def round_of(i, carry):
        @pl.when(i < depth)
        def _():
            column_arrivals(i)

        @pl.when(i == 1)
        def _():
            for step in range(1, groups):
                h = part_at(step)
                for k in range(1, groups):
                    for p in range(PIECES):
                        panel_copy(h, part_at(k), h, p).wait_recv()

        @pl.when(i == depth - 1)
        def _():
            q = index(z, 1 - y, core)

            @pl.when(z > 0)
            def _():
                for p in range(PIECES):
                    row_copy(q, last_part, p, DOWN).start()

            @pl.when(z == depth - 2)
            def _():
                for p in range(PIECES):
                    row_copy(q, last_part, p, UP).start()

        at_z = source_at(z, depth, i - 1)
        products(at_z, y)

        def per_piece(t, c):
            @pl.when((i == depth) & (t == (groups - 1) * PIECES))
            def _():
                begin_late()

            @pl.when((at_z != turned) | (t // PIECES != groups - 1))
            def _():
                side_arrival(at_z, part_at(t // PIECES), lax.rem(t, PIECES))

            return c

        lax.fori_loop(0, groups * PIECES, per_piece, 0)

        @pl.when((at_z != turned) & (at_z != final))
        def _():
            products(at_z, 1 - y)

        return carry

    lax.fori_loop(1, depth + 1, round_of, 0)
    for p in range(PIECES):
        side_arrival(turned, last_part, p)
    for p in range(PIECES):
        arrive(index(final, 1 - y, 1 - core), last_part, p)
        arrive(index(turned, 1 - y, 1 - core), last_part, p)

    for step in range(1, shards):
        count_copy(me, lax.rem(me + step, shards)).wait_send()
    for step in range(1, groups):
        for k in range(groups):
            for p in range(PIECES):
                panel_copy(part, k, part_at(step), p).wait_send()

    def drain(i, carry):
        at_z, h, p = i // (groups * PIECES), lax.rem(i // PIECES, groups), lax.rem(i, PIECES)
        q = index(at_z, y, core)
        across = index(at_z, 1 - y, core)

        @pl.when((at_z <= z) & (z < depth - 1))
        def _():
            row_copy(q, h, p, UP).wait_send()

        @pl.when((at_z >= z) & (z > 0))
        def _():
            row_copy(q, h, p, DOWN).wait_send()

        @pl.when((at_z != turned) | (h != last_part))
        def _():
            row_copy(q, h, p, SIDE).wait_send()

        row_copy(q, h, p, CORE).wait_send()
        row_copy(across, h, p, CORE).wait_send()

        @pl.when((at_z == z) & (h == last_part) & (z > 0))
        def _():
            row_copy(across, h, p, DOWN).wait_send()

        @pl.when((at_z == z) & (h == last_part) & (z == depth - 2))
        def _():
            row_copy(across, h, p, UP).wait_send()

        return carry

    lax.fori_loop(0, depth * groups * PIECES, drain, 0)


def shape_of_line(depth):
    z = lax.axis_index("samp") // 4
    low = z < depth // 2
    inward = jnp.where(low, z + 1, z - 1)
    outward = jnp.clip(jnp.where(low, z - 1, z + 1), 0, depth - 1)
    is_end = (z == 0) | (z == depth - 1)
    return z, inward, outward, is_end


def folded_finish(shards, groups, rows, panel, tiles, codes, steps, out_ref, late, out_sem):
    depth = shards // 4
    me = lax.axis_index("samp")
    y = (me // 2) % 2
    z, inward, outward, is_end = shape_of_line(depth)
    far_mid, far_end = depth - 1 - inward, depth - 1 - z
    last_part = lax.rem(lax.axis_index("snp") + groups - 1, groups)
    piece_rows = rows.shape[3]
    tile_rows = PIECES * piece_rows

    def is_late(q):
        return is_end & ((q // 4 == far_end) | ((q // 4 == far_mid) & ((q // 2) % 2 != y)))

    def put(q, carry):
        @pl.when(jnp.logical_not(is_late(q)))
        def _():
            pltpu.make_async_copy(tiles.at[q], out_ref.at[q, 0], out_sem.at[0]).start()

        return carry

    lax.fori_loop(0, shards, put, 0)

    @pl.when(is_end)
    def _():
        def decode(t, carry):
            for p in range(PIECES):
                for k in range(groups):
                    unit = (t * PIECES + p) * groups + k
                    late[t, p * piece_rows:(p + 1) * piece_rows, k * tile_rows:(k + 1) * tile_rows] = (
                        codes[unit].astype(jnp.float32) * steps[unit])
            q = index(far_end, jnp.where(t // 2 == 0, y, 1 - y), lax.rem(t, 2))
            pltpu.make_async_copy(late.at[t], out_ref.at[q, 0], out_sem.at[0]).start()
            return carry

        lax.fori_loop(0, 4, decode, 0)

        def form(i, carry):
            q = index(far_mid, 1 - y, i)
            late[4 + i] = tiles[q] + product(rows, panel, q, [last_part])
            pltpu.make_async_copy(late.at[4 + i], out_ref.at[q, 0], out_sem.at[0]).start()
            return carry

        lax.fori_loop(0, 2, form, 0)

    pltpu.make_async_copy(tiles, out_ref.at[:, 0], out_sem.at[0]).wait()


def folded(shards, groups, geno_hbm, obs_hbm, panel, rows, tiles, codes, steps, geno_ref, obs_ref, counts, columns,
           made, made_steps, load_sem, count_sem, across_send, across_recv, line_send, side_send, core_send, row_recv,
           core_recv, code_sem):
    row_count, snp_count = geno_ref.shape
    tile_rows = row_count // groups
    piece_rows = tile_rows // PIECES
    depth = shards // 4
    me = lax.axis_index("samp")
    part = lax.axis_index("snp")
    y, core = (me // 2) % 2, me % 2
    z, inward, outward, is_end = shape_of_line(depth)
    other = lax.rem(part + 1, groups)
    load_rows = row_count // LOADS

    def load(i):
        block = pl.ds(pl.multiple_of(i * load_rows, load_rows), load_rows)
        return (pltpu.make_async_copy(geno_hbm.at[block], geno_ref.at[block], load_sem.at[0, i]),
                pltpu.make_async_copy(obs_hbm.at[block], obs_ref.at[block], load_sem.at[1, i]))

    for i in range(LOADS):
        for copy in load(i):
            copy.start()

    barrier = pltpu.get_barrier_semaphore()
    for step in range(1, shards):
        pl.semaphore_signal(barrier, inc=1, device_id={"samp": lax.rem(me + step, shards)}, device_id_type=MESH)
    pl.semaphore_signal(barrier, inc=1, device_id={"snp": other}, device_id_type=MESH)

    def add_strip(i, total):
        alt, call = total
        strip = pl.ds(pl.multiple_of(i * STRIP, STRIP), STRIP)
        present = obs_ref[strip, :].astype(jnp.float32)
        held = present * geno_ref[strip, :]
        for r in range(0, STRIP, 8):
            alt = alt + held[r:r + 8]
            call = call + present[r:r + 8]
        return alt, call

    zero = jnp.zeros((8, snp_count), jnp.float32)
    alt, call = zero, zero
    strips = load_rows // STRIP
    for i in range(LOADS):
        for copy in load(i):
            copy.wait()
        alt, call = lax.fori_loop(i * strips, (i + 1) * strips, add_strip, (alt, call))
    counts[me, 0:1, :] = jnp.sum(alt, axis=0, keepdims=True)
    counts[me, 1:2, :] = jnp.sum(call, axis=0, keepdims=True)

    pl.semaphore_wait(barrier, shards)

    for step in range(shards):
        to = jnp.where(z < depth // 2, shards - 1 - step, step)

        @pl.when(to != me)
        def _():
            pltpu.make_async_remote_copy(
                src_ref=counts.at[me], dst_ref=counts.at[me], send_sem=count_sem.at[0], recv_sem=count_sem.at[1],
                device_id={"samp": to}, device_id_type=MESH).start()

    def await_bytes(ref, sem):
        pltpu.make_async_copy(ref, ref, sem).wait()

    others = counts.at[pl.ds(0, shards - 1)]
    await_bytes(others, count_sem.at[1])
    sums = counts[0]
    for s in range(1, shards):
        sums = sums + counts[s]
    frequency = sums[0:1] / (2.0 * jnp.maximum(sums[1:2], 1.0))
    shift = 2.0 * frequency
    gain = lax.rsqrt(jnp.maximum(shift * (1.0 - frequency), var_floor))

    def piece_of(k, p):
        return pl.ds(pl.multiple_of(k * tile_rows + p * piece_rows, piece_rows), piece_rows)

    strip_rows = min(STRIP, piece_rows)

    def scale_piece(k, p):
        def scale_strip(i, carry):
            start = pl.multiple_of(k * tile_rows + p * piece_rows + i * strip_rows, strip_rows)
            strip = pl.ds(start, strip_rows)
            present = obs_ref[strip, :].astype(jnp.float32)
            panel[part, strip, :] = (present * (geno_ref[strip, :] - shift) * gain).astype(jnp.bfloat16)
            return carry

        lax.fori_loop(0, piece_rows // strip_rows, scale_strip, 0)

    def panel_copy(k, p):
        block = panel.at[part, piece_of(k, p)]
        return pltpu.make_async_remote_copy(
            src_ref=block, dst_ref=block, send_sem=across_send.at[0],
            recv_sem=across_recv.at[jnp.where(k == part, PIECES, p)], device_id={"snp": other}, device_id_type=MESH)

    def column_copy(q, h, p):
        return pltpu.make_async_remote_copy(
            src_ref=rows.at[q, h, p], dst_ref=columns.at[part, h, pl.ds(pl.multiple_of(p * piece_rows, piece_rows), piece_rows)],
            send_sem=across_send.at[1], recv_sem=across_recv.at[PIECES + 1], device_id={"snp": other}, device_id_type=MESH)

    cut = piece_rows * 7 // 8
    head, rest = pl.ds(0, cut), pl.ds(cut, piece_rows - cut)

    def span_copy(q, h, p, span, to, send_sem, recv_sem):
        return pltpu.make_async_remote_copy(
            src_ref=rows.at[q, h, p, span], dst_ref=rows.at[q, h, p, span], send_sem=send_sem, recv_sem=recv_sem,
            device_id={"samp": to}, device_id_type=MESH)

    def own_copy(q, h, p, to, send_sem, src):
        return pltpu.make_async_remote_copy(
            src_ref=rows.at[q, h, p] if src is None else src, dst_ref=rows.at[q, h, p], send_sem=send_sem,
            recv_sem=row_recv.at[q // 2, h, p], device_id={"samp": to}, device_id_type=MESH)

    def send_in(q, h, p, src=None, extra=0):
        own_copy(q, h, p, index(inward, y, core), line_send.at[extra], src).start()

    def send_out(q, h, p, src=None):
        own_copy(q, h, p, index(outward, y, core), line_send.at[2], src).start()

    def send_side(q, h, p, src=None, extra=0):
        own_copy(q, h, p, index(z, 1 - y, core), side_send.at[extra], src).start()

    def half_of(q, h, p):
        return jnp.where(jnp.logical_not(is_end) & (q // 4 == depth - 1 - outward), p, h)

    def send_core(q, h, p, src=None):
        pltpu.make_async_remote_copy(
            src_ref=rows.at[q, h, p] if src is None else src, dst_ref=rows.at[q, h, p], send_sem=core_send.at[0],
            recv_sem=core_recv.at[q // 2, half_of(q, h, p)], device_id={"samp": index(z, y, 1 - core)},
            device_id_type=MESH).start()

    def send_core_span(q, h, p, span):
        span_copy(q, h, p, span, index(z, y, 1 - core), core_send.at[0], core_recv.at[q // 2, half_of(q, h, p)]).start()

    def arrive(q, h, p):
        await_bytes(rows.at[q, h, p], row_recv.at[q // 2, h, p])

    def arrive_core(q, half):
        await_bytes(rows.at[q, 0], core_recv.at[q // 2, half])

    def part_at(i):
        return lax.rem(part + i, groups)

    def send_own(h, p):
        mine = panel.at[h, piece_of(part, p)]
        send_side(me, h, p, mine)
        send_in(me, h, p, mine)

        @pl.when(jnp.logical_not(is_end))
        def _():
            send_out(me, h, p, mine)

        send_core(me, h, p, mine)
        rows[me, h, p] = panel[h, piece_of(part, p), :]

    for p in range(PIECES):
        scale_piece(part, p)
        send_own(part, p)
        scale_piece(other, p)
        panel_copy(other, p).start()
    for p in range(PIECES):
        panel_copy(part, p).start()
    for p in range(PIECES):
        await_bytes(panel.at[other, piece_of(part, p)], across_recv.at[p])
        send_own(other, p)

    def form(at_z, at_y, parts=None, wait=True):
        def per_core(t, carry):
            q = index(at_z, at_y, lax.rem(core + t, 2))
            if wait:
                @pl.when(t == 1)
                def _():
                    for half in (range(2) if parts is None else parts):
                        arrive_core(q, half)

            tiles[q] = product(rows, panel, q, range(groups) if parts is None else parts)
            return carry

        lax.fori_loop(0, 2, per_core, 0)

    def await_panel():
        await_bytes(panel.at[other, pl.ds(pl.multiple_of(other * tile_rows, tile_rows), tile_rows)], across_recv.at[PIECES])

    def pick(i, values):
        chosen = values[-1]
        for n in range(len(values) - 2, -1, -1):
            chosen = jnp.where(i == n, values[n], chosen)
        return chosen

    count = groups * PIECES

    @pl.when(is_end)
    def _():
        far_mid = depth - 1 - inward

        def first(t, carry):
            h, p = part_at(t // PIECES), lax.rem(t, PIECES)
            near, beside = index(inward, y, core), index(z, 1 - y, core)
            arrive(near, h, p)
            send_side(near, h, p)
            send_core(near, h, p)
            arrive(beside, h, p)
            send_in(beside, h, p)
            send_core(beside, h, p)
            return carry

        lax.fori_loop(0, count, first, 0)
        await_panel()

        def second(t, carry):
            h, p = part_at(t // PIECES), lax.rem(t, PIECES)
            far, cross = index(far_mid, y, core), index(inward, 1 - y, core)
            arrive(far, h, p)
            to = index(z, 1 - y, core)

            @pl.when(p == 0)
            def _():
                send_side(far, h, p, extra=1)

            @pl.when(p == 1)
            def _():
                span_copy(far, h, p, head, to, side_send.at[1], row_recv.at[far // 2, h, p]).start()

            @pl.when((p == 1) & (h == other))
            def _():
                span_copy(far, h, p, rest, to, side_send.at[1], code_sem.at[5]).start()

            send_core(far, h, p)
            arrive(cross, h, p)
            send_core(cross, h, p)

            @pl.when(t < 3)
            def _():
                form(pick(t, (z, inward, z)), pick(t, (y, y, 1 - y)))

            return carry

        lax.fori_loop(0, count, second, 0)

        def third(t, carry):
            h, p = part_at(t // PIECES), lax.rem(t, PIECES)
            q = index(far_mid, 1 - y, core)

            @pl.when(p == 0)
            def _():
                arrive(q, h, p)
                send_core(q, h, p)

            @pl.when(p == 1)
            def _():
                await_bytes(rows.at[q, h, p, head], row_recv.at[q // 2, h, p])
                send_core_span(q, h, p, head)

            @pl.when(t < 2)
            def _():
                form(pick(t, (far_mid, inward)), pick(t, (y, 1 - y)))

            @pl.when(t == 2)
            def _():
                await_bytes(rows.at[q, part, 1, rest], code_sem.at[4])
                send_core_span(q, part, 1, rest)

            @pl.when(t == 3)
            def _():
                await_bytes(rows.at[q, other, 1, rest], code_sem.at[5])
                send_core_span(q, other, 1, rest)

            return carry

        lax.fori_loop(0, count, third, 0)
        form(far_mid, 1 - y, [part])
        await_bytes(codes, code_sem.at[1])
        await_bytes(steps, code_sem.at[3])
        arrive_core(index(far_mid, 1 - y, 1 - core), other)
        await_bytes(rows.at[pl.ds(0, 2)], line_send.at[0])
        await_bytes(rows.at[pl.ds(0, 2)], side_send.at[0])
        await_bytes(geno_ref.at[pl.ds(0, (count * piece_rows - (piece_rows - cut)) // 2)], side_send.at[1])
        await_bytes(rows.at[pl.ds(0, 6)], core_send.at[0])

    @pl.when(jnp.logical_not(is_end))
    def _():
        far = depth - 1 - outward

        def first(t, carry):
            h, p = part_at(t // PIECES), lax.rem(t, PIECES)
            end, near, beside = index(outward, y, core), index(inward, y, core), index(z, 1 - y, core)
            arrive(end, h, p)

            @pl.when(p == 0)
            def _():
                send_in(end, h, 0)

            @pl.when(h == other)
            def _():
                send_in(end, jnp.where(p == 0, part, other), 1)

            send_core(end, h, p)
            column_copy(end, h, p).start()
            arrive(near, h, p)
            send_out(near, h, p)
            send_core(near, h, p)
            arrive(beside, h, p)
            send_core(beside, h, p)
            return carry

        lax.fori_loop(0, count, first, 0)
        for p in range(PIECES):
            send_in(index(z, 1 - y, core), part, p, extra=1)
        for h in range(groups):
            columns[part, h] = rows[index(outward, y, core), h].reshape(tile_rows, snp_count)
        await_panel()

        def make(side, p, k):
            def per_core(t, carry):
                which = lax.rem(core + t, 2)
                q = index(far, jnp.where(side == 0, y, 1 - y), which)
                term = None
                for h in range(groups):
                    one = lax.dot_general(rows[q, h, p], columns[k, h], (((1,), (1,)), ((), ())),
                                          preferred_element_type=jnp.float32)
                    term = one if term is None else term + one
                term = term * (1.0 / (groups * snp_count))
                top = jnp.max(jnp.abs(term), axis=0, keepdims=True)
                unit = ((side * 2 + which) * PIECES + p) * groups + k
                made[unit] = jnp.round(term * (CODE_TOP / jnp.maximum(top, TINY))).astype(jnp.int32).astype(jnp.int16)
                made_steps[unit] = top * (1.0 / CODE_TOP)
                for n, (source, target) in enumerate(((made, codes), (made_steps, steps))):
                    pltpu.make_async_remote_copy(
                        src_ref=source.at[unit], dst_ref=target.at[unit], send_sem=code_sem.at[2 * n],
                        recv_sem=code_sem.at[2 * n + 1], device_id={"samp": index(outward, y, core)},
                        device_id_type=MESH).start()
                return carry

            lax.fori_loop(0, 2, per_core, 0)

        def far_core(side, p):
            arrive_core(index(far, jnp.where(side == 0, y, 1 - y), 1 - core), p)

        def make_list(listed):
            def per_entry(i, carry):
                side, p, away = (pick(i, [entry[n] for entry in listed]) for n in range(3))
                make(side, p, lax.rem(part + away, groups))
                return carry

            lax.fori_loop(0, len(listed), per_entry, 0)

        def second(t, carry):
            h, p = part_at(lax.rem(t, groups)), t // groups
            far_q, cross = index(far, y, core), index(outward, 1 - y, core)

            @pl.when(t >= 2)
            def _():
                far_core(t - 2, 0)
                make(t - 2, 0, part)

            arrive(far_q, h, p)
            send_side(far_q, h, p)
            send_core(far_q, h, p)
            ch, cp = part_at(t // PIECES), lax.rem(t, PIECES)
            arrive(cross, ch, cp)
            send_core(cross, ch, cp)

            @pl.when(t > 0)
            def _():
                q = index(far, 1 - y, core)
                h, p = part_at(lax.rem(t - 1, groups)), (t - 1) // groups
                arrive(q, h, p)
                send_core(q, h, p)

            form(pick(t, (z, outward, inward, z)), pick(t, (y, y, y, 1 - y)))
            return carry

        lax.fori_loop(0, count, second, 0)
        for p in range(PIECES):
            send_side(index(inward, y, core), other, p, extra=1)
        far_core(0, 1)
        make_list([(0, 1, 0)])
        await_bytes(columns.at[other], across_recv.at[PIECES + 1])
        make_list([(0, 0, 1), (0, 1, 1), (1, 0, 1)])
        form(outward, 1 - y)
        q = index(far, 1 - y, core)
        arrive(q, other, PIECES - 1)
        send_core(q, other, PIECES - 1)
        cross = index(inward, 1 - y, core)

        def third(t, carry):
            h, p = part_at(t // PIECES), lax.rem(t, PIECES)
            arrive(cross, h, p)
            send_core(cross, h, p)

            @pl.when(t == 1)
            def _():
                span_copy(cross, h, p, rest, index(outward, y, core), line_send.at[3], code_sem.at[4]).start()
                far_core(1, 1)
                make_list([(1, 1, 0), (1, 1, 1)])

            @pl.when(t < 2)
            def _():
                form(far, pick(t, (y, 1 - y)), wait=False)

            return carry

        lax.fori_loop(0, count, third, 0)
        form(inward, 1 - y)
        await_bytes(rows.at[pl.ds(0, 2)], line_send.at[0])
        await_bytes(rows.at[0, 0], line_send.at[1])
        await_bytes(rows.at[pl.ds(0, 2)], line_send.at[2])
        await_bytes(geno_ref.at[pl.ds(0, (piece_rows - cut) // 2)], line_send.at[3])
        await_bytes(rows.at[pl.ds(0, 2)], side_send.at[0])
        await_bytes(rows.at[0, 0], side_send.at[1])
        await_bytes(rows.at[pl.ds(0, 8)], core_send.at[0])
        await_bytes(rows.at[0], across_send.at[1])
        await_bytes(made, code_sem.at[0])
        await_bytes(made_steps, code_sem.at[2])

    await_bytes(others, count_sem.at[0])
    await_bytes(rows.at[0], across_send.at[0])


def folded_body(shards, groups, genotypes, observed):
    row_count, snp_count = genotypes.shape
    tile_rows = row_count // groups
    piece_rows = tile_rows // PIECES
    units = 4 * PIECES * groups
    outs = (
        pltpu.VMEM((groups, row_count, snp_count), jnp.bfloat16),
        pltpu.VMEM((shards, groups, PIECES, piece_rows, snp_count), jnp.bfloat16),
        pltpu.VMEM((shards, tile_rows, row_count), jnp.float32),
        pltpu.VMEM((units, piece_rows, tile_rows), jnp.int16),
        pltpu.VMEM((units, 1, tile_rows), jnp.float32),
    )
    kept = sum(math.prod(o.shape) * jnp.dtype(o.dtype).itemsize for o in outs)
    held = pl.pallas_call(
        functools.partial(folded, shards, groups),
        out_shape=outs,
        in_specs=[pl.BlockSpec(memory_space=pltpu.HBM)] * 2,
        out_specs=[pl.BlockSpec(memory_space=pltpu.VMEM)] * 5,
        scratch_shapes=[
            pltpu.VMEM((row_count, snp_count), jnp.float32),
            pltpu.VMEM((row_count, snp_count), jnp.int32),
            pltpu.VMEM((shards, 2, snp_count), jnp.float32),
            pltpu.VMEM((groups, groups, tile_rows, snp_count), jnp.bfloat16),
            pltpu.VMEM((units, piece_rows, tile_rows), jnp.int16),
            pltpu.VMEM((units, 1, tile_rows), jnp.float32),
            pltpu.SemaphoreType.DMA((2, LOADS)),
            pltpu.SemaphoreType.DMA((2,)),
            pltpu.SemaphoreType.DMA((2,)),
            pltpu.SemaphoreType.DMA((PIECES + 2,)),
            pltpu.SemaphoreType.DMA((4,)),
            pltpu.SemaphoreType.DMA((2,)),
            pltpu.SemaphoreType.DMA((1,)),
            pltpu.SemaphoreType.DMA((shards // 2, groups, PIECES)),
            pltpu.SemaphoreType.DMA((shards // 2, 2)),
            pltpu.SemaphoreType.DMA((6,)),
        ],
        compiler_params=pltpu.CompilerParams(
            collective_id=0, has_side_effects=True, vmem_limit_bytes=VMEM_ALL - FOLDED_SPARE - kept),
    )(genotypes, observed)
    panel, rows, tiles, codes, steps = held
    return pl.pallas_call(
        functools.partial(folded_finish, shards, groups),
        out_shape=jax.ShapeDtypeStruct((shards, 1, tile_rows, row_count), jnp.float32),
        in_specs=[pl.BlockSpec(memory_space=pltpu.VMEM)] * 5,
        out_specs=pl.BlockSpec(memory_space=pltpu.HBM),
        scratch_shapes=[
            pltpu.VMEM((6, tile_rows, row_count), jnp.float32),
            pltpu.SemaphoreType.DMA((1,)),
        ],
        compiler_params=pltpu.CompilerParams(vmem_limit_bytes=FOLDED_FINISH),
    )(rows, panel, tiles, codes, steps)


def solution(mesh):
    shards, groups = mesh.shape["samp"], mesh.shape["snp"]

    def body(genotypes, observed):
        if groups == 2 and shards == 16:
            return folded_body(shards, groups, genotypes, observed)
        row_count, snp_count = genotypes.shape
        tile_rows = row_count // groups
        piece_rows = tile_rows // PIECES
        kept = 2 * (groups * row_count * snp_count) * (1 + shards // groups) + 4 * shards * tile_rows * row_count
        panel, rows, tiles = pl.pallas_call(
            functools.partial(kernel, shards, groups),
            out_shape=(
                pltpu.VMEM((groups, row_count, snp_count), jnp.bfloat16),
                pltpu.VMEM((shards, groups, PIECES, piece_rows, snp_count), jnp.bfloat16),
                pltpu.VMEM((shards, tile_rows, row_count), jnp.float32),
            ),
            in_specs=[pl.BlockSpec(memory_space=pltpu.HBM)] * 2,
            out_specs=[pl.BlockSpec(memory_space=pltpu.VMEM)] * 3,
            scratch_shapes=[
                pltpu.VMEM((row_count, snp_count), jnp.float32),
                pltpu.VMEM((row_count, snp_count), jnp.int32),
                pltpu.VMEM((shards, 2, snp_count), jnp.float32),
                pltpu.SemaphoreType.DMA((2, LOADS)),
                pltpu.SemaphoreType.DMA((shards,)),
                pltpu.SemaphoreType.DMA((shards,)),
                pltpu.SemaphoreType.DMA((groups, groups, PIECES)),
                pltpu.SemaphoreType.DMA((groups, groups, PIECES)),
                pltpu.SemaphoreType.DMA((4, shards, groups, PIECES)),
                pltpu.SemaphoreType.DMA((shards, groups, PIECES)),
            ],
            compiler_params=pltpu.CompilerParams(
                collective_id=0, has_side_effects=True, vmem_limit_bytes=VMEM_ALL - VMEM_SPARE - kept),
        )(genotypes, observed)
        return pl.pallas_call(
            functools.partial(finish, shards, groups),
            out_shape=jax.ShapeDtypeStruct((shards, 1, tile_rows, row_count), jnp.float32),
            in_specs=[pl.BlockSpec(memory_space=pltpu.VMEM)] * 3,
            out_specs=pl.BlockSpec(memory_space=pltpu.HBM),
            scratch_shapes=[
                pltpu.VMEM((4, tile_rows, row_count), jnp.float32),
                pltpu.SemaphoreType.DMA((shards,)),
            ],
            compiler_params=pltpu.CompilerParams(vmem_limit_bytes=VMEM_FINISH),
        )(rows, panel, tiles)

    return jax.shard_map(
        body,
        mesh=mesh,
        in_specs=(P("samp", "snp"), P("samp", "snp")),
        out_specs=P(None, "snp", None, "samp"),
        check_vma=False,
    )
```

```python
import functools
import math

import jax
import jax.numpy as jnp
from jax import lax
from jax.experimental import pallas as pl
from jax.experimental.pallas import tpu as pltpu
from jax.sharding import PartitionSpec as P

MESH = pl.DeviceIdType.MESH
var_floor = 0.1
UP, DOWN, SIDE, CORE = 0, 1, 2, 3
STRIP = 64
PIECES = 2
LOADS = 4
VMEM_ALL = 67043328
VMEM_SPARE = 512 * 1024
VMEM_FINISH = 12 * 1024 * 1024
FOLDED_SPARE = 1024 * 1024
FOLDED_FINISH = 8 * 1024 * 1024
CODE_TOP = 32767.0
TINY = 1e-30
RAW = 32


def index(at_z, at_y, at_core):
    return at_z * 4 + at_y * 2 + at_core


def source_at(z, depth, i):
    pairs = jnp.minimum(z, depth - 1 - z)
    side = jnp.where(i % 2 == 1, z - (i + 1) // 2, z + i // 2)
    far = jnp.where(z < depth - 1 - z, z + i - pairs, z - i + pairs)
    return jnp.where(i <= 2 * pairs, side, far)


def turned_at(z, depth):
    return jnp.where(z < depth - 1, z + 1, depth - 2)


def product(rows, panel, q, parts):
    pieces, piece_rows, snp_count = rows.shape[2:]
    total = None
    for h in parts:
        block = rows[q, h].reshape(pieces * piece_rows, snp_count)
        term = lax.dot_general(block, panel[h], (((1,), (1,)), ((), ())), preferred_element_type=jnp.float32)
        total = term if total is None else total + term
    return total * (1.0 / (rows.shape[1] * snp_count))


def finish(shards, groups, rows, panel, tiles, out_ref, late, out_sem):
    depth = shards // 4
    me = lax.axis_index("samp")
    z, y = me // 4, (me // 2) % 2
    turned = turned_at(z, depth)
    final = source_at(z, depth, depth - 1)
    final = jnp.where(final == turned, source_at(z, depth, depth - 2), final)
    last_part = lax.rem(lax.axis_index("snp") + groups - 1, groups)

    def is_late(q):
        return ((q // 4 == turned) | (q // 4 == final)) & ((q // 2) % 2 != y)

    def put(q, carry):
        @pl.when(jnp.logical_not(is_late(q)))
        def _():
            pltpu.make_async_copy(tiles.at[q], out_ref.at[q, 0], out_sem.at[q]).start()

        return carry

    lax.fori_loop(0, shards, put, 0)

    def form(i, carry):
        q = index(jnp.where(i // 2 == 0, final, turned), 1 - y, lax.rem(i, 2))
        late[i] = tiles[q] + product(rows, panel, q, [last_part])
        pltpu.make_async_copy(late.at[i], out_ref.at[q, 0], out_sem.at[q]).start()
        return carry

    lax.fori_loop(0, 4, form, 0)

    def flush(q, carry):
        pltpu.make_async_copy(tiles.at[q], out_ref.at[q, 0], out_sem.at[q]).wait()
        return carry

    lax.fori_loop(0, shards, flush, 0)


def kernel(shards, groups, geno_hbm, obs_hbm, panel, rows, tiles, geno_ref, obs_ref, counts, load_sem,
           count_send, count_recv, panel_send, panel_recv, row_send, row_recv):
    row_count, snp_count = geno_ref.shape
    tile_rows = row_count // groups
    piece_rows = tile_rows // PIECES
    depth = shards // 4
    me = lax.axis_index("samp")
    part = lax.axis_index("snp")
    z, y, core = me // 4, (me // 2) % 2, me % 2

    load_rows = row_count // LOADS

    def load(i):
        block = pl.ds(pl.multiple_of(i * load_rows, load_rows), load_rows)
        return (pltpu.make_async_copy(geno_hbm.at[block], geno_ref.at[block], load_sem.at[0, i]),
                pltpu.make_async_copy(obs_hbm.at[block], obs_ref.at[block], load_sem.at[1, i]))

    for i in range(LOADS):
        for copy in load(i):
            copy.start()

    barrier = pltpu.get_barrier_semaphore()
    for step in range(1, shards):
        pl.semaphore_signal(barrier, inc=1, device_id={"samp": lax.rem(me + step, shards)}, device_id_type=MESH)
    for step in range(1, groups):
        pl.semaphore_signal(barrier, inc=1, device_id={"snp": lax.rem(part + step, groups)}, device_id_type=MESH)

    def add_strip(i, total):
        alt, call = total
        strip = pl.ds(pl.multiple_of(i * STRIP, STRIP), STRIP)
        present = obs_ref[strip, :].astype(jnp.float32)
        held = present * geno_ref[strip, :]
        for r in range(0, STRIP, 8):
            alt = alt + held[r:r + 8]
            call = call + present[r:r + 8]
        return alt, call

    zero = jnp.zeros((8, snp_count), jnp.float32)
    alt, call = zero, zero
    strips = load_rows // STRIP
    for i in range(LOADS):
        for copy in load(i):
            copy.wait()
        alt, call = lax.fori_loop(i * strips, (i + 1) * strips, add_strip, (alt, call))
    counts[me, 0:1, :] = jnp.sum(alt, axis=0, keepdims=True)
    counts[me, 1:2, :] = jnp.sum(call, axis=0, keepdims=True)

    pl.semaphore_wait(barrier, shards + groups - 2)

    def count_copy(owner, to):
        return pltpu.make_async_remote_copy(
            src_ref=counts.at[owner], dst_ref=counts.at[owner], send_sem=count_send.at[to],
            recv_sem=count_recv.at[owner], device_id={"samp": to}, device_id_type=MESH)

    for step in range(1, shards):
        count_copy(me, lax.rem(me + step, shards)).start()
    for step in range(1, shards):
        other = lax.rem(me + step, shards)
        count_copy(other, other).wait_recv()
    sums = counts[0]
    for s in range(1, shards):
        sums = sums + counts[s]
    frequency = sums[0:1] / (2.0 * jnp.maximum(sums[1:2], 1.0))
    shift = 2.0 * frequency
    gain = lax.rsqrt(jnp.maximum(shift * (1.0 - frequency), var_floor))

    def piece_of(k, p):
        return pl.ds(pl.multiple_of(k * tile_rows + p * piece_rows, piece_rows), piece_rows)

    def panel_copy(h, k, to, p):
        block = panel.at[h, piece_of(k, p)]
        return pltpu.make_async_remote_copy(
            src_ref=block, dst_ref=block, send_sem=panel_send.at[to, k, p],
            recv_sem=panel_recv.at[h, k, p], device_id={"snp": to}, device_id_type=MESH)

    strip_rows = min(STRIP, piece_rows)

    def scale_piece(k, p):
        def scale_strip(i, carry):
            start = pl.multiple_of(k * tile_rows + p * piece_rows + i * strip_rows, strip_rows)
            strip = pl.ds(start, strip_rows)
            present = obs_ref[strip, :].astype(jnp.float32)
            panel[part, strip, :] = (present * (geno_ref[strip, :] - shift) * gain).astype(jnp.bfloat16)
            return carry

        lax.fori_loop(0, piece_rows // strip_rows, scale_strip, 0)

    def row_copy(q, h, p, way, src=None):
        to = (index(z + 1, y, core), index(z - 1, y, core), index(z, 1 - y, core), index(z, y, 1 - core))[way]
        return pltpu.make_async_remote_copy(
            src_ref=rows.at[q, h, p] if src is None else src, dst_ref=rows.at[q, h, p],
            send_sem=row_send.at[way, q, h, p], recv_sem=row_recv.at[q, h, p],
            device_id={"samp": to}, device_id_type=MESH)

    def arrive(q, h, p):
        row_copy(q, h, p, CORE).wait_recv()

    last_part = lax.rem(part + groups - 1, groups)
    turned = turned_at(z, depth)

    def part_at(i):
        return lax.rem(part + i, groups)

    def send_own(h, p):
        mine = panel.at[h, piece_of(part, p)]
        row_copy(me, h, p, SIDE, mine).start()

        @pl.when(z < depth - 1)
        def _():
            row_copy(me, h, p, UP, mine).start()

        @pl.when(z > 0)
        def _():
            row_copy(me, h, p, DOWN, mine).start()

        row_copy(me, h, p, CORE, mine).start()
        rows[me, h, p] = panel[h, piece_of(part, p), :]

    for p in range(PIECES):
        for step in range(1, groups):
            other = part_at(step)
            scale_piece(other, p)
            panel_copy(part, other, other, p).start()
        scale_piece(part, p)
        send_own(part, p)
    for step in range(1, groups):
        other = part_at(step)
        for k in range(1, groups):
            for p in range(PIECES):
                panel_copy(part, lax.rem(other + k, groups), other, p).start()
    for step in range(1, groups):
        h = part_at(step)
        for p in range(PIECES):
            panel_copy(h, part, h, p).wait_recv()
            send_own(h, p)

    def column_arrival(at_z, h, p, way):
        q = index(at_z, y, core)
        arrive(q, h, p)

        @pl.when(z < depth - 1 if way == UP else z > 0)
        def _():
            row_copy(q, h, p, way).start()

        @pl.when((at_z != turned) | (h != last_part))
        def _():
            row_copy(q, h, p, SIDE).start()

        row_copy(q, h, p, CORE).start()

    def column_arrivals(i):
        def per_piece(t, carry):
            h, p = part_at(t // PIECES), lax.rem(t, PIECES)

            @pl.when(z - i >= 0)
            def _():
                column_arrival(z - i, h, p, UP)

            @pl.when(z + i < depth)
            def _():
                column_arrival(z + i, h, p, DOWN)

            return carry

        lax.fori_loop(0, groups * PIECES, per_piece, 0)

    def arrive_all(q):
        def per_piece(t, carry):
            arrive(q, t // PIECES, lax.rem(t, PIECES))
            return carry

        lax.fori_loop(0, groups * PIECES, per_piece, 0)

    def products(at_z, at_y):
        def per_core(t, carry):
            q = index(at_z, at_y, lax.rem(core + t, 2))

            @pl.when(t == 1)
            def _():
                arrive_all(q)

            tiles[q] = product(rows, panel, q, range(groups))
            return carry

        lax.fori_loop(0, 2, per_core, 0)

    def side_arrival(at_z, h, p):
        q = index(at_z, 1 - y, core)
        arrive(q, h, p)
        row_copy(q, h, p, CORE).start()

    final = source_at(z, depth, depth - 1)
    final = jnp.where(final == turned, source_at(z, depth, depth - 2), final)

    def begin_late():
        def per_tile(t, carry):
            q = index(jnp.where(t % 2 == 0, turned, final), 1 - y, lax.rem(core + t // 2, 2))

            @pl.when(t >= 2)
            def _():
                for step in range(groups - 1):
                    for p in range(PIECES):
                        arrive(q, part_at(step), p)

            tiles[q] = product(rows, panel, q, [part_at(step) for step in range(groups - 1)])
            return carry

        lax.fori_loop(0, 4, per_tile, 0)

    def round_of(i, carry):
        @pl.when(i < depth)
        def _():
            column_arrivals(i)

        @pl.when(i == 1)
        def _():
            for step in range(1, groups):
                h = part_at(step)
                for k in range(1, groups):
                    for p in range(PIECES):
                        panel_copy(h, part_at(k), h, p).wait_recv()

        @pl.when(i == depth - 1)
        def _():
            q = index(z, 1 - y, core)

            @pl.when(z > 0)
            def _():
                for p in range(PIECES):
                    row_copy(q, last_part, p, DOWN).start()

            @pl.when(z == depth - 2)
            def _():
                for p in range(PIECES):
                    row_copy(q, last_part, p, UP).start()

        at_z = source_at(z, depth, i - 1)
        products(at_z, y)

        def per_piece(t, c):
            @pl.when((i == depth) & (t == (groups - 1) * PIECES))
            def _():
                begin_late()

            @pl.when((at_z != turned) | (t // PIECES != groups - 1))
            def _():
                side_arrival(at_z, part_at(t // PIECES), lax.rem(t, PIECES))

            return c

        lax.fori_loop(0, groups * PIECES, per_piece, 0)

        @pl.when((at_z != turned) & (at_z != final))
        def _():
            products(at_z, 1 - y)

        return carry

    lax.fori_loop(1, depth + 1, round_of, 0)
    for p in range(PIECES):
        side_arrival(turned, last_part, p)
    for p in range(PIECES):
        arrive(index(final, 1 - y, 1 - core), last_part, p)
        arrive(index(turned, 1 - y, 1 - core), last_part, p)

    for step in range(1, shards):
        count_copy(me, lax.rem(me + step, shards)).wait_send()
    for step in range(1, groups):
        for k in range(groups):
            for p in range(PIECES):
                panel_copy(part, k, part_at(step), p).wait_send()

    def drain(i, carry):
        at_z, h, p = i // (groups * PIECES), lax.rem(i // PIECES, groups), lax.rem(i, PIECES)
        q = index(at_z, y, core)
        across = index(at_z, 1 - y, core)

        @pl.when((at_z <= z) & (z < depth - 1))
        def _():
            row_copy(q, h, p, UP).wait_send()

        @pl.when((at_z >= z) & (z > 0))
        def _():
            row_copy(q, h, p, DOWN).wait_send()

        @pl.when((at_z != turned) | (h != last_part))
        def _():
            row_copy(q, h, p, SIDE).wait_send()

        row_copy(q, h, p, CORE).wait_send()
        row_copy(across, h, p, CORE).wait_send()

        @pl.when((at_z == z) & (h == last_part) & (z > 0))
        def _():
            row_copy(across, h, p, DOWN).wait_send()

        @pl.when((at_z == z) & (h == last_part) & (z == depth - 2))
        def _():
            row_copy(across, h, p, UP).wait_send()

        return carry

    lax.fori_loop(0, depth * groups * PIECES, drain, 0)


def shape_of_line(depth):
    z = lax.axis_index("samp") // 4
    low = z < depth // 2
    inward = jnp.where(low, z + 1, z - 1)
    outward = jnp.clip(jnp.where(low, z - 1, z + 1), 0, depth - 1)
    is_end = (z == 0) | (z == depth - 1)
    return z, inward, outward, is_end


def folded_finish(shards, groups, rows, panel, tiles, codes, steps, out_ref, late, out_sem):
    depth = shards // 4
    me = lax.axis_index("samp")
    y = (me // 2) % 2
    z, inward, outward, is_end = shape_of_line(depth)
    far_mid, far_end = depth - 1 - inward, depth - 1 - z
    last_part = lax.rem(lax.axis_index("snp") + groups - 1, groups)
    piece_rows = rows.shape[3]
    tile_rows = PIECES * piece_rows

    def is_late(q):
        return is_end & ((q // 4 == far_end) | ((q // 4 == far_mid) & ((q // 2) % 2 != y)))

    def put(q, carry):
        @pl.when(jnp.logical_not(is_late(q)))
        def _():
            pltpu.make_async_copy(tiles.at[q], out_ref.at[q, 0], out_sem.at[0]).start()

        return carry

    lax.fori_loop(0, shards, put, 0)

    @pl.when(is_end)
    def _():
        def decode(t, carry):
            for p in range(PIECES):
                for k in range(groups):
                    unit = (t * PIECES + p) * groups + k
                    late[t, p * piece_rows:(p + 1) * piece_rows, k * tile_rows:(k + 1) * tile_rows] = (
                        codes[unit].astype(jnp.float32) * steps[unit])
            q = index(far_end, jnp.where(t // 2 == 0, y, 1 - y), lax.rem(t, 2))
            pltpu.make_async_copy(late.at[t], out_ref.at[q, 0], out_sem.at[0]).start()
            return carry

        lax.fori_loop(0, 4, decode, 0)

        def form(i, carry):
            q = index(far_mid, 1 - y, i)
            late[4 + i] = tiles[q] + product(rows, panel, q, [last_part])
            pltpu.make_async_copy(late.at[4 + i], out_ref.at[q, 0], out_sem.at[0]).start()
            return carry

        lax.fori_loop(0, 2, form, 0)

    pltpu.make_async_copy(tiles, out_ref.at[:, 0], out_sem.at[0]).wait()


def folded(shards, groups, geno_hbm, obs_hbm, panel, rows, tiles, codes, steps, geno_ref, obs_ref, counts, columns,
           made, made_steps, raw, raw_in, load_sem, count_sem, across_send, across_recv, line_send, side_send, core_send, row_recv,
           core_recv, code_sem, raw_sem):
    row_count, snp_count = geno_ref.shape
    tile_rows = row_count // groups
    piece_rows = tile_rows // PIECES
    depth = shards // 4
    me = lax.axis_index("samp")
    part = lax.axis_index("snp")
    y, core = (me // 2) % 2, me % 2
    z, inward, outward, is_end = shape_of_line(depth)
    other = lax.rem(part + 1, groups)
    load_rows = row_count // LOADS

    def load(i):
        block = pl.ds(pl.multiple_of(i * load_rows, load_rows), load_rows)
        return (pltpu.make_async_copy(geno_hbm.at[block], geno_ref.at[block], load_sem.at[0, i]),
                pltpu.make_async_copy(obs_hbm.at[block], obs_ref.at[block], load_sem.at[1, i]))

    for i in range(LOADS):
        for copy in load(i):
            copy.start()

    barrier = pltpu.get_barrier_semaphore()
    for step in range(1, shards):
        pl.semaphore_signal(barrier, inc=1, device_id={"samp": lax.rem(me + step, shards)}, device_id_type=MESH)
    pl.semaphore_signal(barrier, inc=1, device_id={"snp": other}, device_id_type=MESH)

    def add_strip(i, total):
        alt, call = total
        strip = pl.ds(pl.multiple_of(i * STRIP, STRIP), STRIP)
        present = obs_ref[strip, :].astype(jnp.float32)
        held = present * geno_ref[strip, :]
        for r in range(0, STRIP, 8):
            alt = alt + held[r:r + 8]
            call = call + present[r:r + 8]
        return alt, call

    zero = jnp.zeros((8, snp_count), jnp.float32)
    alt, call = zero, zero
    strips = load_rows // STRIP
    for i in range(LOADS):
        for copy in load(i):
            copy.wait()
        alt, call = lax.fori_loop(i * strips, (i + 1) * strips, add_strip, (alt, call))
    alt_step = 2.0 * row_count / CODE_TOP
    both = jnp.concatenate([jnp.sum(alt, axis=0, keepdims=True) * (1.0 / alt_step), jnp.sum(call, axis=0, keepdims=True)])
    counts[me] = jnp.round(both).astype(jnp.int32).astype(jnp.int16)

    pl.semaphore_wait(barrier, shards)

    for step in range(shards):
        to = jnp.where(z < depth // 2, shards - 1 - step, step)

        @pl.when(to != me)
        def _():
            pltpu.make_async_remote_copy(
                src_ref=counts.at[me], dst_ref=counts.at[me], send_sem=count_sem.at[0], recv_sem=count_sem.at[1],
                device_id={"samp": to}, device_id_type=MESH).start()

    def await_bytes(ref, sem):
        pltpu.make_async_copy(ref, ref, sem).wait()

    def await_rows(count, sem):
        await_bytes(geno_ref.at[pl.ds(0, count // 2)], sem)

    def raw_copy(to, slot):
        return pltpu.make_async_remote_copy(
            src_ref=raw, dst_ref=raw_in.at[slot], send_sem=raw_sem.at[0], recv_sem=raw_sem.at[1 + slot],
            device_id={"samp": to}, device_id_type=MESH)

    early = pl.ds(pl.multiple_of(part * tile_rows, tile_rows), RAW)
    raw[...] = jnp.where(obs_ref[early, :] > 0, geno_ref[early, :], -1.0)
    raw_copy(index(z, 1 - y, core), 0).start()
    raw_copy(index(inward, y, core), jnp.where(is_end, 2, 1)).start()

    @pl.when(jnp.logical_not(is_end))
    def _():
        raw_copy(index(outward, y, core), 1).start()

    others = counts.at[pl.ds(0, shards - 1)]
    await_bytes(others, count_sem.at[1])
    sums = counts[0].astype(jnp.float32)
    for s in range(1, shards):
        sums = sums + counts[s].astype(jnp.float32)
    frequency = sums[0:1] * alt_step / (2.0 * jnp.maximum(sums[1:2], 1.0))
    shift = 2.0 * frequency
    gain = lax.rsqrt(jnp.maximum(shift * (1.0 - frequency), var_floor))

    def piece_of(k, p):
        return pl.ds(pl.multiple_of(k * tile_rows + p * piece_rows, piece_rows), piece_rows)

    strip_rows = min(STRIP, piece_rows)

    def scale_piece(k, p):
        def scale_strip(i, carry):
            start = pl.multiple_of(k * tile_rows + p * piece_rows + i * strip_rows, strip_rows)
            strip = pl.ds(start, strip_rows)
            present = obs_ref[strip, :].astype(jnp.float32)
            panel[part, strip, :] = (present * (geno_ref[strip, :] - shift) * gain).astype(jnp.bfloat16)
            return carry

        lax.fori_loop(0, piece_rows // strip_rows, scale_strip, 0)

    def panel_copy(k, p):
        block = panel.at[part, piece_of(k, p)]
        return pltpu.make_async_remote_copy(
            src_ref=block, dst_ref=block, send_sem=across_send.at[0],
            recv_sem=across_recv.at[jnp.where(k == part, PIECES, p)], device_id={"snp": other}, device_id_type=MESH)

    def column_copy(q, h, p):
        return pltpu.make_async_remote_copy(
            src_ref=rows.at[q, h, p], dst_ref=columns.at[part, h, pl.ds(pl.multiple_of(p * piece_rows, piece_rows), piece_rows)],
            send_sem=across_send.at[1], recv_sem=across_recv.at[PIECES + 1], device_id={"snp": other}, device_id_type=MESH)

    cut = piece_rows * 7 // 8
    head, rest = pl.ds(0, cut), pl.ds(cut, piece_rows - cut)

    def span_copy(q, h, p, span, to, send_sem, recv_sem):
        return pltpu.make_async_remote_copy(
            src_ref=rows.at[q, h, p, span], dst_ref=rows.at[q, h, p, span], send_sem=send_sem, recv_sem=recv_sem,
            device_id={"samp": to}, device_id_type=MESH)

    def own_copy(q, h, p, to, send_sem, src=None, dst=None):
        return pltpu.make_async_remote_copy(
            src_ref=rows.at[q, h, p] if src is None else src, dst_ref=rows.at[q, h, p] if dst is None else dst,
            send_sem=send_sem,
            recv_sem=row_recv.at[q // 2, h, p], device_id={"samp": to}, device_id_type=MESH)

    def send_in(q, h, p, extra=0):
        own_copy(q, h, p, index(inward, y, core), line_send.at[extra]).start()

    def send_out(q, h, p):
        own_copy(q, h, p, index(outward, y, core), line_send.at[2]).start()

    def send_side(q, h, p, extra=0):
        own_copy(q, h, p, index(z, 1 - y, core), side_send.at[extra]).start()

    def half_of(q, h, p):
        return jnp.where(jnp.logical_not(is_end) & (q // 4 == depth - 1 - outward), p, h)

    def send_core(q, h, p, src=None):
        pltpu.make_async_remote_copy(
            src_ref=rows.at[q, h, p] if src is None else src, dst_ref=rows.at[q, h, p], send_sem=core_send.at[0],
            recv_sem=core_recv.at[q // 2, half_of(q, h, p)], device_id={"samp": index(z, y, 1 - core)},
            device_id_type=MESH).start()

    def send_core_span(q, h, p, span):
        span_copy(q, h, p, span, index(z, y, 1 - core), core_send.at[0], core_recv.at[q // 2, half_of(q, h, p)]).start()

    def arrive(q, h, p):
        await_bytes(rows.at[q, h, p], row_recv.at[q // 2, h, p])

    def arrive_core(q, half):
        await_bytes(rows.at[q, 0], core_recv.at[q // 2, half])

    def part_at(i):
        return lax.rem(part + i, groups)

    def send_own(h, p, skip=0):
        mine = panel.at[h, piece_of(part, p)]
        kept = panel.at[h, pl.ds(pl.multiple_of(part * tile_rows + p * piece_rows + skip, 16), piece_rows - skip)]
        kept_to = rows.at[me, h, p, pl.ds(skip, piece_rows - skip)]
        own_copy(me, h, p, index(z, 1 - y, core), side_send.at[0], kept, kept_to).start()
        own_copy(me, h, p, index(inward, y, core), line_send.at[0], kept, kept_to).start()

        @pl.when(jnp.logical_not(is_end))
        def _():
            own_copy(me, h, p, index(outward, y, core), line_send.at[2], kept, kept_to).start()

        send_core(me, h, p, mine)
        rows[me, h, p] = panel[h, piece_of(part, p), :]

    def scale_raw(slot, q):
        await_bytes(raw_in.at[slot], raw_sem.at[1 + slot])
        sent = raw_in[slot]
        rows[q, part, 0, 0:RAW, :] = jnp.where(sent >= 0.0, (sent - shift) * gain, 0.0).astype(jnp.bfloat16)

    def arrive_near(q, h, p):
        @pl.when((h == part) & (p == 0))
        def _():
            await_bytes(rows.at[q, h, p, pl.ds(RAW, piece_rows - RAW)], row_recv.at[q // 2, h, p])

        @pl.when((h != part) | (p != 0))
        def _():
            arrive(q, h, p)

    for p in range(PIECES):
        scale_piece(part, p)
        send_own(part, p, 0 if p else RAW)
        scale_piece(other, p)
        panel_copy(other, p).start()
    for p in range(PIECES):
        panel_copy(part, p).start()
    scale_raw(0, index(z, 1 - y, core))
    scale_raw(1, index(inward, y, core))

    @pl.when(jnp.logical_not(is_end))
    def _():
        scale_raw(2, index(outward, y, core))

    for p in range(PIECES):
        await_bytes(panel.at[other, piece_of(part, p)], across_recv.at[p])
        send_own(other, p)

    def form(at_z, at_y, parts=None, wait=True):
        def per_core(t, carry):
            q = index(at_z, at_y, lax.rem(core + t, 2))
            if wait:
                @pl.when(t == 1)
                def _():
                    for half in (range(2) if parts is None else parts):
                        arrive_core(q, half)

            tiles[q] = product(rows, panel, q, range(groups) if parts is None else parts)
            return carry

        lax.fori_loop(0, 2, per_core, 0)

    def await_panel():
        await_bytes(panel.at[other, pl.ds(pl.multiple_of(other * tile_rows, tile_rows), tile_rows)], across_recv.at[PIECES])

    def pick(i, values):
        chosen = values[-1]
        for n in range(len(values) - 2, -1, -1):
            chosen = jnp.where(i == n, values[n], chosen)
        return chosen

    count = groups * PIECES

    @pl.when(is_end)
    def _():
        far_mid = depth - 1 - inward

        def first(t, carry):
            h, p = part_at(t // PIECES), lax.rem(t, PIECES)
            near, beside = index(inward, y, core), index(z, 1 - y, core)
            arrive_near(near, h, p)
            send_side(near, h, p)
            send_core(near, h, p)
            arrive_near(beside, h, p)
            send_in(beside, h, p)
            send_core(beside, h, p)
            return carry

        lax.fori_loop(0, count, first, 0)
        await_panel()

        def second(t, carry):
            h, p = part_at(t // PIECES), lax.rem(t, PIECES)
            far, cross = index(far_mid, y, core), index(inward, 1 - y, core)
            arrive(far, h, p)
            to = index(z, 1 - y, core)

            @pl.when(p == 0)
            def _():
                send_side(far, h, p, extra=1)

            @pl.when(p == 1)
            def _():
                span_copy(far, h, p, head, to, side_send.at[1], row_recv.at[far // 2, h, p]).start()

            @pl.when((p == 1) & (h == other))
            def _():
                span_copy(far, h, p, rest, to, side_send.at[1], code_sem.at[5]).start()

            send_core(far, h, p)
            arrive(cross, h, p)
            send_core(cross, h, p)

            @pl.when(t < 3)
            def _():
                form(pick(t, (z, inward, z)), pick(t, (y, y, 1 - y)))

            return carry

        lax.fori_loop(0, count, second, 0)

        def third(t, carry):
            h, p = part_at(t // PIECES), lax.rem(t, PIECES)
            q = index(far_mid, 1 - y, core)

            @pl.when(p == 0)
            def _():
                arrive(q, h, p)
                send_core(q, h, p)

            @pl.when(p == 1)
            def _():
                await_bytes(rows.at[q, h, p, head], row_recv.at[q // 2, h, p])
                send_core_span(q, h, p, head)

            @pl.when(t < 2)
            def _():
                form(pick(t, (far_mid, inward)), pick(t, (y, 1 - y)))

            @pl.when(t == 2)
            def _():
                await_bytes(rows.at[q, part, 1, rest], code_sem.at[4])
                send_core_span(q, part, 1, rest)

            @pl.when(t == 3)
            def _():
                await_bytes(rows.at[q, other, 1, rest], code_sem.at[5])
                send_core_span(q, other, 1, rest)

            return carry

        lax.fori_loop(0, count, third, 0)
        form(far_mid, 1 - y, [part])
        await_bytes(codes, code_sem.at[1])
        await_bytes(steps, code_sem.at[3])
        arrive_core(index(far_mid, 1 - y, 1 - core), other)
        await_rows(2 * row_count - RAW, line_send.at[0])
        await_rows(2 * row_count - RAW, side_send.at[0])
        await_rows(count * piece_rows - (piece_rows - cut), side_send.at[1])
        await_bytes(raw_in.at[pl.ds(0, 2)], raw_sem.at[0])
        await_bytes(rows.at[pl.ds(0, 6)], core_send.at[0])

    @pl.when(jnp.logical_not(is_end))
    def _():
        far = depth - 1 - outward

        def first(t, carry):
            h, p = part_at(t // PIECES), lax.rem(t, PIECES)
            end, near, beside = index(outward, y, core), index(inward, y, core), index(z, 1 - y, core)
            arrive_near(end, h, p)

            @pl.when(p == 0)
            def _():
                send_in(end, h, 0)

            @pl.when(h == other)
            def _():
                send_in(end, jnp.where(p == 0, part, other), 1)

            send_core(end, h, p)
            column_copy(end, h, p).start()
            arrive_near(near, h, p)
            send_out(near, h, p)
            send_core(near, h, p)
            arrive_near(beside, h, p)
            send_core(beside, h, p)
            return carry

        lax.fori_loop(0, count, first, 0)
        for p in range(PIECES):
            send_in(index(z, 1 - y, core), part, p, extra=1)
        for h in range(groups):
            columns[part, h] = rows[index(outward, y, core), h].reshape(tile_rows, snp_count)
        await_panel()

        def make(side, p, k):
            def per_core(t, carry):
                which = lax.rem(core + t, 2)
                q = index(far, jnp.where(side == 0, y, 1 - y), which)
                term = None
                for h in range(groups):
                    one = lax.dot_general(rows[q, h, p], columns[k, h], (((1,), (1,)), ((), ())),
                                          preferred_element_type=jnp.float32)
                    term = one if term is None else term + one
                term = term * (1.0 / (groups * snp_count))
                top = jnp.max(jnp.abs(term), axis=0, keepdims=True)
                unit = ((side * 2 + which) * PIECES + p) * groups + k
                made[unit] = jnp.round(term * (CODE_TOP / jnp.maximum(top, TINY))).astype(jnp.int32).astype(jnp.int16)
                made_steps[unit] = top * (1.0 / CODE_TOP)
                for n, (source, target) in enumerate(((made, codes), (made_steps, steps))):
                    pltpu.make_async_remote_copy(
                        src_ref=source.at[unit], dst_ref=target.at[unit], send_sem=code_sem.at[2 * n],
                        recv_sem=code_sem.at[2 * n + 1], device_id={"samp": index(outward, y, core)},
                        device_id_type=MESH).start()
                return carry

            lax.fori_loop(0, 2, per_core, 0)

        def far_core(side, p):
            arrive_core(index(far, jnp.where(side == 0, y, 1 - y), 1 - core), p)

        def make_list(listed):
            def per_entry(i, carry):
                side, p, away = (pick(i, [entry[n] for entry in listed]) for n in range(3))
                make(side, p, lax.rem(part + away, groups))
                return carry

            lax.fori_loop(0, len(listed), per_entry, 0)

        def second(t, carry):
            h, p = part_at(lax.rem(t, groups)), t // groups
            far_q, cross = index(far, y, core), index(outward, 1 - y, core)

            @pl.when(t >= 2)
            def _():
                far_core(t - 2, 0)
                make(t - 2, 0, part)

            arrive(far_q, h, p)
            send_side(far_q, h, p)
            send_core(far_q, h, p)
            ch, cp = part_at(t // PIECES), lax.rem(t, PIECES)
            arrive(cross, ch, cp)
            send_core(cross, ch, cp)

            @pl.when(t > 0)
            def _():
                q = index(far, 1 - y, core)
                h, p = part_at(lax.rem(t - 1, groups)), (t - 1) // groups
                arrive(q, h, p)
                send_core(q, h, p)

            form(pick(t, (z, outward, inward, z)), pick(t, (y, y, y, 1 - y)))
            return carry

        lax.fori_loop(0, count, second, 0)
        for p in range(PIECES):
            send_side(index(inward, y, core), other, p, extra=1)
        far_core(0, 1)
        make_list([(0, 1, 0)])
        await_bytes(columns.at[other], across_recv.at[PIECES + 1])
        make_list([(0, 0, 1), (0, 1, 1), (1, 0, 1)])
        form(outward, 1 - y)
        q = index(far, 1 - y, core)
        arrive(q, other, PIECES - 1)
        send_core(q, other, PIECES - 1)
        cross = index(inward, 1 - y, core)

        def third(t, carry):
            h, p = part_at(t // PIECES), lax.rem(t, PIECES)
            arrive(cross, h, p)
            send_core(cross, h, p)

            @pl.when(t == 1)
            def _():
                span_copy(cross, h, p, rest, index(outward, y, core), line_send.at[3], code_sem.at[4]).start()
                far_core(1, 1)
                make_list([(1, 1, 0), (1, 1, 1)])

            @pl.when(t < 2)
            def _():
                form(far, pick(t, (y, 1 - y)), wait=False)

            return carry

        lax.fori_loop(0, count, third, 0)
        form(inward, 1 - y)
        await_rows(2 * row_count - RAW, line_send.at[0])
        await_bytes(rows.at[0, 0], line_send.at[1])
        await_rows(2 * row_count - RAW, line_send.at[2])
        await_bytes(raw_in, raw_sem.at[0])
        await_rows(piece_rows - cut, line_send.at[3])
        await_rows(2 * row_count - RAW, side_send.at[0])
        await_bytes(rows.at[0, 0], side_send.at[1])
        await_bytes(rows.at[pl.ds(0, 8)], core_send.at[0])
        await_bytes(rows.at[0], across_send.at[1])
        await_bytes(made, code_sem.at[0])
        await_bytes(made_steps, code_sem.at[2])

    await_bytes(others, count_sem.at[0])
    await_bytes(rows.at[0], across_send.at[0])


def folded_body(shards, groups, genotypes, observed):
    row_count, snp_count = genotypes.shape
    tile_rows = row_count // groups
    piece_rows = tile_rows // PIECES
    units = 4 * PIECES * groups
    outs = (
        pltpu.VMEM((groups, row_count, snp_count), jnp.bfloat16),
        pltpu.VMEM((shards, groups, PIECES, piece_rows, snp_count), jnp.bfloat16),
        pltpu.VMEM((shards, tile_rows, row_count), jnp.float32),
        pltpu.VMEM((units, piece_rows, tile_rows), jnp.int16),
        pltpu.VMEM((units, 1, tile_rows), jnp.float32),
    )
    kept = sum(math.prod(o.shape) * jnp.dtype(o.dtype).itemsize for o in outs)
    held = pl.pallas_call(
        functools.partial(folded, shards, groups),
        out_shape=outs,
        in_specs=[pl.BlockSpec(memory_space=pltpu.HBM)] * 2,
        out_specs=[pl.BlockSpec(memory_space=pltpu.VMEM)] * 5,
        scratch_shapes=[
            pltpu.VMEM((row_count, snp_count), jnp.float32),
            pltpu.VMEM((row_count, snp_count), jnp.int32),
            pltpu.VMEM((shards, 2, snp_count), jnp.int16),
            pltpu.VMEM((groups, groups, tile_rows, snp_count), jnp.bfloat16),
            pltpu.VMEM((units, piece_rows, tile_rows), jnp.int16),
            pltpu.VMEM((units, 1, tile_rows), jnp.float32),
            pltpu.VMEM((RAW, snp_count), jnp.float32),
            pltpu.VMEM((3, RAW, snp_count), jnp.float32),
            pltpu.SemaphoreType.DMA((2, LOADS)),
            pltpu.SemaphoreType.DMA((2,)),
            pltpu.SemaphoreType.DMA((2,)),
            pltpu.SemaphoreType.DMA((PIECES + 2,)),
            pltpu.SemaphoreType.DMA((4,)),
            pltpu.SemaphoreType.DMA((2,)),
            pltpu.SemaphoreType.DMA((1,)),
            pltpu.SemaphoreType.DMA((shards // 2, groups, PIECES)),
            pltpu.SemaphoreType.DMA((shards // 2, 2)),
            pltpu.SemaphoreType.DMA((6,)),
            pltpu.SemaphoreType.DMA((4,)),
        ],
        compiler_params=pltpu.CompilerParams(
            collective_id=0, has_side_effects=True, vmem_limit_bytes=VMEM_ALL - FOLDED_SPARE - kept),
    )(genotypes, observed)
    panel, rows, tiles, codes, steps = held
    return pl.pallas_call(
        functools.partial(folded_finish, shards, groups),
        out_shape=jax.ShapeDtypeStruct((shards, 1, tile_rows, row_count), jnp.float32),
        in_specs=[pl.BlockSpec(memory_space=pltpu.VMEM)] * 5,
        out_specs=pl.BlockSpec(memory_space=pltpu.HBM),
        scratch_shapes=[
            pltpu.VMEM((6, tile_rows, row_count), jnp.float32),
            pltpu.SemaphoreType.DMA((1,)),
        ],
        compiler_params=pltpu.CompilerParams(vmem_limit_bytes=FOLDED_FINISH),
    )(rows, panel, tiles, codes, steps)


def solution(mesh):
    shards, groups = mesh.shape["samp"], mesh.shape["snp"]

    def body(genotypes, observed):
        if groups == 2 and shards == 16:
            return folded_body(shards, groups, genotypes, observed)
        row_count, snp_count = genotypes.shape
        tile_rows = row_count // groups
        piece_rows = tile_rows // PIECES
        kept = 2 * (groups * row_count * snp_count) * (1 + shards // groups) + 4 * shards * tile_rows * row_count
        panel, rows, tiles = pl.pallas_call(
            functools.partial(kernel, shards, groups),
            out_shape=(
                pltpu.VMEM((groups, row_count, snp_count), jnp.bfloat16),
                pltpu.VMEM((shards, groups, PIECES, piece_rows, snp_count), jnp.bfloat16),
                pltpu.VMEM((shards, tile_rows, row_count), jnp.float32),
            ),
            in_specs=[pl.BlockSpec(memory_space=pltpu.HBM)] * 2,
            out_specs=[pl.BlockSpec(memory_space=pltpu.VMEM)] * 3,
            scratch_shapes=[
                pltpu.VMEM((row_count, snp_count), jnp.float32),
                pltpu.VMEM((row_count, snp_count), jnp.int32),
                pltpu.VMEM((shards, 2, snp_count), jnp.float32),
                pltpu.SemaphoreType.DMA((2, LOADS)),
                pltpu.SemaphoreType.DMA((shards,)),
                pltpu.SemaphoreType.DMA((shards,)),
                pltpu.SemaphoreType.DMA((groups, groups, PIECES)),
                pltpu.SemaphoreType.DMA((groups, groups, PIECES)),
                pltpu.SemaphoreType.DMA((4, shards, groups, PIECES)),
                pltpu.SemaphoreType.DMA((shards, groups, PIECES)),
            ],
            compiler_params=pltpu.CompilerParams(
                collective_id=0, has_side_effects=True, vmem_limit_bytes=VMEM_ALL - VMEM_SPARE - kept),
        )(genotypes, observed)
        return pl.pallas_call(
            functools.partial(finish, shards, groups),
            out_shape=jax.ShapeDtypeStruct((shards, 1, tile_rows, row_count), jnp.float32),
            in_specs=[pl.BlockSpec(memory_space=pltpu.VMEM)] * 3,
            out_specs=pl.BlockSpec(memory_space=pltpu.HBM),
            scratch_shapes=[
                pltpu.VMEM((4, tile_rows, row_count), jnp.float32),
                pltpu.SemaphoreType.DMA((shards,)),
            ],
            compiler_params=pltpu.CompilerParams(vmem_limit_bytes=VMEM_FINISH),
        )(rows, panel, tiles)

    return jax.shard_map(
        body,
        mesh=mesh,
        in_specs=(P("samp", "snp"), P("samp", "snp")),
        out_specs=P(None, "snp", None, "samp"),
        check_vma=False,
    )
```

```python
import functools
import math

import jax
import jax.numpy as jnp
from jax import lax
from jax.experimental import pallas as pl
from jax.experimental.pallas import tpu as pltpu
from jax.sharding import PartitionSpec as P

MESH = pl.DeviceIdType.MESH
var_floor = 0.1
UP, DOWN, SIDE, CORE = 0, 1, 2, 3
STRIP = 64
PIECES = 2
LOADS = 4
VMEM_ALL = 67043328
VMEM_SPARE = 512 * 1024
VMEM_FINISH = 12 * 1024 * 1024
FOLDED_SPARE = 1024 * 1024
FOLDED_FINISH = 8 * 1024 * 1024
CODE_TOP = 32767.0
TINY = 1e-30
RAW = 32


def index(at_z, at_y, at_core):
    return at_z * 4 + at_y * 2 + at_core


def source_at(z, depth, i):
    pairs = jnp.minimum(z, depth - 1 - z)
    side = jnp.where(i % 2 == 1, z - (i + 1) // 2, z + i // 2)
    far = jnp.where(z < depth - 1 - z, z + i - pairs, z - i + pairs)
    return jnp.where(i <= 2 * pairs, side, far)


def turned_at(z, depth):
    return jnp.where(z < depth - 1, z + 1, depth - 2)


def product(rows, panel, q, parts):
    pieces, piece_rows, snp_count = rows.shape[2:]
    total = None
    for h in parts:
        block = rows[q, h].reshape(pieces * piece_rows, snp_count)
        term = lax.dot_general(block, panel[h], (((1,), (1,)), ((), ())), preferred_element_type=jnp.float32)
        total = term if total is None else total + term
    return total * (1.0 / (rows.shape[1] * snp_count))


def finish(shards, groups, rows, panel, tiles, out_ref, late, out_sem):
    depth = shards // 4
    me = lax.axis_index("samp")
    z, y = me // 4, (me // 2) % 2
    turned = turned_at(z, depth)
    final = source_at(z, depth, depth - 1)
    final = jnp.where(final == turned, source_at(z, depth, depth - 2), final)
    last_part = lax.rem(lax.axis_index("snp") + groups - 1, groups)

    def is_late(q):
        return ((q // 4 == turned) | (q // 4 == final)) & ((q // 2) % 2 != y)

    def put(q, carry):
        @pl.when(jnp.logical_not(is_late(q)))
        def _():
            pltpu.make_async_copy(tiles.at[q], out_ref.at[q, 0], out_sem.at[q]).start()

        return carry

    lax.fori_loop(0, shards, put, 0)

    def form(i, carry):
        q = index(jnp.where(i // 2 == 0, final, turned), 1 - y, lax.rem(i, 2))
        late[i] = tiles[q] + product(rows, panel, q, [last_part])
        pltpu.make_async_copy(late.at[i], out_ref.at[q, 0], out_sem.at[q]).start()
        return carry

    lax.fori_loop(0, 4, form, 0)

    def flush(q, carry):
        pltpu.make_async_copy(tiles.at[q], out_ref.at[q, 0], out_sem.at[q]).wait()
        return carry

    lax.fori_loop(0, shards, flush, 0)


def kernel(shards, groups, geno_hbm, obs_hbm, panel, rows, tiles, geno_ref, obs_ref, counts, load_sem,
           count_send, count_recv, panel_send, panel_recv, row_send, row_recv):
    row_count, snp_count = geno_ref.shape
    tile_rows = row_count // groups
    piece_rows = tile_rows // PIECES
    depth = shards // 4
    me = lax.axis_index("samp")
    part = lax.axis_index("snp")
    z, y, core = me // 4, (me // 2) % 2, me % 2

    load_rows = row_count // LOADS

    def load(i):
        block = pl.ds(pl.multiple_of(i * load_rows, load_rows), load_rows)
        return (pltpu.make_async_copy(geno_hbm.at[block], geno_ref.at[block], load_sem.at[0, i]),
                pltpu.make_async_copy(obs_hbm.at[block], obs_ref.at[block], load_sem.at[1, i]))

    for i in range(LOADS):
        for copy in load(i):
            copy.start()

    barrier = pltpu.get_barrier_semaphore()
    for step in range(1, shards):
        pl.semaphore_signal(barrier, inc=1, device_id={"samp": lax.rem(me + step, shards)}, device_id_type=MESH)
    for step in range(1, groups):
        pl.semaphore_signal(barrier, inc=1, device_id={"snp": lax.rem(part + step, groups)}, device_id_type=MESH)

    def add_strip(i, total):
        alt, call = total
        strip = pl.ds(pl.multiple_of(i * STRIP, STRIP), STRIP)
        present = obs_ref[strip, :].astype(jnp.float32)
        held = present * geno_ref[strip, :]
        for r in range(0, STRIP, 8):
            alt = alt + held[r:r + 8]
            call = call + present[r:r + 8]
        return alt, call

    zero = jnp.zeros((8, snp_count), jnp.float32)
    alt, call = zero, zero
    strips = load_rows // STRIP
    for i in range(LOADS):
        for copy in load(i):
            copy.wait()
        alt, call = lax.fori_loop(i * strips, (i + 1) * strips, add_strip, (alt, call))
    counts[me, 0:1, :] = jnp.sum(alt, axis=0, keepdims=True)
    counts[me, 1:2, :] = jnp.sum(call, axis=0, keepdims=True)

    pl.semaphore_wait(barrier, shards + groups - 2)

    def count_copy(owner, to):
        return pltpu.make_async_remote_copy(
            src_ref=counts.at[owner], dst_ref=counts.at[owner], send_sem=count_send.at[to],
            recv_sem=count_recv.at[owner], device_id={"samp": to}, device_id_type=MESH)

    for step in range(1, shards):
        count_copy(me, lax.rem(me + step, shards)).start()
    for step in range(1, shards):
        other = lax.rem(me + step, shards)
        count_copy(other, other).wait_recv()
    sums = counts[0]
    for s in range(1, shards):
        sums = sums + counts[s]
    frequency = sums[0:1] / (2.0 * jnp.maximum(sums[1:2], 1.0))
    shift = 2.0 * frequency
    gain = lax.rsqrt(jnp.maximum(shift * (1.0 - frequency), var_floor))

    def piece_of(k, p):
        return pl.ds(pl.multiple_of(k * tile_rows + p * piece_rows, piece_rows), piece_rows)

    def panel_copy(h, k, to, p):
        block = panel.at[h, piece_of(k, p)]
        return pltpu.make_async_remote_copy(
            src_ref=block, dst_ref=block, send_sem=panel_send.at[to, k, p],
            recv_sem=panel_recv.at[h, k, p], device_id={"snp": to}, device_id_type=MESH)

    strip_rows = min(STRIP, piece_rows)

    def scale_piece(k, p):
        def scale_strip(i, carry):
            start = pl.multiple_of(k * tile_rows + p * piece_rows + i * strip_rows, strip_rows)
            strip = pl.ds(start, strip_rows)
            present = obs_ref[strip, :].astype(jnp.float32)
            panel[part, strip, :] = (present * (geno_ref[strip, :] - shift) * gain).astype(jnp.bfloat16)
            return carry

        lax.fori_loop(0, piece_rows // strip_rows, scale_strip, 0)

    def row_copy(q, h, p, way, src=None):
        to = (index(z + 1, y, core), index(z - 1, y, core), index(z, 1 - y, core), index(z, y, 1 - core))[way]
        return pltpu.make_async_remote_copy(
            src_ref=rows.at[q, h, p] if src is None else src, dst_ref=rows.at[q, h, p],
            send_sem=row_send.at[way, q, h, p], recv_sem=row_recv.at[q, h, p],
            device_id={"samp": to}, device_id_type=MESH)

    def arrive(q, h, p):
        row_copy(q, h, p, CORE).wait_recv()

    last_part = lax.rem(part + groups - 1, groups)
    turned = turned_at(z, depth)

    def part_at(i):
        return lax.rem(part + i, groups)

    def send_own(h, p):
        mine = panel.at[h, piece_of(part, p)]
        row_copy(me, h, p, SIDE, mine).start()

        @pl.when(z < depth - 1)
        def _():
            row_copy(me, h, p, UP, mine).start()

        @pl.when(z > 0)
        def _():
            row_copy(me, h, p, DOWN, mine).start()

        row_copy(me, h, p, CORE, mine).start()
        rows[me, h, p] = panel[h, piece_of(part, p), :]

    for p in range(PIECES):
        for step in range(1, groups):
            other = part_at(step)
            scale_piece(other, p)
            panel_copy(part, other, other, p).start()
        scale_piece(part, p)
        send_own(part, p)
    for step in range(1, groups):
        other = part_at(step)
        for k in range(1, groups):
            for p in range(PIECES):
                panel_copy(part, lax.rem(other + k, groups), other, p).start()
    for step in range(1, groups):
        h = part_at(step)
        for p in range(PIECES):
            panel_copy(h, part, h, p).wait_recv()
            send_own(h, p)

    def column_arrival(at_z, h, p, way):
        q = index(at_z, y, core)
        arrive(q, h, p)

        @pl.when(z < depth - 1 if way == UP else z > 0)
        def _():
            row_copy(q, h, p, way).start()

        @pl.when((at_z != turned) | (h != last_part))
        def _():
            row_copy(q, h, p, SIDE).start()

        row_copy(q, h, p, CORE).start()

    def column_arrivals(i):
        def per_piece(t, carry):
            h, p = part_at(t // PIECES), lax.rem(t, PIECES)

            @pl.when(z - i >= 0)
            def _():
                column_arrival(z - i, h, p, UP)

            @pl.when(z + i < depth)
            def _():
                column_arrival(z + i, h, p, DOWN)

            return carry

        lax.fori_loop(0, groups * PIECES, per_piece, 0)

    def arrive_all(q):
        def per_piece(t, carry):
            arrive(q, t // PIECES, lax.rem(t, PIECES))
            return carry

        lax.fori_loop(0, groups * PIECES, per_piece, 0)

    def products(at_z, at_y):
        def per_core(t, carry):
            q = index(at_z, at_y, lax.rem(core + t, 2))

            @pl.when(t == 1)
            def _():
                arrive_all(q)

            tiles[q] = product(rows, panel, q, range(groups))
            return carry

        lax.fori_loop(0, 2, per_core, 0)

    def side_arrival(at_z, h, p):
        q = index(at_z, 1 - y, core)
        arrive(q, h, p)
        row_copy(q, h, p, CORE).start()

    final = source_at(z, depth, depth - 1)
    final = jnp.where(final == turned, source_at(z, depth, depth - 2), final)

    def begin_late():
        def per_tile(t, carry):
            q = index(jnp.where(t % 2 == 0, turned, final), 1 - y, lax.rem(core + t // 2, 2))

            @pl.when(t >= 2)
            def _():
                for step in range(groups - 1):
                    for p in range(PIECES):
                        arrive(q, part_at(step), p)

            tiles[q] = product(rows, panel, q, [part_at(step) for step in range(groups - 1)])
            return carry

        lax.fori_loop(0, 4, per_tile, 0)

    def round_of(i, carry):
        @pl.when(i < depth)
        def _():
            column_arrivals(i)

        @pl.when(i == 1)
        def _():
            for step in range(1, groups):
                h = part_at(step)
                for k in range(1, groups):
                    for p in range(PIECES):
                        panel_copy(h, part_at(k), h, p).wait_recv()

        @pl.when(i == depth - 1)
        def _():
            q = index(z, 1 - y, core)

            @pl.when(z > 0)
            def _():
                for p in range(PIECES):
                    row_copy(q, last_part, p, DOWN).start()

            @pl.when(z == depth - 2)
            def _():
                for p in range(PIECES):
                    row_copy(q, last_part, p, UP).start()

        at_z = source_at(z, depth, i - 1)
        products(at_z, y)

        def per_piece(t, c):
            @pl.when((i == depth) & (t == (groups - 1) * PIECES))
            def _():
                begin_late()

            @pl.when((at_z != turned) | (t // PIECES != groups - 1))
            def _():
                side_arrival(at_z, part_at(t // PIECES), lax.rem(t, PIECES))

            return c

        lax.fori_loop(0, groups * PIECES, per_piece, 0)

        @pl.when((at_z != turned) & (at_z != final))
        def _():
            products(at_z, 1 - y)

        return carry

    lax.fori_loop(1, depth + 1, round_of, 0)
    for p in range(PIECES):
        side_arrival(turned, last_part, p)
    for p in range(PIECES):
        arrive(index(final, 1 - y, 1 - core), last_part, p)
        arrive(index(turned, 1 - y, 1 - core), last_part, p)

    for step in range(1, shards):
        count_copy(me, lax.rem(me + step, shards)).wait_send()
    for step in range(1, groups):
        for k in range(groups):
            for p in range(PIECES):
                panel_copy(part, k, part_at(step), p).wait_send()

    def drain(i, carry):
        at_z, h, p = i // (groups * PIECES), lax.rem(i // PIECES, groups), lax.rem(i, PIECES)
        q = index(at_z, y, core)
        across = index(at_z, 1 - y, core)

        @pl.when((at_z <= z) & (z < depth - 1))
        def _():
            row_copy(q, h, p, UP).wait_send()

        @pl.when((at_z >= z) & (z > 0))
        def _():
            row_copy(q, h, p, DOWN).wait_send()

        @pl.when((at_z != turned) | (h != last_part))
        def _():
            row_copy(q, h, p, SIDE).wait_send()

        row_copy(q, h, p, CORE).wait_send()
        row_copy(across, h, p, CORE).wait_send()

        @pl.when((at_z == z) & (h == last_part) & (z > 0))
        def _():
            row_copy(across, h, p, DOWN).wait_send()

        @pl.when((at_z == z) & (h == last_part) & (z == depth - 2))
        def _():
            row_copy(across, h, p, UP).wait_send()

        return carry

    lax.fori_loop(0, depth * groups * PIECES, drain, 0)


def shape_of_line(depth):
    z = lax.axis_index("samp") // 4
    low = z < depth // 2
    inward = jnp.where(low, z + 1, z - 1)
    outward = jnp.clip(jnp.where(low, z - 1, z + 1), 0, depth - 1)
    is_end = (z == 0) | (z == depth - 1)
    return z, inward, outward, is_end


def folded_finish(shards, groups, rows, panel, tiles, codes, steps, out_ref, late, out_sem):
    depth = shards // 4
    me = lax.axis_index("samp")
    y = (me // 2) % 2
    z, inward, outward, is_end = shape_of_line(depth)
    far_mid, far_end = depth - 1 - inward, depth - 1 - z
    last_part = lax.rem(lax.axis_index("snp") + groups - 1, groups)
    piece_rows = rows.shape[3]
    tile_rows = PIECES * piece_rows

    def is_late(q):
        return is_end & ((q // 4 == far_end) | ((q // 4 == far_mid) & ((q // 2) % 2 != y)))

    def put(q, carry):
        @pl.when(jnp.logical_not(is_late(q)))
        def _():
            pltpu.make_async_copy(tiles.at[q], out_ref.at[q, 0], out_sem.at[0]).start()

        return carry

    lax.fori_loop(0, shards, put, 0)

    @pl.when(is_end)
    def _():
        def decode(t, carry):
            for p in range(PIECES):
                for k in range(groups):
                    unit = (t * PIECES + p) * groups + k
                    late[t, p * piece_rows:(p + 1) * piece_rows, k * tile_rows:(k + 1) * tile_rows] = (
                        codes[unit].astype(jnp.float32) * steps[unit])
            q = index(far_end, jnp.where(t // 2 == 0, y, 1 - y), lax.rem(t, 2))
            pltpu.make_async_copy(late.at[t], out_ref.at[q, 0], out_sem.at[0]).start()
            return carry

        lax.fori_loop(0, 4, decode, 0)

        def form(i, carry):
            q = index(far_mid, 1 - y, i)
            late[4 + i] = tiles[q] + product(rows, panel, q, [last_part])
            pltpu.make_async_copy(late.at[4 + i], out_ref.at[q, 0], out_sem.at[0]).start()
            return carry

        lax.fori_loop(0, 2, form, 0)

    pltpu.make_async_copy(tiles, out_ref.at[:, 0], out_sem.at[0]).wait()


def folded(shards, groups, geno_hbm, obs_hbm, panel, rows, tiles, codes, steps, geno_ref, obs_ref, alts, calls, columns,
           made, made_steps, raw, raw_in, load_sem, count_sem, across_send, across_recv, line_send, side_send, core_send, row_recv,
           core_recv, code_sem, raw_sem):
    row_count, snp_count = geno_ref.shape
    tile_rows = row_count // groups
    piece_rows = tile_rows // PIECES
    depth = shards // 4
    me = lax.axis_index("samp")
    part = lax.axis_index("snp")
    y, core = (me // 2) % 2, me % 2
    z, inward, outward, is_end = shape_of_line(depth)
    other = lax.rem(part + 1, groups)
    load_rows = row_count // LOADS

    def load(i):
        block = pl.ds(pl.multiple_of(i * load_rows, load_rows), load_rows)
        return (pltpu.make_async_copy(geno_hbm.at[block], geno_ref.at[block], load_sem.at[0, i]),
                pltpu.make_async_copy(obs_hbm.at[block], obs_ref.at[block], load_sem.at[1, i]))

    for i in range(LOADS):
        for copy in load(i):
            copy.start()

    barrier = pltpu.get_barrier_semaphore()
    for step in range(1, shards):
        pl.semaphore_signal(barrier, inc=1, device_id={"samp": lax.rem(me + step, shards)}, device_id_type=MESH)
    pl.semaphore_signal(barrier, inc=1, device_id={"snp": other}, device_id_type=MESH)

    def add_strip(i, total):
        alt, call = total
        strip = pl.ds(pl.multiple_of(i * STRIP, STRIP), STRIP)
        present = obs_ref[strip, :].astype(jnp.float32)
        held = present * geno_ref[strip, :]
        for r in range(0, STRIP, 8):
            alt = alt + held[r:r + 8]
            call = call + present[r:r + 8]
        return alt, call

    zero = jnp.zeros((8, snp_count), jnp.float32)
    alt, call = zero, zero
    strips = load_rows // STRIP
    for i in range(LOADS):
        for copy in load(i):
            copy.wait()
        alt, call = lax.fori_loop(i * strips, (i + 1) * strips, add_strip, (alt, call))
    alts[me] = jnp.sum(alt, axis=0, keepdims=True)
    call = jnp.sum(call, axis=0, keepdims=True).astype(jnp.int32)
    half = snp_count // 2
    calls[me] = jnp.concatenate([call[:, :half], call[:, half:]]).astype(jnp.int16)

    pl.semaphore_wait(barrier, shards)

    for step in range(shards):
        to = jnp.where(z < depth // 2, shards - 1 - step, step)

        @pl.when(to != me)
        def _():
            for n, sent in enumerate((alts, calls)):
                pltpu.make_async_remote_copy(
                    src_ref=sent.at[me], dst_ref=sent.at[me], send_sem=count_sem.at[2 * n],
                    recv_sem=count_sem.at[2 * n + 1], device_id={"samp": to}, device_id_type=MESH).start()

    def await_bytes(ref, sem):
        pltpu.make_async_copy(ref, ref, sem).wait()

    def await_rows(count, sem):
        await_bytes(geno_ref.at[pl.ds(0, count // 2)], sem)

    def raw_copy(to, slot):
        return pltpu.make_async_remote_copy(
            src_ref=raw, dst_ref=raw_in.at[slot], send_sem=raw_sem.at[0], recv_sem=raw_sem.at[1 + slot],
            device_id={"samp": to}, device_id_type=MESH)

    early = pl.ds(pl.multiple_of(part * tile_rows, tile_rows), RAW)
    raw[...] = jnp.where(obs_ref[early, :] > 0, geno_ref[early, :], -1.0)
    raw_copy(index(z, 1 - y, core), 0).start()
    raw_copy(index(inward, y, core), jnp.where(is_end, 2, 1)).start()

    @pl.when(jnp.logical_not(is_end))
    def _():
        raw_copy(index(outward, y, core), 1).start()

    def await_counts(way):
        for n, sent in enumerate((alts, calls)):
            await_bytes(sent.at[pl.ds(0, shards - 1)], count_sem.at[2 * n + way])

    await_counts(1)
    alt, call = alts[0], calls[0].astype(jnp.int32)
    for s in range(1, shards):
        alt, call = alt + alts[s], call + calls[s].astype(jnp.int32)
    call = jnp.concatenate([call[0:1], call[1:2]], axis=1).astype(jnp.float32)
    frequency = alt / (2.0 * jnp.maximum(call, 1.0))
    shift = 2.0 * frequency
    gain = lax.rsqrt(jnp.maximum(shift * (1.0 - frequency), var_floor))

    def piece_of(k, p):
        return pl.ds(pl.multiple_of(k * tile_rows + p * piece_rows, piece_rows), piece_rows)

    strip_rows = min(STRIP, piece_rows)

    def scale_piece(k, p):
        def scale_strip(i, carry):
            start = pl.multiple_of(k * tile_rows + p * piece_rows + i * strip_rows, strip_rows)
            strip = pl.ds(start, strip_rows)
            present = obs_ref[strip, :].astype(jnp.float32)
            panel[part, strip, :] = (present * (geno_ref[strip, :] - shift) * gain).astype(jnp.bfloat16)
            return carry

        lax.fori_loop(0, piece_rows // strip_rows, scale_strip, 0)

    def panel_copy(k, p):
        block = panel.at[part, piece_of(k, p)]
        return pltpu.make_async_remote_copy(
            src_ref=block, dst_ref=block, send_sem=across_send.at[0],
            recv_sem=across_recv.at[jnp.where(k == part, PIECES, p)], device_id={"snp": other}, device_id_type=MESH)

    def column_copy(q, h, p):
        return pltpu.make_async_remote_copy(
            src_ref=rows.at[q, h, p], dst_ref=columns.at[part, h, pl.ds(pl.multiple_of(p * piece_rows, piece_rows), piece_rows)],
            send_sem=across_send.at[1], recv_sem=across_recv.at[PIECES + 1], device_id={"snp": other}, device_id_type=MESH)

    cut = piece_rows * 7 // 8
    head, rest = pl.ds(0, cut), pl.ds(cut, piece_rows - cut)

    def span_copy(q, h, p, span, to, send_sem, recv_sem):
        return pltpu.make_async_remote_copy(
            src_ref=rows.at[q, h, p, span], dst_ref=rows.at[q, h, p, span], send_sem=send_sem, recv_sem=recv_sem,
            device_id={"samp": to}, device_id_type=MESH)

    def own_copy(q, h, p, to, send_sem, src=None, dst=None):
        return pltpu.make_async_remote_copy(
            src_ref=rows.at[q, h, p] if src is None else src, dst_ref=rows.at[q, h, p] if dst is None else dst,
            send_sem=send_sem,
            recv_sem=row_recv.at[q // 2, h, p], device_id={"samp": to}, device_id_type=MESH)

    def send_in(q, h, p, extra=0):
        own_copy(q, h, p, index(inward, y, core), line_send.at[extra]).start()

    def send_out(q, h, p):
        own_copy(q, h, p, index(outward, y, core), line_send.at[2]).start()

    def send_side(q, h, p, extra=0):
        own_copy(q, h, p, index(z, 1 - y, core), side_send.at[extra]).start()

    def half_of(q, h, p):
        return jnp.where(jnp.logical_not(is_end) & (q // 4 == depth - 1 - outward), p, h)

    def send_core(q, h, p, src=None):
        pltpu.make_async_remote_copy(
            src_ref=rows.at[q, h, p] if src is None else src, dst_ref=rows.at[q, h, p], send_sem=core_send.at[0],
            recv_sem=core_recv.at[q // 2, half_of(q, h, p)], device_id={"samp": index(z, y, 1 - core)},
            device_id_type=MESH).start()

    def send_core_span(q, h, p, span):
        span_copy(q, h, p, span, index(z, y, 1 - core), core_send.at[0], core_recv.at[q // 2, half_of(q, h, p)]).start()

    def arrive(q, h, p):
        await_bytes(rows.at[q, h, p], row_recv.at[q // 2, h, p])

    def arrive_core(q, half):
        await_bytes(rows.at[q, 0], core_recv.at[q // 2, half])

    def part_at(i):
        return lax.rem(part + i, groups)

    def send_own(h, p, skip=0):
        mine = panel.at[h, piece_of(part, p)]
        kept = panel.at[h, pl.ds(pl.multiple_of(part * tile_rows + p * piece_rows + skip, 16), piece_rows - skip)]
        kept_to = rows.at[me, h, p, pl.ds(skip, piece_rows - skip)]
        own_copy(me, h, p, index(z, 1 - y, core), side_send.at[0], kept, kept_to).start()
        own_copy(me, h, p, index(inward, y, core), line_send.at[0], kept, kept_to).start()

        @pl.when(jnp.logical_not(is_end))
        def _():
            own_copy(me, h, p, index(outward, y, core), line_send.at[2], kept, kept_to).start()

        send_core(me, h, p, mine)
        rows[me, h, p] = panel[h, piece_of(part, p), :]

    def scale_raw(slot, q):
        await_bytes(raw_in.at[slot], raw_sem.at[1 + slot])
        sent = raw_in[slot]
        rows[q, part, 0, 0:RAW, :] = jnp.where(sent >= 0.0, (sent - shift) * gain, 0.0).astype(jnp.bfloat16)

    def arrive_near(q, h, p):
        @pl.when((h == part) & (p == 0))
        def _():
            await_bytes(rows.at[q, h, p, pl.ds(RAW, piece_rows - RAW)], row_recv.at[q // 2, h, p])

        @pl.when((h != part) | (p != 0))
        def _():
            arrive(q, h, p)

    for p in range(PIECES):
        scale_piece(part, p)
        send_own(part, p, 0 if p else RAW)
        scale_piece(other, p)
        panel_copy(other, p).start()
    for p in range(PIECES):
        panel_copy(part, p).start()
    scale_raw(0, index(z, 1 - y, core))
    scale_raw(1, index(inward, y, core))

    @pl.when(jnp.logical_not(is_end))
    def _():
        scale_raw(2, index(outward, y, core))

    for p in range(PIECES):
        await_bytes(panel.at[other, piece_of(part, p)], across_recv.at[p])
        send_own(other, p)

    def form(at_z, at_y, parts=None, wait=True):
        def per_core(t, carry):
            q = index(at_z, at_y, lax.rem(core + t, 2))
            if wait:
                @pl.when(t == 1)
                def _():
                    for half in (range(2) if parts is None else parts):
                        arrive_core(q, half)

            tiles[q] = product(rows, panel, q, range(groups) if parts is None else parts)
            return carry

        lax.fori_loop(0, 2, per_core, 0)

    def await_panel():
        await_bytes(panel.at[other, pl.ds(pl.multiple_of(other * tile_rows, tile_rows), tile_rows)], across_recv.at[PIECES])

    def pick(i, values):
        chosen = values[-1]
        for n in range(len(values) - 2, -1, -1):
            chosen = jnp.where(i == n, values[n], chosen)
        return chosen

    count = groups * PIECES

    @pl.when(is_end)
    def _():
        far_mid = depth - 1 - inward

        def first(t, carry):
            h, p = part_at(t // PIECES), lax.rem(t, PIECES)
            near, beside = index(inward, y, core), index(z, 1 - y, core)
            arrive_near(near, h, p)
            send_side(near, h, p)
            send_core(near, h, p)
            arrive_near(beside, h, p)
            send_in(beside, h, p)
            send_core(beside, h, p)
            return carry

        lax.fori_loop(0, count, first, 0)
        await_panel()

        def second(t, carry):
            h, p = part_at(t // PIECES), lax.rem(t, PIECES)
            far, cross = index(far_mid, y, core), index(inward, 1 - y, core)
            arrive(far, h, p)
            to = index(z, 1 - y, core)

            @pl.when(p == 0)
            def _():
                send_side(far, h, p, extra=1)

            @pl.when(p == 1)
            def _():
                span_copy(far, h, p, head, to, side_send.at[1], row_recv.at[far // 2, h, p]).start()

            @pl.when((p == 1) & (h == other))
            def _():
                span_copy(far, h, p, rest, to, side_send.at[1], code_sem.at[5]).start()

            send_core(far, h, p)
            arrive(cross, h, p)
            send_core(cross, h, p)

            @pl.when(t < 3)
            def _():
                form(pick(t, (z, inward, z)), pick(t, (y, y, 1 - y)))

            return carry

        lax.fori_loop(0, count, second, 0)

        def third(t, carry):
            h, p = part_at(t // PIECES), lax.rem(t, PIECES)
            q = index(far_mid, 1 - y, core)

            @pl.when(p == 0)
            def _():
                arrive(q, h, p)
                send_core(q, h, p)

            @pl.when(p == 1)
            def _():
                await_bytes(rows.at[q, h, p, head], row_recv.at[q // 2, h, p])
                send_core_span(q, h, p, head)

            @pl.when(t < 2)
            def _():
                form(pick(t, (far_mid, inward)), pick(t, (y, 1 - y)))

            @pl.when(t == 2)
            def _():
                await_bytes(rows.at[q, part, 1, rest], code_sem.at[4])
                send_core_span(q, part, 1, rest)

            @pl.when(t == 3)
            def _():
                await_bytes(rows.at[q, other, 1, rest], code_sem.at[5])
                send_core_span(q, other, 1, rest)

            return carry

        lax.fori_loop(0, count, third, 0)
        form(far_mid, 1 - y, [part])
        await_bytes(codes, code_sem.at[1])
        await_bytes(steps, code_sem.at[3])
        arrive_core(index(far_mid, 1 - y, 1 - core), other)
        await_rows(2 * row_count - RAW, line_send.at[0])
        await_rows(2 * row_count - RAW, side_send.at[0])
        await_rows(count * piece_rows - (piece_rows - cut), side_send.at[1])
        await_bytes(raw_in.at[pl.ds(0, 2)], raw_sem.at[0])
        await_bytes(rows.at[pl.ds(0, 6)], core_send.at[0])

    @pl.when(jnp.logical_not(is_end))
    def _():
        far = depth - 1 - outward

        def first(t, carry):
            h, p = part_at(t // PIECES), lax.rem(t, PIECES)
            end, near, beside = index(outward, y, core), index(inward, y, core), index(z, 1 - y, core)
            arrive_near(end, h, p)

            @pl.when(p == 0)
            def _():
                send_in(end, h, 0)

            @pl.when(h == other)
            def _():
                send_in(end, jnp.where(p == 0, part, other), 1)

            send_core(end, h, p)
            column_copy(end, h, p).start()
            arrive_near(near, h, p)
            send_out(near, h, p)
            send_core(near, h, p)
            arrive_near(beside, h, p)
            send_core(beside, h, p)
            return carry

        lax.fori_loop(0, count, first, 0)
        for p in range(PIECES):
            send_in(index(z, 1 - y, core), part, p, extra=1)
        for h in range(groups):
            columns[part, h] = rows[index(outward, y, core), h].reshape(tile_rows, snp_count)
        await_panel()

        def make(side, p, k):
            def per_core(t, carry):
                which = lax.rem(core + t, 2)
                q = index(far, jnp.where(side == 0, y, 1 - y), which)
                term = None
                for h in range(groups):
                    one = lax.dot_general(rows[q, h, p], columns[k, h], (((1,), (1,)), ((), ())),
                                          preferred_element_type=jnp.float32)
                    term = one if term is None else term + one
                term = term * (1.0 / (groups * snp_count))
                top = jnp.max(jnp.abs(term), axis=0, keepdims=True)
                unit = ((side * 2 + which) * PIECES + p) * groups + k
                made[unit] = jnp.round(term * (CODE_TOP / jnp.maximum(top, TINY))).astype(jnp.int32).astype(jnp.int16)
                made_steps[unit] = top * (1.0 / CODE_TOP)
                for n, (source, target) in enumerate(((made, codes), (made_steps, steps))):
                    pltpu.make_async_remote_copy(
                        src_ref=source.at[unit], dst_ref=target.at[unit], send_sem=code_sem.at[2 * n],
                        recv_sem=code_sem.at[2 * n + 1], device_id={"samp": index(outward, y, core)},
                        device_id_type=MESH).start()
                return carry

            lax.fori_loop(0, 2, per_core, 0)

        def far_core(side, p):
            arrive_core(index(far, jnp.where(side == 0, y, 1 - y), 1 - core), p)

        def make_list(listed):
            def per_entry(i, carry):
                side, p, away = (pick(i, [entry[n] for entry in listed]) for n in range(3))
                make(side, p, lax.rem(part + away, groups))
                return carry

            lax.fori_loop(0, len(listed), per_entry, 0)

        def second(t, carry):
            h, p = part_at(lax.rem(t, groups)), t // groups
            far_q, cross = index(far, y, core), index(outward, 1 - y, core)

            @pl.when(t >= 2)
            def _():
                far_core(t - 2, 0)
                make(t - 2, 0, part)

            arrive(far_q, h, p)
            send_side(far_q, h, p)
            send_core(far_q, h, p)
            ch, cp = part_at(t // PIECES), lax.rem(t, PIECES)
            arrive(cross, ch, cp)
            send_core(cross, ch, cp)

            @pl.when(t > 0)
            def _():
                q = index(far, 1 - y, core)
                h, p = part_at(lax.rem(t - 1, groups)), (t - 1) // groups
                arrive(q, h, p)
                send_core(q, h, p)

            form(pick(t, (z, outward, inward, z)), pick(t, (y, y, y, 1 - y)))
            return carry

        lax.fori_loop(0, count, second, 0)
        for p in range(PIECES):
            send_side(index(inward, y, core), other, p, extra=1)
        far_core(0, 1)
        make_list([(0, 1, 0)])
        await_bytes(columns.at[other], across_recv.at[PIECES + 1])
        make_list([(0, 0, 1), (0, 1, 1), (1, 0, 1)])
        form(outward, 1 - y)
        q = index(far, 1 - y, core)
        arrive(q, other, PIECES - 1)
        send_core(q, other, PIECES - 1)
        cross = index(inward, 1 - y, core)

        def third(t, carry):
            h, p = part_at(t // PIECES), lax.rem(t, PIECES)
            arrive(cross, h, p)
            send_core(cross, h, p)

            @pl.when(t == 1)
            def _():
                span_copy(cross, h, p, rest, index(outward, y, core), line_send.at[3], code_sem.at[4]).start()
                far_core(1, 1)
                make_list([(1, 1, 0), (1, 1, 1)])

            @pl.when(t < 2)
            def _():
                form(far, pick(t, (y, 1 - y)), wait=False)

            return carry

        lax.fori_loop(0, count, third, 0)
        form(inward, 1 - y)
        await_rows(2 * row_count - RAW, line_send.at[0])
        await_bytes(rows.at[0, 0], line_send.at[1])
        await_rows(2 * row_count - RAW, line_send.at[2])
        await_bytes(raw_in, raw_sem.at[0])
        await_rows(piece_rows - cut, line_send.at[3])
        await_rows(2 * row_count - RAW, side_send.at[0])
        await_bytes(rows.at[0, 0], side_send.at[1])
        await_bytes(rows.at[pl.ds(0, 8)], core_send.at[0])
        await_bytes(rows.at[0], across_send.at[1])
        await_bytes(made, code_sem.at[0])
        await_bytes(made_steps, code_sem.at[2])

    await_counts(0)
    await_bytes(rows.at[0], across_send.at[0])


def folded_body(shards, groups, genotypes, observed):
    row_count, snp_count = genotypes.shape
    tile_rows = row_count // groups
    piece_rows = tile_rows // PIECES
    units = 4 * PIECES * groups
    outs = (
        pltpu.VMEM((groups, row_count, snp_count), jnp.bfloat16),
        pltpu.VMEM((shards, groups, PIECES, piece_rows, snp_count), jnp.bfloat16),
        pltpu.VMEM((shards, tile_rows, row_count), jnp.float32),
        pltpu.VMEM((units, piece_rows, tile_rows), jnp.int16),
        pltpu.VMEM((units, 1, tile_rows), jnp.float32),
    )
    kept = sum(math.prod(o.shape) * jnp.dtype(o.dtype).itemsize for o in outs)
    held = pl.pallas_call(
        functools.partial(folded, shards, groups),
        out_shape=outs,
        in_specs=[pl.BlockSpec(memory_space=pltpu.HBM)] * 2,
        out_specs=[pl.BlockSpec(memory_space=pltpu.VMEM)] * 5,
        scratch_shapes=[
            pltpu.VMEM((row_count, snp_count), jnp.float32),
            pltpu.VMEM((row_count, snp_count), jnp.int32),
            pltpu.VMEM((shards, 1, snp_count), jnp.float32),
            pltpu.VMEM((shards, 2, snp_count // 2), jnp.int16),
            pltpu.VMEM((groups, groups, tile_rows, snp_count), jnp.bfloat16),
            pltpu.VMEM((units, piece_rows, tile_rows), jnp.int16),
            pltpu.VMEM((units, 1, tile_rows), jnp.float32),
            pltpu.VMEM((RAW, snp_count), jnp.float32),
            pltpu.VMEM((3, RAW, snp_count), jnp.float32),
            pltpu.SemaphoreType.DMA((2, LOADS)),
            pltpu.SemaphoreType.DMA((4,)),
            pltpu.SemaphoreType.DMA((2,)),
            pltpu.SemaphoreType.DMA((PIECES + 2,)),
            pltpu.SemaphoreType.DMA((4,)),
            pltpu.SemaphoreType.DMA((2,)),
            pltpu.SemaphoreType.DMA((1,)),
            pltpu.SemaphoreType.DMA((shards // 2, groups, PIECES)),
            pltpu.SemaphoreType.DMA((shards // 2, 2)),
            pltpu.SemaphoreType.DMA((6,)),
            pltpu.SemaphoreType.DMA((4,)),
        ],
        compiler_params=pltpu.CompilerParams(
            collective_id=0, has_side_effects=True, vmem_limit_bytes=VMEM_ALL - FOLDED_SPARE - kept),
    )(genotypes, observed)
    panel, rows, tiles, codes, steps = held
    return pl.pallas_call(
        functools.partial(folded_finish, shards, groups),
        out_shape=jax.ShapeDtypeStruct((shards, 1, tile_rows, row_count), jnp.float32),
        in_specs=[pl.BlockSpec(memory_space=pltpu.VMEM)] * 5,
        out_specs=pl.BlockSpec(memory_space=pltpu.HBM),
        scratch_shapes=[
            pltpu.VMEM((6, tile_rows, row_count), jnp.float32),
            pltpu.SemaphoreType.DMA((1,)),
        ],
        compiler_params=pltpu.CompilerParams(vmem_limit_bytes=FOLDED_FINISH),
    )(rows, panel, tiles, codes, steps)


def solution(mesh):
    shards, groups = mesh.shape["samp"], mesh.shape["snp"]

    def body(genotypes, observed):
        if groups == 2 and shards == 16:
            return folded_body(shards, groups, genotypes, observed)
        row_count, snp_count = genotypes.shape
        tile_rows = row_count // groups
        piece_rows = tile_rows // PIECES
        kept = 2 * (groups * row_count * snp_count) * (1 + shards // groups) + 4 * shards * tile_rows * row_count
        panel, rows, tiles = pl.pallas_call(
            functools.partial(kernel, shards, groups),
            out_shape=(
                pltpu.VMEM((groups, row_count, snp_count), jnp.bfloat16),
                pltpu.VMEM((shards, groups, PIECES, piece_rows, snp_count), jnp.bfloat16),
                pltpu.VMEM((shards, tile_rows, row_count), jnp.float32),
            ),
            in_specs=[pl.BlockSpec(memory_space=pltpu.HBM)] * 2,
            out_specs=[pl.BlockSpec(memory_space=pltpu.VMEM)] * 3,
            scratch_shapes=[
                pltpu.VMEM((row_count, snp_count), jnp.float32),
                pltpu.VMEM((row_count, snp_count), jnp.int32),
                pltpu.VMEM((shards, 2, snp_count), jnp.float32),
                pltpu.SemaphoreType.DMA((2, LOADS)),
                pltpu.SemaphoreType.DMA((shards,)),
                pltpu.SemaphoreType.DMA((shards,)),
                pltpu.SemaphoreType.DMA((groups, groups, PIECES)),
                pltpu.SemaphoreType.DMA((groups, groups, PIECES)),
                pltpu.SemaphoreType.DMA((4, shards, groups, PIECES)),
                pltpu.SemaphoreType.DMA((shards, groups, PIECES)),
            ],
            compiler_params=pltpu.CompilerParams(
                collective_id=0, has_side_effects=True, vmem_limit_bytes=VMEM_ALL - VMEM_SPARE - kept),
        )(genotypes, observed)
        return pl.pallas_call(
            functools.partial(finish, shards, groups),
            out_shape=jax.ShapeDtypeStruct((shards, 1, tile_rows, row_count), jnp.float32),
            in_specs=[pl.BlockSpec(memory_space=pltpu.VMEM)] * 3,
            out_specs=pl.BlockSpec(memory_space=pltpu.HBM),
            scratch_shapes=[
                pltpu.VMEM((4, tile_rows, row_count), jnp.float32),
                pltpu.SemaphoreType.DMA((shards,)),
            ],
            compiler_params=pltpu.CompilerParams(vmem_limit_bytes=VMEM_FINISH),
        )(rows, panel, tiles)

    return jax.shard_map(
        body,
        mesh=mesh,
        in_specs=(P("samp", "snp"), P("samp", "snp")),
        out_specs=P(None, "snp", None, "samp"),
        check_vma=False,
    )
```

```python
import functools
import math

import jax
import jax.numpy as jnp
from jax import lax
from jax.experimental import pallas as pl
from jax.experimental.pallas import tpu as pltpu
from jax.sharding import PartitionSpec as P

MESH = pl.DeviceIdType.MESH
var_floor = 0.1
UP, DOWN, SIDE, CORE = 0, 1, 2, 3
STRIP = 64
PIECES = 2
LOADS = 4
VMEM_ALL = 67043328
VMEM_SPARE = 512 * 1024
VMEM_FINISH = 12 * 1024 * 1024
FOLDED_SPARE = 1024 * 1024
FOLDED_FINISH = 8 * 1024 * 1024
CODE_TOP = 32767.0
TINY = 1e-30
RAW = 32


def index(at_z, at_y, at_core):
    return at_z * 4 + at_y * 2 + at_core


def source_at(z, depth, i):
    pairs = jnp.minimum(z, depth - 1 - z)
    side = jnp.where(i % 2 == 1, z - (i + 1) // 2, z + i // 2)
    far = jnp.where(z < depth - 1 - z, z + i - pairs, z - i + pairs)
    return jnp.where(i <= 2 * pairs, side, far)


def turned_at(z, depth):
    return jnp.where(z < depth - 1, z + 1, depth - 2)


def product(rows, panel, q, parts):
    pieces, piece_rows, snp_count = rows.shape[2:]
    total = None
    for h in parts:
        block = rows[q, h].reshape(pieces * piece_rows, snp_count)
        term = lax.dot_general(block, panel[h], (((1,), (1,)), ((), ())), preferred_element_type=jnp.float32)
        total = term if total is None else total + term
    return total * (1.0 / (rows.shape[1] * snp_count))


def finish(shards, groups, rows, panel, tiles, out_ref, late, out_sem):
    depth = shards // 4
    me = lax.axis_index("samp")
    z, y = me // 4, (me // 2) % 2
    turned = turned_at(z, depth)
    final = source_at(z, depth, depth - 1)
    final = jnp.where(final == turned, source_at(z, depth, depth - 2), final)
    last_part = lax.rem(lax.axis_index("snp") + groups - 1, groups)

    def is_late(q):
        return ((q // 4 == turned) | (q // 4 == final)) & ((q // 2) % 2 != y)

    def put(q, carry):
        @pl.when(jnp.logical_not(is_late(q)))
        def _():
            pltpu.make_async_copy(tiles.at[q], out_ref.at[q, 0], out_sem.at[q]).start()

        return carry

    lax.fori_loop(0, shards, put, 0)

    def form(i, carry):
        q = index(jnp.where(i // 2 == 0, final, turned), 1 - y, lax.rem(i, 2))
        late[i] = tiles[q] + product(rows, panel, q, [last_part])
        pltpu.make_async_copy(late.at[i], out_ref.at[q, 0], out_sem.at[q]).start()
        return carry

    lax.fori_loop(0, 4, form, 0)

    def flush(q, carry):
        pltpu.make_async_copy(tiles.at[q], out_ref.at[q, 0], out_sem.at[q]).wait()
        return carry

    lax.fori_loop(0, shards, flush, 0)


def kernel(shards, groups, geno_hbm, obs_hbm, panel, rows, tiles, geno_ref, obs_ref, counts, load_sem,
           count_send, count_recv, panel_send, panel_recv, row_send, row_recv):
    row_count, snp_count = geno_ref.shape
    tile_rows = row_count // groups
    piece_rows = tile_rows // PIECES
    depth = shards // 4
    me = lax.axis_index("samp")
    part = lax.axis_index("snp")
    z, y, core = me // 4, (me // 2) % 2, me % 2

    load_rows = row_count // LOADS

    def load(i):
        block = pl.ds(pl.multiple_of(i * load_rows, load_rows), load_rows)
        return (pltpu.make_async_copy(geno_hbm.at[block], geno_ref.at[block], load_sem.at[0, i]),
                pltpu.make_async_copy(obs_hbm.at[block], obs_ref.at[block], load_sem.at[1, i]))

    for i in range(LOADS):
        for copy in load(i):
            copy.start()

    barrier = pltpu.get_barrier_semaphore()
    for step in range(1, shards):
        pl.semaphore_signal(barrier, inc=1, device_id={"samp": lax.rem(me + step, shards)}, device_id_type=MESH)
    for step in range(1, groups):
        pl.semaphore_signal(barrier, inc=1, device_id={"snp": lax.rem(part + step, groups)}, device_id_type=MESH)

    def add_strip(i, total):
        alt, call = total
        strip = pl.ds(pl.multiple_of(i * STRIP, STRIP), STRIP)
        present = obs_ref[strip, :].astype(jnp.float32)
        held = present * geno_ref[strip, :]
        for r in range(0, STRIP, 8):
            alt = alt + held[r:r + 8]
            call = call + present[r:r + 8]
        return alt, call

    zero = jnp.zeros((8, snp_count), jnp.float32)
    alt, call = zero, zero
    strips = load_rows // STRIP
    for i in range(LOADS):
        for copy in load(i):
            copy.wait()
        alt, call = lax.fori_loop(i * strips, (i + 1) * strips, add_strip, (alt, call))
    counts[me, 0:1, :] = jnp.sum(alt, axis=0, keepdims=True)
    counts[me, 1:2, :] = jnp.sum(call, axis=0, keepdims=True)

    pl.semaphore_wait(barrier, shards + groups - 2)

    def count_copy(owner, to):
        return pltpu.make_async_remote_copy(
            src_ref=counts.at[owner], dst_ref=counts.at[owner], send_sem=count_send.at[to],
            recv_sem=count_recv.at[owner], device_id={"samp": to}, device_id_type=MESH)

    for step in range(1, shards):
        count_copy(me, lax.rem(me + step, shards)).start()
    for step in range(1, shards):
        other = lax.rem(me + step, shards)
        count_copy(other, other).wait_recv()
    sums = counts[0]
    for s in range(1, shards):
        sums = sums + counts[s]
    frequency = sums[0:1] / (2.0 * jnp.maximum(sums[1:2], 1.0))
    shift = 2.0 * frequency
    gain = lax.rsqrt(jnp.maximum(shift * (1.0 - frequency), var_floor))

    def piece_of(k, p):
        return pl.ds(pl.multiple_of(k * tile_rows + p * piece_rows, piece_rows), piece_rows)

    def panel_copy(h, k, to, p):
        block = panel.at[h, piece_of(k, p)]
        return pltpu.make_async_remote_copy(
            src_ref=block, dst_ref=block, send_sem=panel_send.at[to, k, p],
            recv_sem=panel_recv.at[h, k, p], device_id={"snp": to}, device_id_type=MESH)

    strip_rows = min(STRIP, piece_rows)

    def scale_piece(k, p):
        def scale_strip(i, carry):
            start = pl.multiple_of(k * tile_rows + p * piece_rows + i * strip_rows, strip_rows)
            strip = pl.ds(start, strip_rows)
            present = obs_ref[strip, :].astype(jnp.float32)
            panel[part, strip, :] = (present * (geno_ref[strip, :] - shift) * gain).astype(jnp.bfloat16)
            return carry

        lax.fori_loop(0, piece_rows // strip_rows, scale_strip, 0)

    def row_copy(q, h, p, way, src=None):
        to = (index(z + 1, y, core), index(z - 1, y, core), index(z, 1 - y, core), index(z, y, 1 - core))[way]
        return pltpu.make_async_remote_copy(
            src_ref=rows.at[q, h, p] if src is None else src, dst_ref=rows.at[q, h, p],
            send_sem=row_send.at[way, q, h, p], recv_sem=row_recv.at[q, h, p],
            device_id={"samp": to}, device_id_type=MESH)

    def arrive(q, h, p):
        row_copy(q, h, p, CORE).wait_recv()

    last_part = lax.rem(part + groups - 1, groups)
    turned = turned_at(z, depth)

    def part_at(i):
        return lax.rem(part + i, groups)

    def send_own(h, p):
        mine = panel.at[h, piece_of(part, p)]
        row_copy(me, h, p, SIDE, mine).start()

        @pl.when(z < depth - 1)
        def _():
            row_copy(me, h, p, UP, mine).start()

        @pl.when(z > 0)
        def _():
            row_copy(me, h, p, DOWN, mine).start()

        row_copy(me, h, p, CORE, mine).start()
        rows[me, h, p] = panel[h, piece_of(part, p), :]

    for p in range(PIECES):
        for step in range(1, groups):
            other = part_at(step)
            scale_piece(other, p)
            panel_copy(part, other, other, p).start()
        scale_piece(part, p)
        send_own(part, p)
    for step in range(1, groups):
        other = part_at(step)
        for k in range(1, groups):
            for p in range(PIECES):
                panel_copy(part, lax.rem(other + k, groups), other, p).start()
    for step in range(1, groups):
        h = part_at(step)
        for p in range(PIECES):
            panel_copy(h, part, h, p).wait_recv()
            send_own(h, p)

    def column_arrival(at_z, h, p, way):
        q = index(at_z, y, core)
        arrive(q, h, p)

        @pl.when(z < depth - 1 if way == UP else z > 0)
        def _():
            row_copy(q, h, p, way).start()

        @pl.when((at_z != turned) | (h != last_part))
        def _():
            row_copy(q, h, p, SIDE).start()

        row_copy(q, h, p, CORE).start()

    def column_arrivals(i):
        def per_piece(t, carry):
            h, p = part_at(t // PIECES), lax.rem(t, PIECES)

            @pl.when(z - i >= 0)
            def _():
                column_arrival(z - i, h, p, UP)

            @pl.when(z + i < depth)
            def _():
                column_arrival(z + i, h, p, DOWN)

            return carry

        lax.fori_loop(0, groups * PIECES, per_piece, 0)

    def arrive_all(q):
        def per_piece(t, carry):
            arrive(q, t // PIECES, lax.rem(t, PIECES))
            return carry

        lax.fori_loop(0, groups * PIECES, per_piece, 0)

    def products(at_z, at_y):
        def per_core(t, carry):
            q = index(at_z, at_y, lax.rem(core + t, 2))

            @pl.when(t == 1)
            def _():
                arrive_all(q)

            tiles[q] = product(rows, panel, q, range(groups))
            return carry

        lax.fori_loop(0, 2, per_core, 0)

    def side_arrival(at_z, h, p):
        q = index(at_z, 1 - y, core)
        arrive(q, h, p)
        row_copy(q, h, p, CORE).start()

    final = source_at(z, depth, depth - 1)
    final = jnp.where(final == turned, source_at(z, depth, depth - 2), final)

    def begin_late():
        def per_tile(t, carry):
            q = index(jnp.where(t % 2 == 0, turned, final), 1 - y, lax.rem(core + t // 2, 2))

            @pl.when(t >= 2)
            def _():
                for step in range(groups - 1):
                    for p in range(PIECES):
                        arrive(q, part_at(step), p)

            tiles[q] = product(rows, panel, q, [part_at(step) for step in range(groups - 1)])
            return carry

        lax.fori_loop(0, 4, per_tile, 0)

    def round_of(i, carry):
        @pl.when(i < depth)
        def _():
            column_arrivals(i)

        @pl.when(i == 1)
        def _():
            for step in range(1, groups):
                h = part_at(step)
                for k in range(1, groups):
                    for p in range(PIECES):
                        panel_copy(h, part_at(k), h, p).wait_recv()

        @pl.when(i == depth - 1)
        def _():
            q = index(z, 1 - y, core)

            @pl.when(z > 0)
            def _():
                for p in range(PIECES):
                    row_copy(q, last_part, p, DOWN).start()

            @pl.when(z == depth - 2)
            def _():
                for p in range(PIECES):
                    row_copy(q, last_part, p, UP).start()

        at_z = source_at(z, depth, i - 1)
        products(at_z, y)

        def per_piece(t, c):
            @pl.when((i == depth) & (t == (groups - 1) * PIECES))
            def _():
                begin_late()

            @pl.when((at_z != turned) | (t // PIECES != groups - 1))
            def _():
                side_arrival(at_z, part_at(t // PIECES), lax.rem(t, PIECES))

            return c

        lax.fori_loop(0, groups * PIECES, per_piece, 0)

        @pl.when((at_z != turned) & (at_z != final))
        def _():
            products(at_z, 1 - y)

        return carry

    lax.fori_loop(1, depth + 1, round_of, 0)
    for p in range(PIECES):
        side_arrival(turned, last_part, p)
    for p in range(PIECES):
        arrive(index(final, 1 - y, 1 - core), last_part, p)
        arrive(index(turned, 1 - y, 1 - core), last_part, p)

    for step in range(1, shards):
        count_copy(me, lax.rem(me + step, shards)).wait_send()
    for step in range(1, groups):
        for k in range(groups):
            for p in range(PIECES):
                panel_copy(part, k, part_at(step), p).wait_send()

    def drain(i, carry):
        at_z, h, p = i // (groups * PIECES), lax.rem(i // PIECES, groups), lax.rem(i, PIECES)
        q = index(at_z, y, core)
        across = index(at_z, 1 - y, core)

        @pl.when((at_z <= z) & (z < depth - 1))
        def _():
            row_copy(q, h, p, UP).wait_send()

        @pl.when((at_z >= z) & (z > 0))
        def _():
            row_copy(q, h, p, DOWN).wait_send()

        @pl.when((at_z != turned) | (h != last_part))
        def _():
            row_copy(q, h, p, SIDE).wait_send()

        row_copy(q, h, p, CORE).wait_send()
        row_copy(across, h, p, CORE).wait_send()

        @pl.when((at_z == z) & (h == last_part) & (z > 0))
        def _():
            row_copy(across, h, p, DOWN).wait_send()

        @pl.when((at_z == z) & (h == last_part) & (z == depth - 2))
        def _():
            row_copy(across, h, p, UP).wait_send()

        return carry

    lax.fori_loop(0, depth * groups * PIECES, drain, 0)


def shape_of_line(depth):
    z = lax.axis_index("samp") // 4
    low = z < depth // 2
    inward = jnp.where(low, z + 1, z - 1)
    outward = jnp.clip(jnp.where(low, z - 1, z + 1), 0, depth - 1)
    is_end = (z == 0) | (z == depth - 1)
    return z, inward, outward, is_end


def folded_finish(shards, groups, rows, panel, tiles, codes, steps, out_ref, late, out_sem):
    depth = shards // 4
    me = lax.axis_index("samp")
    y = (me // 2) % 2
    z, inward, outward, is_end = shape_of_line(depth)
    far_mid, far_end = depth - 1 - inward, depth - 1 - z
    last_part = lax.rem(lax.axis_index("snp") + groups - 1, groups)
    piece_rows = rows.shape[3]
    tile_rows = PIECES * piece_rows

    def is_late(q):
        return is_end & ((q // 4 == far_end) | ((q // 4 == far_mid) & ((q // 2) % 2 != y)))

    def put(q, carry):
        @pl.when(jnp.logical_not(is_late(q)))
        def _():
            pltpu.make_async_copy(tiles.at[q], out_ref.at[q, 0], out_sem.at[0]).start()

        return carry

    lax.fori_loop(0, shards, put, 0)

    @pl.when(is_end)
    def _():
        def decode(t, carry):
            for p in range(PIECES):
                for k in range(groups):
                    unit = (t * PIECES + p) * groups + k
                    late[t, p * piece_rows:(p + 1) * piece_rows, k * tile_rows:(k + 1) * tile_rows] = (
                        codes[unit].astype(jnp.float32) * steps[unit])
            q = index(far_end, jnp.where(t // 2 == 0, y, 1 - y), lax.rem(t, 2))
            pltpu.make_async_copy(late.at[t], out_ref.at[q, 0], out_sem.at[0]).start()
            return carry

        lax.fori_loop(0, 4, decode, 0)

        def form(i, carry):
            q = index(far_mid, 1 - y, i)
            late[4 + i] = tiles[q] + product(rows, panel, q, [last_part])
            pltpu.make_async_copy(late.at[4 + i], out_ref.at[q, 0], out_sem.at[0]).start()
            return carry

        lax.fori_loop(0, 2, form, 0)

    pltpu.make_async_copy(tiles, out_ref.at[:, 0], out_sem.at[0]).wait()


def folded(shards, groups, geno_hbm, obs_hbm, panel, rows, tiles, codes, steps, geno_ref, obs_ref, alts, calls, columns,
           made, made_steps, raw, raw_in, load_sem, count_sem, across_send, across_recv, line_send, side_send, core_send, row_recv,
           core_recv, code_sem, raw_sem):
    row_count, snp_count = geno_ref.shape
    tile_rows = row_count // groups
    piece_rows = tile_rows // PIECES
    depth = shards // 4
    me = lax.axis_index("samp")
    part = lax.axis_index("snp")
    y, core = (me // 2) % 2, me % 2
    z, inward, outward, is_end = shape_of_line(depth)
    other = lax.rem(part + 1, groups)
    load_rows = row_count // LOADS

    def load(i):
        block = pl.ds(pl.multiple_of(i * load_rows, load_rows), load_rows)
        return (pltpu.make_async_copy(geno_hbm.at[block], geno_ref.at[block], load_sem.at[0, i]),
                pltpu.make_async_copy(obs_hbm.at[block], obs_ref.at[block], load_sem.at[1, i]))

    for i in range(LOADS):
        for copy in load(i):
            copy.start()

    barrier = pltpu.get_barrier_semaphore()
    for step in range(1, shards):
        pl.semaphore_signal(barrier, inc=1, device_id={"samp": lax.rem(me + step, shards)}, device_id_type=MESH)
    pl.semaphore_signal(barrier, inc=1, device_id={"snp": other}, device_id_type=MESH)

    def add_strip(i, total):
        alt, call = total
        strip = pl.ds(pl.multiple_of(i * STRIP, STRIP), STRIP)
        present = obs_ref[strip, :].astype(jnp.float32)
        held = present * geno_ref[strip, :]
        for r in range(0, STRIP, 8):
            alt = alt + held[r:r + 8]
            call = call + present[r:r + 8]
        return alt, call

    zero = jnp.zeros((8, snp_count), jnp.float32)
    alt, call = zero, zero
    strips = load_rows // STRIP
    for i in range(LOADS):
        for copy in load(i):
            copy.wait()
        alt, call = lax.fori_loop(i * strips, (i + 1) * strips, add_strip, (alt, call))
    alts[me] = jnp.sum(alt, axis=0, keepdims=True)
    call = jnp.sum(call, axis=0, keepdims=True).astype(jnp.int32)
    half = snp_count // 2
    calls[me] = jnp.concatenate([call[:, :half], call[:, half:]]).astype(jnp.int16)

    pl.semaphore_wait(barrier, shards)

    for step in range(shards):
        to = jnp.where(z < depth // 2, shards - 1 - step, step)

        @pl.when(to != me)
        def _():
            for n, sent in enumerate((alts, calls)):
                pltpu.make_async_remote_copy(
                    src_ref=sent.at[me], dst_ref=sent.at[me], send_sem=count_sem.at[2 * n],
                    recv_sem=count_sem.at[2 * n + 1], device_id={"samp": to}, device_id_type=MESH).start()

    def await_bytes(ref, sem):
        pltpu.make_async_copy(ref, ref, sem).wait()

    def await_rows(count, sem):
        await_bytes(geno_ref.at[pl.ds(0, count // 2)], sem)

    def raw_copy(to, slot):
        return pltpu.make_async_remote_copy(
            src_ref=raw, dst_ref=raw_in.at[slot], send_sem=raw_sem.at[0], recv_sem=raw_sem.at[1 + slot],
            device_id={"samp": to}, device_id_type=MESH)

    early = pl.ds(pl.multiple_of(part * tile_rows, tile_rows), RAW)
    raw[...] = jnp.where(obs_ref[early, :] > 0, geno_ref[early, :], -1.0)
    raw_copy(index(z, 1 - y, core), 0).start()
    raw_copy(index(inward, y, core), jnp.where(is_end, 2, 1)).start()

    @pl.when(jnp.logical_not(is_end))
    def _():
        raw_copy(index(outward, y, core), 1).start()

    def await_counts(way):
        for n, sent in enumerate((alts, calls)):
            await_bytes(sent.at[pl.ds(0, shards - 1)], count_sem.at[2 * n + way])

    await_counts(1)
    alt, call = alts[0], calls[0].astype(jnp.int32)
    for s in range(1, shards):
        alt, call = alt + alts[s], call + calls[s].astype(jnp.int32)
    call = jnp.concatenate([call[0:1], call[1:2]], axis=1).astype(jnp.float32)
    frequency = alt / (2.0 * jnp.maximum(call, 1.0))
    shift = 2.0 * frequency
    gain = lax.rsqrt(jnp.maximum(shift * (1.0 - frequency), var_floor))

    def piece_of(k, p):
        return pl.ds(pl.multiple_of(k * tile_rows + p * piece_rows, piece_rows), piece_rows)

    strip_rows = min(STRIP, piece_rows)

    def scale_piece(k, p):
        def scale_strip(i, carry):
            start = pl.multiple_of(k * tile_rows + p * piece_rows + i * strip_rows, strip_rows)
            strip = pl.ds(start, strip_rows)
            present = obs_ref[strip, :].astype(jnp.float32)
            panel[part, strip, :] = (present * (geno_ref[strip, :] - shift) * gain).astype(jnp.bfloat16)
            return carry

        lax.fori_loop(0, piece_rows // strip_rows, scale_strip, 0)

    def panel_copy(k, p):
        block = panel.at[part, piece_of(k, p)]
        return pltpu.make_async_remote_copy(
            src_ref=block, dst_ref=block, send_sem=across_send.at[0],
            recv_sem=across_recv.at[jnp.where(k == part, PIECES, p)], device_id={"snp": other}, device_id_type=MESH)

    def column_copy(q, h, p):
        return pltpu.make_async_remote_copy(
            src_ref=rows.at[q, h, p], dst_ref=columns.at[part, h, pl.ds(pl.multiple_of(p * piece_rows, piece_rows), piece_rows)],
            send_sem=across_send.at[1], recv_sem=across_recv.at[PIECES + 1], device_id={"snp": other}, device_id_type=MESH)

    cut = piece_rows * 7 // 8
    head, rest = pl.ds(0, cut), pl.ds(cut, piece_rows - cut)

    def span_copy(q, h, p, span, to, send_sem, recv_sem):
        return pltpu.make_async_remote_copy(
            src_ref=rows.at[q, h, p, span], dst_ref=rows.at[q, h, p, span], send_sem=send_sem, recv_sem=recv_sem,
            device_id={"samp": to}, device_id_type=MESH)

    def own_copy(q, h, p, to, send_sem, src=None, dst=None):
        return pltpu.make_async_remote_copy(
            src_ref=rows.at[q, h, p] if src is None else src, dst_ref=rows.at[q, h, p] if dst is None else dst,
            send_sem=send_sem,
            recv_sem=row_recv.at[q // 2, h, p], device_id={"samp": to}, device_id_type=MESH)

    def send_in(q, h, p, extra=0):
        own_copy(q, h, p, index(inward, y, core), line_send.at[extra]).start()

    def send_out(q, h, p):
        own_copy(q, h, p, index(outward, y, core), line_send.at[2]).start()

    def send_side(q, h, p, extra=0):
        own_copy(q, h, p, index(z, 1 - y, core), side_send.at[extra]).start()

    def half_of(q, h, p):
        return jnp.where(jnp.logical_not(is_end) & (q // 4 == depth - 1 - outward), p, h)

    def send_core(q, h, p, src=None):
        pltpu.make_async_remote_copy(
            src_ref=rows.at[q, h, p] if src is None else src, dst_ref=rows.at[q, h, p], send_sem=core_send.at[0],
            recv_sem=core_recv.at[q // 2, half_of(q, h, p)], device_id={"samp": index(z, y, 1 - core)},
            device_id_type=MESH).start()

    def send_core_span(q, h, p, span):
        span_copy(q, h, p, span, index(z, y, 1 - core), core_send.at[0], core_recv.at[q // 2, half_of(q, h, p)]).start()

    def arrive(q, h, p):
        await_bytes(rows.at[q, h, p], row_recv.at[q // 2, h, p])

    def arrive_core(q, half):
        await_bytes(rows.at[q, 0], core_recv.at[q // 2, half])

    def part_at(i):
        return lax.rem(part + i, groups)

    def send_own(h, p, skip=0):
        mine = panel.at[h, piece_of(part, p)]
        kept = panel.at[h, pl.ds(pl.multiple_of(part * tile_rows + p * piece_rows + skip, 16), piece_rows - skip)]
        kept_to = rows.at[me, h, p, pl.ds(skip, piece_rows - skip)]
        own_copy(me, h, p, index(z, 1 - y, core), side_send.at[0], kept, kept_to).start()
        own_copy(me, h, p, index(inward, y, core), line_send.at[0], kept, kept_to).start()

        @pl.when(jnp.logical_not(is_end))
        def _():
            own_copy(me, h, p, index(outward, y, core), line_send.at[2], kept, kept_to).start()

        send_core(me, h, p, mine)
        rows[me, h, p] = panel[h, piece_of(part, p), :]

    def scale_raw(slot, q):
        await_bytes(raw_in.at[slot], raw_sem.at[1 + slot])
        sent = raw_in[slot]
        rows[q, part, 0, 0:RAW, :] = jnp.where(sent >= 0.0, (sent - shift) * gain, 0.0).astype(jnp.bfloat16)

    def arrive_near(q, h, p):
        @pl.when((h == part) & (p == 0))
        def _():
            await_bytes(rows.at[q, h, p, pl.ds(RAW, piece_rows - RAW)], row_recv.at[q // 2, h, p])

        @pl.when((h != part) | (p != 0))
        def _():
            arrive(q, h, p)

    for p in range(PIECES):
        scale_piece(part, p)
        send_own(part, p, 0 if p else RAW)
        scale_piece(other, p)
        panel_copy(other, p).start()
    for p in range(PIECES):
        panel_copy(part, p).start()
    scale_raw(0, index(z, 1 - y, core))
    scale_raw(1, index(inward, y, core))

    @pl.when(jnp.logical_not(is_end))
    def _():
        scale_raw(2, index(outward, y, core))

    for p in range(PIECES):
        await_bytes(panel.at[other, piece_of(part, p)], across_recv.at[p])
        send_own(other, p)

    def form(at_z, at_y, parts=None, wait=True):
        def per_core(t, carry):
            q = index(at_z, at_y, lax.rem(core + t, 2))
            if wait:
                @pl.when(t == 1)
                def _():
                    for half in (range(2) if parts is None else parts):
                        arrive_core(q, half)

            tiles[q] = product(rows, panel, q, range(groups) if parts is None else parts)
            return carry

        lax.fori_loop(0, 2, per_core, 0)

    def await_panel():
        await_bytes(panel.at[other, pl.ds(pl.multiple_of(other * tile_rows, tile_rows), tile_rows)], across_recv.at[PIECES])

    def pick(i, values):
        chosen = values[-1]
        for n in range(len(values) - 2, -1, -1):
            chosen = jnp.where(i == n, values[n], chosen)
        return chosen

    count = groups * PIECES

    @pl.when(is_end)
    def _():
        far_mid = depth - 1 - inward

        def first(t, carry):
            h, p = part_at(t // PIECES), lax.rem(t, PIECES)
            near, beside = index(inward, y, core), index(z, 1 - y, core)
            arrive_near(near, h, p)
            send_side(near, h, p)
            send_core(near, h, p)
            arrive_near(beside, h, p)
            send_in(beside, h, p)
            send_core(beside, h, p)
            return carry

        lax.fori_loop(0, count, first, 0)
        await_panel()

        def second(t, carry):
            h, p = part_at(t // PIECES), lax.rem(t, PIECES)
            far, cross = index(far_mid, y, core), index(inward, 1 - y, core)
            arrive(far, h, p)
            to = index(z, 1 - y, core)

            @pl.when(t < count - 1)
            def _():
                send_side(far, h, p, extra=1)

            @pl.when(t == count - 1)
            def _():
                span_copy(far, h, p, head, to, side_send.at[1], row_recv.at[far // 2, h, p]).start()
                span_copy(far, h, p, rest, to, side_send.at[1], code_sem.at[4]).start()

            send_core(far, h, p)
            arrive(cross, h, p)
            send_core(cross, h, p)

            @pl.when(t < 3)
            def _():
                form(pick(t, (z, inward, z)), pick(t, (y, y, 1 - y)))

            return carry

        lax.fori_loop(0, count, second, 0)

        def third(t, carry):
            h, p = part_at(t // PIECES), lax.rem(t, PIECES)
            q = index(far_mid, 1 - y, core)

            @pl.when(t < count - 1)
            def _():
                arrive(q, h, p)
                send_core(q, h, p)

            @pl.when(t == count - 1)
            def _():
                await_bytes(rows.at[q, h, p, head], row_recv.at[q // 2, h, p])
                send_core_span(q, h, p, head)
                await_bytes(rows.at[q, h, p, rest], code_sem.at[4])
                send_core_span(q, h, p, rest)

            @pl.when(t < 2)
            def _():
                form(pick(t, (far_mid, inward)), pick(t, (y, 1 - y)))

            return carry

        lax.fori_loop(0, count, third, 0)
        form(far_mid, 1 - y, [part])
        await_bytes(codes, code_sem.at[1])
        await_bytes(steps, code_sem.at[3])
        arrive_core(index(far_mid, 1 - y, 1 - core), other)
        await_rows(2 * row_count - RAW, line_send.at[0])
        await_rows(2 * row_count - RAW, side_send.at[0])
        await_rows(count * piece_rows, side_send.at[1])
        await_bytes(raw_in.at[pl.ds(0, 2)], raw_sem.at[0])
        await_bytes(rows.at[pl.ds(0, 6)], core_send.at[0])

    @pl.when(jnp.logical_not(is_end))
    def _():
        far = depth - 1 - outward

        def first(t, carry):
            h, p = part_at(t // PIECES), lax.rem(t, PIECES)
            end, near, beside = index(outward, y, core), index(inward, y, core), index(z, 1 - y, core)
            arrive_near(end, h, p)

            @pl.when(p == 0)
            def _():
                send_in(end, h, 0)

            @pl.when(h == other)
            def _():
                send_in(end, jnp.where(p == 0, part, other), 1)

            send_core(end, h, p)
            column_copy(end, h, p).start()
            arrive_near(near, h, p)
            send_out(near, h, p)
            send_core(near, h, p)
            arrive_near(beside, h, p)
            send_core(beside, h, p)
            return carry

        lax.fori_loop(0, count, first, 0)
        for p in range(PIECES):
            send_in(index(z, 1 - y, core), part, p, extra=1)
        for h in range(groups):
            columns[part, h] = rows[index(outward, y, core), h].reshape(tile_rows, snp_count)
        await_panel()

        def code_copy(source, target, n):
            return pltpu.make_async_remote_copy(
                src_ref=source, dst_ref=target, send_sem=code_sem.at[n], recv_sem=code_sem.at[n + 1],
                device_id={"samp": index(outward, y, core)}, device_id_type=MESH)

        def make(side, p, k):
            def per_core(t, carry):
                which = lax.rem(core + t, 2)
                q = index(far, jnp.where(side == 0, y, 1 - y), which)
                term = None
                for h in range(groups):
                    one = lax.dot_general(rows[q, h, p], columns[k, h], (((1,), (1,)), ((), ())),
                                          preferred_element_type=jnp.float32)
                    term = one if term is None else term + one
                term = term * (1.0 / (groups * snp_count))
                top = jnp.max(jnp.abs(term), axis=0, keepdims=True)
                unit = ((side * 2 + which) * PIECES + p) * groups + k
                made[unit] = jnp.round(term * (CODE_TOP / jnp.maximum(top, TINY))).astype(jnp.int32).astype(jnp.int16)
                made_steps[unit] = top * (1.0 / CODE_TOP)
                code_copy(made.at[unit], codes.at[unit], 0).start()
                return carry

            lax.fori_loop(0, 2, per_core, 0)

        def far_core(side, p):
            arrive_core(index(far, jnp.where(side == 0, y, 1 - y), 1 - core), p)

        def make_list(listed):
            def per_entry(i, carry):
                side, p, away = (pick(i, [entry[n] for entry in listed]) for n in range(3))
                make(side, p, lax.rem(part + away, groups))
                return carry

            lax.fori_loop(0, len(listed), per_entry, 0)

        def second(t, carry):
            h, p = part_at(lax.rem(t, groups)), t // groups
            far_q, cross = index(far, y, core), index(outward, 1 - y, core)

            @pl.when(t >= 2)
            def _():
                far_core(t - 2, 0)
                make(t - 2, 0, part)

            arrive(far_q, h, p)
            send_side(far_q, h, p)
            send_core(far_q, h, p)
            ch, cp = part_at(t // PIECES), lax.rem(t, PIECES)
            arrive(cross, ch, cp)
            send_core(cross, ch, cp)

            @pl.when(t > 0)
            def _():
                q = index(far, 1 - y, core)
                h, p = part_at(lax.rem(t - 1, groups)), (t - 1) // groups
                arrive(q, h, p)
                send_core(q, h, p)

            form(pick(t, (z, outward, inward, z)), pick(t, (y, y, y, 1 - y)))
            return carry

        lax.fori_loop(0, count, second, 0)
        for p in range(PIECES):
            send_side(index(inward, y, core), other, p, extra=1)
        far_core(0, 1)
        make_list([(0, 1, 0)])
        await_bytes(columns.at[other], across_recv.at[PIECES + 1])
        make_list([(0, 0, 1), (0, 1, 1), (1, 0, 1)])
        form(outward, 1 - y)
        q = index(far, 1 - y, core)
        arrive(q, other, PIECES - 1)
        send_core(q, other, PIECES - 1)
        cross = index(inward, 1 - y, core)

        def third(t, carry):
            h, p = part_at(t // PIECES), lax.rem(t, PIECES)
            arrive(cross, h, p)
            send_core(cross, h, p)

            @pl.when(t == 1)
            def _():
                far_core(1, 1)
                make_list([(1, 1, 0), (1, 1, 1)])
                code_copy(made_steps, steps, 2).start()

            @pl.when(t < 2)
            def _():
                form(far, pick(t, (y, 1 - y)), wait=False)

            return carry

        lax.fori_loop(0, count, third, 0)
        form(inward, 1 - y)
        await_rows(2 * row_count - RAW, line_send.at[0])
        await_bytes(rows.at[0, 0], line_send.at[1])
        await_rows(2 * row_count - RAW, line_send.at[2])
        await_bytes(raw_in, raw_sem.at[0])
        await_rows(2 * row_count - RAW, side_send.at[0])
        await_bytes(rows.at[0, 0], side_send.at[1])
        await_bytes(rows.at[pl.ds(0, 8)], core_send.at[0])
        await_bytes(rows.at[0], across_send.at[1])
        await_bytes(made, code_sem.at[0])
        await_bytes(made_steps, code_sem.at[2])

    await_counts(0)
    await_bytes(rows.at[0], across_send.at[0])


def folded_body(shards, groups, genotypes, observed):
    row_count, snp_count = genotypes.shape
    tile_rows = row_count // groups
    piece_rows = tile_rows // PIECES
    units = 4 * PIECES * groups
    outs = (
        pltpu.VMEM((groups, row_count, snp_count), jnp.bfloat16),
        pltpu.VMEM((shards, groups, PIECES, piece_rows, snp_count), jnp.bfloat16),
        pltpu.VMEM((shards, tile_rows, row_count), jnp.float32),
        pltpu.VMEM((units, piece_rows, tile_rows), jnp.int16),
        pltpu.VMEM((units, 1, tile_rows), jnp.float32),
    )
    kept = sum(math.prod(o.shape) * jnp.dtype(o.dtype).itemsize for o in outs)
    held = pl.pallas_call(
        functools.partial(folded, shards, groups),
        out_shape=outs,
        in_specs=[pl.BlockSpec(memory_space=pltpu.HBM)] * 2,
        out_specs=[pl.BlockSpec(memory_space=pltpu.VMEM)] * 5,
        scratch_shapes=[
            pltpu.VMEM((row_count, snp_count), jnp.float32),
            pltpu.VMEM((row_count, snp_count), jnp.int32),
            pltpu.VMEM((shards, 1, snp_count), jnp.float32),
            pltpu.VMEM((shards, 2, snp_count // 2), jnp.int16),
            pltpu.VMEM((groups, groups, tile_rows, snp_count), jnp.bfloat16),
            pltpu.VMEM((units, piece_rows, tile_rows), jnp.int16),
            pltpu.VMEM((units, 1, tile_rows), jnp.float32),
            pltpu.VMEM((RAW, snp_count), jnp.float32),
            pltpu.VMEM((3, RAW, snp_count), jnp.float32),
            pltpu.SemaphoreType.DMA((2, LOADS)),
            pltpu.SemaphoreType.DMA((4,)),
            pltpu.SemaphoreType.DMA((2,)),
            pltpu.SemaphoreType.DMA((PIECES + 2,)),
            pltpu.SemaphoreType.DMA((3,)),
            pltpu.SemaphoreType.DMA((2,)),
            pltpu.SemaphoreType.DMA((1,)),
            pltpu.SemaphoreType.DMA((shards // 2, groups, PIECES)),
            pltpu.SemaphoreType.DMA((shards // 2, 2)),
            pltpu.SemaphoreType.DMA((5,)),
            pltpu.SemaphoreType.DMA((4,)),
        ],
        compiler_params=pltpu.CompilerParams(
            collective_id=0, has_side_effects=True, vmem_limit_bytes=VMEM_ALL - FOLDED_SPARE - kept),
    )(genotypes, observed)
    panel, rows, tiles, codes, steps = held
    return pl.pallas_call(
        functools.partial(folded_finish, shards, groups),
        out_shape=jax.ShapeDtypeStruct((shards, 1, tile_rows, row_count), jnp.float32),
        in_specs=[pl.BlockSpec(memory_space=pltpu.VMEM)] * 5,
        out_specs=pl.BlockSpec(memory_space=pltpu.HBM),
        scratch_shapes=[
            pltpu.VMEM((6, tile_rows, row_count), jnp.float32),
            pltpu.SemaphoreType.DMA((1,)),
        ],
        compiler_params=pltpu.CompilerParams(vmem_limit_bytes=FOLDED_FINISH),
    )(rows, panel, tiles, codes, steps)


def solution(mesh):
    shards, groups = mesh.shape["samp"], mesh.shape["snp"]

    def body(genotypes, observed):
        if groups == 2 and shards == 16:
            return folded_body(shards, groups, genotypes, observed)
        row_count, snp_count = genotypes.shape
        tile_rows = row_count // groups
        piece_rows = tile_rows // PIECES
        kept = 2 * (groups * row_count * snp_count) * (1 + shards // groups) + 4 * shards * tile_rows * row_count
        panel, rows, tiles = pl.pallas_call(
            functools.partial(kernel, shards, groups),
            out_shape=(
                pltpu.VMEM((groups, row_count, snp_count), jnp.bfloat16),
                pltpu.VMEM((shards, groups, PIECES, piece_rows, snp_count), jnp.bfloat16),
                pltpu.VMEM((shards, tile_rows, row_count), jnp.float32),
            ),
            in_specs=[pl.BlockSpec(memory_space=pltpu.HBM)] * 2,
            out_specs=[pl.BlockSpec(memory_space=pltpu.VMEM)] * 3,
            scratch_shapes=[
                pltpu.VMEM((row_count, snp_count), jnp.float32),
                pltpu.VMEM((row_count, snp_count), jnp.int32),
                pltpu.VMEM((shards, 2, snp_count), jnp.float32),
                pltpu.SemaphoreType.DMA((2, LOADS)),
                pltpu.SemaphoreType.DMA((shards,)),
                pltpu.SemaphoreType.DMA((shards,)),
                pltpu.SemaphoreType.DMA((groups, groups, PIECES)),
                pltpu.SemaphoreType.DMA((groups, groups, PIECES)),
                pltpu.SemaphoreType.DMA((4, shards, groups, PIECES)),
                pltpu.SemaphoreType.DMA((shards, groups, PIECES)),
            ],
            compiler_params=pltpu.CompilerParams(
                collective_id=0, has_side_effects=True, vmem_limit_bytes=VMEM_ALL - VMEM_SPARE - kept),
        )(genotypes, observed)
        return pl.pallas_call(
            functools.partial(finish, shards, groups),
            out_shape=jax.ShapeDtypeStruct((shards, 1, tile_rows, row_count), jnp.float32),
            in_specs=[pl.BlockSpec(memory_space=pltpu.VMEM)] * 3,
            out_specs=pl.BlockSpec(memory_space=pltpu.HBM),
            scratch_shapes=[
                pltpu.VMEM((4, tile_rows, row_count), jnp.float32),
                pltpu.SemaphoreType.DMA((shards,)),
            ],
            compiler_params=pltpu.CompilerParams(vmem_limit_bytes=VMEM_FINISH),
        )(rows, panel, tiles)

    return jax.shard_map(
        body,
        mesh=mesh,
        in_specs=(P("samp", "snp"), P("samp", "snp")),
        out_specs=P(None, "snp", None, "samp"),
        check_vma=False,
    )
```

```python
import functools
import math

import jax
import jax.numpy as jnp
from jax import lax
from jax.experimental import pallas as pl
from jax.experimental.pallas import tpu as pltpu
from jax.sharding import PartitionSpec as P

MESH = pl.DeviceIdType.MESH
var_floor = 0.1
UP, DOWN, SIDE, CORE = 0, 1, 2, 3
STRIP = 64
PIECES = 2
LOADS = 4
VMEM_ALL = 67043328
VMEM_SPARE = 512 * 1024
VMEM_FINISH = 12 * 1024 * 1024
FOLDED_SPARE = 1024 * 1024
FOLDED_FINISH = 8 * 1024 * 1024
CODE_TOP = 32767.0
TINY = 1e-30
RAW = 32


def index(at_z, at_y, at_core):
    return at_z * 4 + at_y * 2 + at_core


def source_at(z, depth, i):
    pairs = jnp.minimum(z, depth - 1 - z)
    side = jnp.where(i % 2 == 1, z - (i + 1) // 2, z + i // 2)
    far = jnp.where(z < depth - 1 - z, z + i - pairs, z - i + pairs)
    return jnp.where(i <= 2 * pairs, side, far)


def turned_at(z, depth):
    return jnp.where(z < depth - 1, z + 1, depth - 2)


def product(rows, panel, q, parts):
    pieces, piece_rows, snp_count = rows.shape[2:]
    total = None
    for h in parts:
        block = rows[q, h].reshape(pieces * piece_rows, snp_count)
        term = lax.dot_general(block, panel[h], (((1,), (1,)), ((), ())), preferred_element_type=jnp.float32)
        total = term if total is None else total + term
    return total * (1.0 / (rows.shape[1] * snp_count))


def finish(shards, groups, rows, panel, tiles, out_ref, late, out_sem):
    depth = shards // 4
    me = lax.axis_index("samp")
    z, y = me // 4, (me // 2) % 2
    turned = turned_at(z, depth)
    final = source_at(z, depth, depth - 1)
    final = jnp.where(final == turned, source_at(z, depth, depth - 2), final)
    last_part = lax.rem(lax.axis_index("snp") + groups - 1, groups)

    def is_late(q):
        return ((q // 4 == turned) | (q // 4 == final)) & ((q // 2) % 2 != y)

    def put(q, carry):
        @pl.when(jnp.logical_not(is_late(q)))
        def _():
            pltpu.make_async_copy(tiles.at[q], out_ref.at[q, 0], out_sem.at[q]).start()

        return carry

    lax.fori_loop(0, shards, put, 0)

    def form(i, carry):
        q = index(jnp.where(i // 2 == 0, final, turned), 1 - y, lax.rem(i, 2))
        late[i] = tiles[q] + product(rows, panel, q, [last_part])
        pltpu.make_async_copy(late.at[i], out_ref.at[q, 0], out_sem.at[q]).start()
        return carry

    lax.fori_loop(0, 4, form, 0)

    def flush(q, carry):
        pltpu.make_async_copy(tiles.at[q], out_ref.at[q, 0], out_sem.at[q]).wait()
        return carry

    lax.fori_loop(0, shards, flush, 0)


def kernel(shards, groups, geno_hbm, obs_hbm, panel, rows, tiles, geno_ref, obs_ref, counts, load_sem,
           count_send, count_recv, panel_send, panel_recv, row_send, row_recv):
    row_count, snp_count = geno_ref.shape
    tile_rows = row_count // groups
    piece_rows = tile_rows // PIECES
    depth = shards // 4
    me = lax.axis_index("samp")
    part = lax.axis_index("snp")
    z, y, core = me // 4, (me // 2) % 2, me % 2

    load_rows = row_count // LOADS

    def load(i):
        block = pl.ds(pl.multiple_of(i * load_rows, load_rows), load_rows)
        return (pltpu.make_async_copy(geno_hbm.at[block], geno_ref.at[block], load_sem.at[0, i]),
                pltpu.make_async_copy(obs_hbm.at[block], obs_ref.at[block], load_sem.at[1, i]))

    for i in range(LOADS):
        for copy in load(i):
            copy.start()

    barrier = pltpu.get_barrier_semaphore()
    for step in range(1, shards):
        pl.semaphore_signal(barrier, inc=1, device_id={"samp": lax.rem(me + step, shards)}, device_id_type=MESH)
    for step in range(1, groups):
        pl.semaphore_signal(barrier, inc=1, device_id={"snp": lax.rem(part + step, groups)}, device_id_type=MESH)

    def add_strip(i, total):
        alt, call = total
        strip = pl.ds(pl.multiple_of(i * STRIP, STRIP), STRIP)
        present = obs_ref[strip, :].astype(jnp.float32)
        held = present * geno_ref[strip, :]
        for r in range(0, STRIP, 8):
            alt = alt + held[r:r + 8]
            call = call + present[r:r + 8]
        return alt, call

    zero = jnp.zeros((8, snp_count), jnp.float32)
    alt, call = zero, zero
    strips = load_rows // STRIP
    for i in range(LOADS):
        for copy in load(i):
            copy.wait()
        alt, call = lax.fori_loop(i * strips, (i + 1) * strips, add_strip, (alt, call))
    counts[me, 0:1, :] = jnp.sum(alt, axis=0, keepdims=True)
    counts[me, 1:2, :] = jnp.sum(call, axis=0, keepdims=True)

    pl.semaphore_wait(barrier, shards + groups - 2)

    def count_copy(owner, to):
        return pltpu.make_async_remote_copy(
            src_ref=counts.at[owner], dst_ref=counts.at[owner], send_sem=count_send.at[to],
            recv_sem=count_recv.at[owner], device_id={"samp": to}, device_id_type=MESH)

    for step in range(1, shards):
        count_copy(me, lax.rem(me + step, shards)).start()
    for step in range(1, shards):
        other = lax.rem(me + step, shards)
        count_copy(other, other).wait_recv()
    sums = counts[0]
    for s in range(1, shards):
        sums = sums + counts[s]
    frequency = sums[0:1] / (2.0 * jnp.maximum(sums[1:2], 1.0))
    shift = 2.0 * frequency
    gain = lax.rsqrt(jnp.maximum(shift * (1.0 - frequency), var_floor))

    def piece_of(k, p):
        return pl.ds(pl.multiple_of(k * tile_rows + p * piece_rows, piece_rows), piece_rows)

    def panel_copy(h, k, to, p):
        block = panel.at[h, piece_of(k, p)]
        return pltpu.make_async_remote_copy(
            src_ref=block, dst_ref=block, send_sem=panel_send.at[to, k, p],
            recv_sem=panel_recv.at[h, k, p], device_id={"snp": to}, device_id_type=MESH)

    strip_rows = min(STRIP, piece_rows)

    def scale_piece(k, p):
        def scale_strip(i, carry):
            start = pl.multiple_of(k * tile_rows + p * piece_rows + i * strip_rows, strip_rows)
            strip = pl.ds(start, strip_rows)
            present = obs_ref[strip, :].astype(jnp.float32)
            panel[part, strip, :] = (present * (geno_ref[strip, :] - shift) * gain).astype(jnp.bfloat16)
            return carry

        lax.fori_loop(0, piece_rows // strip_rows, scale_strip, 0)

    def row_copy(q, h, p, way, src=None):
        to = (index(z + 1, y, core), index(z - 1, y, core), index(z, 1 - y, core), index(z, y, 1 - core))[way]
        return pltpu.make_async_remote_copy(
            src_ref=rows.at[q, h, p] if src is None else src, dst_ref=rows.at[q, h, p],
            send_sem=row_send.at[way, q, h, p], recv_sem=row_recv.at[q, h, p],
            device_id={"samp": to}, device_id_type=MESH)

    def arrive(q, h, p):
        row_copy(q, h, p, CORE).wait_recv()

    last_part = lax.rem(part + groups - 1, groups)
    turned = turned_at(z, depth)

    def part_at(i):
        return lax.rem(part + i, groups)

    def send_own(h, p):
        mine = panel.at[h, piece_of(part, p)]
        row_copy(me, h, p, SIDE, mine).start()

        @pl.when(z < depth - 1)
        def _():
            row_copy(me, h, p, UP, mine).start()

        @pl.when(z > 0)
        def _():
            row_copy(me, h, p, DOWN, mine).start()

        row_copy(me, h, p, CORE, mine).start()
        rows[me, h, p] = panel[h, piece_of(part, p), :]

    for p in range(PIECES):
        for step in range(1, groups):
            other = part_at(step)
            scale_piece(other, p)
            panel_copy(part, other, other, p).start()
        scale_piece(part, p)
        send_own(part, p)
    for step in range(1, groups):
        other = part_at(step)
        for k in range(1, groups):
            for p in range(PIECES):
                panel_copy(part, lax.rem(other + k, groups), other, p).start()
    for step in range(1, groups):
        h = part_at(step)
        for p in range(PIECES):
            panel_copy(h, part, h, p).wait_recv()
            send_own(h, p)

    def column_arrival(at_z, h, p, way):
        q = index(at_z, y, core)
        arrive(q, h, p)

        @pl.when(z < depth - 1 if way == UP else z > 0)
        def _():
            row_copy(q, h, p, way).start()

        @pl.when((at_z != turned) | (h != last_part))
        def _():
            row_copy(q, h, p, SIDE).start()

        row_copy(q, h, p, CORE).start()

    def column_arrivals(i):
        def per_piece(t, carry):
            h, p = part_at(t // PIECES), lax.rem(t, PIECES)

            @pl.when(z - i >= 0)
            def _():
                column_arrival(z - i, h, p, UP)

            @pl.when(z + i < depth)
            def _():
                column_arrival(z + i, h, p, DOWN)

            return carry

        lax.fori_loop(0, groups * PIECES, per_piece, 0)

    def arrive_all(q):
        def per_piece(t, carry):
            arrive(q, t // PIECES, lax.rem(t, PIECES))
            return carry

        lax.fori_loop(0, groups * PIECES, per_piece, 0)

    def products(at_z, at_y):
        def per_core(t, carry):
            q = index(at_z, at_y, lax.rem(core + t, 2))

            @pl.when(t == 1)
            def _():
                arrive_all(q)

            tiles[q] = product(rows, panel, q, range(groups))
            return carry

        lax.fori_loop(0, 2, per_core, 0)

    def side_arrival(at_z, h, p):
        q = index(at_z, 1 - y, core)
        arrive(q, h, p)
        row_copy(q, h, p, CORE).start()

    final = source_at(z, depth, depth - 1)
    final = jnp.where(final == turned, source_at(z, depth, depth - 2), final)

    def begin_late():
        def per_tile(t, carry):
            q = index(jnp.where(t % 2 == 0, turned, final), 1 - y, lax.rem(core + t // 2, 2))

            @pl.when(t >= 2)
            def _():
                for step in range(groups - 1):
                    for p in range(PIECES):
                        arrive(q, part_at(step), p)

            tiles[q] = product(rows, panel, q, [part_at(step) for step in range(groups - 1)])
            return carry

        lax.fori_loop(0, 4, per_tile, 0)

    def round_of(i, carry):
        @pl.when(i < depth)
        def _():
            column_arrivals(i)

        @pl.when(i == 1)
        def _():
            for step in range(1, groups):
                h = part_at(step)
                for k in range(1, groups):
                    for p in range(PIECES):
                        panel_copy(h, part_at(k), h, p).wait_recv()

        @pl.when(i == depth - 1)
        def _():
            q = index(z, 1 - y, core)

            @pl.when(z > 0)
            def _():
                for p in range(PIECES):
                    row_copy(q, last_part, p, DOWN).start()

            @pl.when(z == depth - 2)
            def _():
                for p in range(PIECES):
                    row_copy(q, last_part, p, UP).start()

        at_z = source_at(z, depth, i - 1)
        products(at_z, y)

        def per_piece(t, c):
            @pl.when((i == depth) & (t == (groups - 1) * PIECES))
            def _():
                begin_late()

            @pl.when((at_z != turned) | (t // PIECES != groups - 1))
            def _():
                side_arrival(at_z, part_at(t // PIECES), lax.rem(t, PIECES))

            return c

        lax.fori_loop(0, groups * PIECES, per_piece, 0)

        @pl.when((at_z != turned) & (at_z != final))
        def _():
            products(at_z, 1 - y)

        return carry

    lax.fori_loop(1, depth + 1, round_of, 0)
    for p in range(PIECES):
        side_arrival(turned, last_part, p)
    for p in range(PIECES):
        arrive(index(final, 1 - y, 1 - core), last_part, p)
        arrive(index(turned, 1 - y, 1 - core), last_part, p)

    for step in range(1, shards):
        count_copy(me, lax.rem(me + step, shards)).wait_send()
    for step in range(1, groups):
        for k in range(groups):
            for p in range(PIECES):
                panel_copy(part, k, part_at(step), p).wait_send()

    def drain(i, carry):
        at_z, h, p = i // (groups * PIECES), lax.rem(i // PIECES, groups), lax.rem(i, PIECES)
        q = index(at_z, y, core)
        across = index(at_z, 1 - y, core)

        @pl.when((at_z <= z) & (z < depth - 1))
        def _():
            row_copy(q, h, p, UP).wait_send()

        @pl.when((at_z >= z) & (z > 0))
        def _():
            row_copy(q, h, p, DOWN).wait_send()

        @pl.when((at_z != turned) | (h != last_part))
        def _():
            row_copy(q, h, p, SIDE).wait_send()

        row_copy(q, h, p, CORE).wait_send()
        row_copy(across, h, p, CORE).wait_send()

        @pl.when((at_z == z) & (h == last_part) & (z > 0))
        def _():
            row_copy(across, h, p, DOWN).wait_send()

        @pl.when((at_z == z) & (h == last_part) & (z == depth - 2))
        def _():
            row_copy(across, h, p, UP).wait_send()

        return carry

    lax.fori_loop(0, depth * groups * PIECES, drain, 0)


def shape_of_line(depth):
    z = lax.axis_index("samp") // 4
    low = z < depth // 2
    inward = jnp.where(low, z + 1, z - 1)
    outward = jnp.clip(jnp.where(low, z - 1, z + 1), 0, depth - 1)
    is_end = (z == 0) | (z == depth - 1)
    return z, inward, outward, is_end


def folded_finish(shards, groups, rows, panel, tiles, codes, steps, out_ref, late, out_sem):
    depth = shards // 4
    me = lax.axis_index("samp")
    y = (me // 2) % 2
    z, inward, outward, is_end = shape_of_line(depth)
    far_mid, far_end = depth - 1 - inward, depth - 1 - z
    last_part = lax.rem(lax.axis_index("snp") + groups - 1, groups)
    piece_rows = rows.shape[3]
    tile_rows = PIECES * piece_rows

    def is_late(q):
        return is_end & ((q // 4 == far_end) | ((q // 4 == far_mid) & ((q // 2) % 2 != y)))

    def put(q, carry):
        @pl.when(jnp.logical_not(is_late(q)))
        def _():
            pltpu.make_async_copy(tiles.at[q], out_ref.at[q, 0], out_sem.at[0]).start()

        return carry

    lax.fori_loop(0, shards, put, 0)

    @pl.when(is_end)
    def _():
        def decode(t, carry):
            for p in range(PIECES):
                for k in range(groups):
                    unit = (t * PIECES + p) * groups + k
                    late[t, p * piece_rows:(p + 1) * piece_rows, k * tile_rows:(k + 1) * tile_rows] = (
                        codes[unit].astype(jnp.float32) * steps[unit])
            q = index(far_end, jnp.where(t // 2 == 0, y, 1 - y), lax.rem(t, 2))
            pltpu.make_async_copy(late.at[t], out_ref.at[q, 0], out_sem.at[0]).start()
            return carry

        lax.fori_loop(0, 4, decode, 0)

        def form(i, carry):
            q = index(far_mid, 1 - y, i)
            late[4 + i] = tiles[q] + product(rows, panel, q, [last_part])
            pltpu.make_async_copy(late.at[4 + i], out_ref.at[q, 0], out_sem.at[0]).start()
            return carry

        lax.fori_loop(0, 2, form, 0)

    pltpu.make_async_copy(tiles, out_ref.at[:, 0], out_sem.at[0]).wait()


def folded(shards, groups, geno_hbm, obs_hbm, panel, rows, tiles, codes, steps, geno_ref, obs_ref, alts, calls, columns,
           made, made_steps, raw, raw_in, load_sem, count_sem, across_send, across_recv, line_send, side_send, core_send, row_recv,
           core_recv, code_sem, raw_sem):
    row_count, snp_count = geno_ref.shape
    tile_rows = row_count // groups
    piece_rows = tile_rows // PIECES
    depth = shards // 4
    me = lax.axis_index("samp")
    part = lax.axis_index("snp")
    y, core = (me // 2) % 2, me % 2
    z, inward, outward, is_end = shape_of_line(depth)
    other = lax.rem(part + 1, groups)
    load_rows = row_count // LOADS

    def load(i):
        block = pl.ds(pl.multiple_of(i * load_rows, load_rows), load_rows)
        return (pltpu.make_async_copy(geno_hbm.at[block], geno_ref.at[block], load_sem.at[i]),
                pltpu.make_async_copy(obs_hbm.at[block], obs_ref.at[block], load_sem.at[i]))

    for i in range(LOADS):
        for copy in load(i):
            copy.start()

    barrier = pltpu.get_barrier_semaphore()
    for step in range(1, shards):
        pl.semaphore_signal(barrier, inc=1, device_id={"samp": lax.rem(me + step, shards)}, device_id_type=MESH)
    pl.semaphore_signal(barrier, inc=1, device_id={"snp": other}, device_id_type=MESH)

    def add_strip(i, total):
        alt, call = total
        strip = pl.ds(pl.multiple_of(i * STRIP, STRIP), STRIP)
        present = obs_ref[strip, :].astype(jnp.float32)
        held = present * geno_ref[strip, :]
        for r in range(0, STRIP, 8):
            alt = alt + held[r:r + 8]
            call = call + present[r:r + 8]
        return alt, call

    zero = jnp.zeros((8, snp_count), jnp.float32)
    alt, call = zero, zero
    strips = load_rows // STRIP
    for i in range(LOADS):
        loaded = geno_ref.at[pl.ds(0, 2 * load_rows)]
        pltpu.make_async_copy(loaded, loaded, load_sem.at[i]).wait()
        alt, call = lax.fori_loop(i * strips, (i + 1) * strips, add_strip, (alt, call))
    alts[me] = jnp.sum(alt, axis=0, keepdims=True)
    call = jnp.sum(call, axis=0, keepdims=True).astype(jnp.int32)
    half = snp_count // 2
    calls[me] = jnp.concatenate([call[:, :half], call[:, half:]]).astype(jnp.int16)

    pl.semaphore_wait(barrier, shards)

    for step in range(shards):
        to = jnp.where(z < depth // 2, shards - 1 - step, step)

        @pl.when(to != me)
        def _():
            for n, sent in enumerate((alts, calls)):
                pltpu.make_async_remote_copy(
                    src_ref=sent.at[me], dst_ref=sent.at[me], send_sem=count_sem.at[2 * n],
                    recv_sem=count_sem.at[2 * n + 1], device_id={"samp": to}, device_id_type=MESH).start()

    def await_bytes(ref, sem):
        pltpu.make_async_copy(ref, ref, sem).wait()

    def await_rows(count, sem):
        await_bytes(geno_ref.at[pl.ds(0, count // 2)], sem)

    def raw_copy(to, slot):
        return pltpu.make_async_remote_copy(
            src_ref=raw, dst_ref=raw_in.at[slot], send_sem=raw_sem.at[0], recv_sem=raw_sem.at[1 + slot],
            device_id={"samp": to}, device_id_type=MESH)

    early = pl.ds(pl.multiple_of(part * tile_rows, tile_rows), RAW)
    raw[...] = jnp.where(obs_ref[early, :] > 0, geno_ref[early, :], -1.0)
    raw_copy(index(z, 1 - y, core), 0).start()
    raw_copy(index(inward, y, core), jnp.where(is_end, 2, 1)).start()

    @pl.when(jnp.logical_not(is_end))
    def _():
        raw_copy(index(outward, y, core), 1).start()

    def await_counts(way):
        for n, sent in enumerate((alts, calls)):
            await_bytes(sent.at[pl.ds(0, shards - 1)], count_sem.at[2 * n + way])

    await_counts(1)
    alt, call = alts[0], calls[0].astype(jnp.int32)
    for s in range(1, shards):
        alt, call = alt + alts[s], call + calls[s].astype(jnp.int32)
    call = jnp.concatenate([call[0:1], call[1:2]], axis=1).astype(jnp.float32)
    frequency = alt / (2.0 * jnp.maximum(call, 1.0))
    shift = 2.0 * frequency
    gain = lax.rsqrt(jnp.maximum(shift * (1.0 - frequency), var_floor))

    def piece_of(k, p):
        return pl.ds(pl.multiple_of(k * tile_rows + p * piece_rows, piece_rows), piece_rows)

    strip_rows = min(STRIP, piece_rows)

    def scale_piece(k, p):
        def scale_strip(i, carry):
            start = pl.multiple_of(k * tile_rows + p * piece_rows + i * strip_rows, strip_rows)
            strip = pl.ds(start, strip_rows)
            present = obs_ref[strip, :].astype(jnp.float32)
            panel[part, strip, :] = (present * (geno_ref[strip, :] - shift) * gain).astype(jnp.bfloat16)
            return carry

        lax.fori_loop(0, piece_rows // strip_rows, scale_strip, 0)

    def panel_copy(k, p):
        block = panel.at[part, piece_of(k, p)]
        return pltpu.make_async_remote_copy(
            src_ref=block, dst_ref=block, send_sem=across_send.at[0],
            recv_sem=across_recv.at[jnp.where(k == part, PIECES, p)], device_id={"snp": other}, device_id_type=MESH)

    def column_copy(q, h, p):
        return pltpu.make_async_remote_copy(
            src_ref=rows.at[q, h, p], dst_ref=columns.at[part, h, pl.ds(pl.multiple_of(p * piece_rows, piece_rows), piece_rows)],
            send_sem=across_send.at[1], recv_sem=across_recv.at[PIECES + 1], device_id={"snp": other}, device_id_type=MESH)

    cut = piece_rows * 7 // 8
    head, rest = pl.ds(0, cut), pl.ds(cut, piece_rows - cut)

    def span_copy(q, h, p, span, to, send_sem, recv_sem):
        return pltpu.make_async_remote_copy(
            src_ref=rows.at[q, h, p, span], dst_ref=rows.at[q, h, p, span], send_sem=send_sem, recv_sem=recv_sem,
            device_id={"samp": to}, device_id_type=MESH)

    def slot_of(q, at):
        return lax.rem(q // 2 - at // 2 + shards // 2, shards // 2) - 1

    def own_copy(q, h, p, to, send_sem, src=None, dst=None):
        return pltpu.make_async_remote_copy(
            src_ref=rows.at[q, h, p] if src is None else src, dst_ref=rows.at[q, h, p] if dst is None else dst,
            send_sem=send_sem,
            recv_sem=row_recv.at[slot_of(q, to), h, p], device_id={"samp": to}, device_id_type=MESH)

    def send_in(q, h, p, extra=0):
        own_copy(q, h, p, index(inward, y, core), line_send.at[extra]).start()

    def send_out(q, h, p):
        own_copy(q, h, p, index(outward, y, core), line_send.at[2]).start()

    def send_side(q, h, p, extra=0):
        own_copy(q, h, p, index(z, 1 - y, core), side_send.at[extra]).start()

    def core_slot(q, h, p):
        late = jnp.where(is_end, (q // 2 == (depth - 1 - inward) * 2 + 1 - y) & (h != part),
                         (q // 4 == depth - 1 - outward) & (p == 1))
        return jnp.where(late, late_slot(q), q // 2)

    def late_slot(q):
        return shards // 2 + lax.rem(q // 2, 2)

    def send_core(q, h, p, src=None):
        pltpu.make_async_remote_copy(
            src_ref=rows.at[q, h, p] if src is None else src, dst_ref=rows.at[q, h, p], send_sem=core_send.at[0],
            recv_sem=core_recv.at[core_slot(q, h, p)], device_id={"samp": index(z, y, 1 - core)},
            device_id_type=MESH).start()

    def send_core_span(q, h, p, span):
        span_copy(q, h, p, span, index(z, y, 1 - core), core_send.at[0], core_recv.at[core_slot(q, h, p)]).start()

    def arrive(q, h, p):
        await_bytes(rows.at[q, h, p], row_recv.at[slot_of(q, me), h, p])

    def arrive_core(q, late):
        await_bytes(rows.at[q, 0], core_recv.at[late_slot(q) if late else q // 2])

    def part_at(i):
        return lax.rem(part + i, groups)

    def send_own(h, p, skip=0):
        mine = panel.at[h, piece_of(part, p)]
        kept = panel.at[h, pl.ds(pl.multiple_of(part * tile_rows + p * piece_rows + skip, 16), piece_rows - skip)]
        kept_to = rows.at[me, h, p, pl.ds(skip, piece_rows - skip)]
        own_copy(me, h, p, index(z, 1 - y, core), side_send.at[0], kept, kept_to).start()
        own_copy(me, h, p, index(inward, y, core), line_send.at[0], kept, kept_to).start()

        @pl.when(jnp.logical_not(is_end))
        def _():
            own_copy(me, h, p, index(outward, y, core), line_send.at[2], kept, kept_to).start()

        send_core(me, h, p, mine)
        rows[me, h, p] = panel[h, piece_of(part, p), :]

    def scale_raw(slot, q):
        await_bytes(raw_in.at[slot], raw_sem.at[1 + slot])
        sent = raw_in[slot]
        rows[q, part, 0, 0:RAW, :] = jnp.where(sent >= 0.0, (sent - shift) * gain, 0.0).astype(jnp.bfloat16)

    def arrive_near(q, h, p):
        @pl.when((h == part) & (p == 0))
        def _():
            await_bytes(rows.at[q, h, p, pl.ds(RAW, piece_rows - RAW)], row_recv.at[slot_of(q, me), h, p])

        @pl.when((h != part) | (p != 0))
        def _():
            arrive(q, h, p)

    for p in range(PIECES):
        scale_piece(part, p)
        send_own(part, p, 0 if p else RAW)
        scale_piece(other, p)
        panel_copy(other, p).start()
    for p in range(PIECES):
        panel_copy(part, p).start()
    scale_raw(0, index(z, 1 - y, core))
    scale_raw(1, index(inward, y, core))

    @pl.when(jnp.logical_not(is_end))
    def _():
        scale_raw(2, index(outward, y, core))

    for p in range(PIECES):
        await_bytes(panel.at[other, piece_of(part, p)], across_recv.at[p])
        send_own(other, p)

    def form(at_z, at_y, parts=None, wait=True):
        def per_core(t, carry):
            q = index(at_z, at_y, lax.rem(core + t, 2))
            if wait:
                @pl.when(t == 1)
                def _():
                    if parts is None:
                        await_bytes(rows.at[q], core_recv.at[q // 2])
                    else:
                        arrive_core(q, False)

            tiles[q] = product(rows, panel, q, range(groups) if parts is None else parts)
            return carry

        lax.fori_loop(0, 2, per_core, 0)

    def await_panel():
        await_bytes(panel.at[other, pl.ds(pl.multiple_of(other * tile_rows, tile_rows), tile_rows)], across_recv.at[PIECES])

    def pick(i, values):
        chosen = values[-1]
        for n in range(len(values) - 2, -1, -1):
            chosen = jnp.where(i == n, values[n], chosen)
        return chosen

    count = groups * PIECES

    @pl.when(is_end)
    def _():
        far_mid = depth - 1 - inward

        def first(t, carry):
            h, p = part_at(t // PIECES), lax.rem(t, PIECES)
            near, beside = index(inward, y, core), index(z, 1 - y, core)
            arrive_near(near, h, p)
            send_side(near, h, p)
            send_core(near, h, p)
            arrive_near(beside, h, p)
            send_in(beside, h, p)
            send_core(beside, h, p)
            return carry

        lax.fori_loop(0, count, first, 0)
        await_panel()

        def second(t, carry):
            h, p = part_at(t // PIECES), lax.rem(t, PIECES)
            far, cross = index(far_mid, y, core), index(inward, 1 - y, core)
            arrive(far, h, p)
            to = index(z, 1 - y, core)

            @pl.when(t < count - 1)
            def _():
                send_side(far, h, p, extra=1)

            @pl.when(t == count - 1)
            def _():
                span_copy(far, h, p, head, to, side_send.at[1], row_recv.at[slot_of(far, to), h, p]).start()
                span_copy(far, h, p, rest, to, side_send.at[1], code_sem.at[4]).start()

            send_core(far, h, p)
            arrive(cross, h, p)
            send_core(cross, h, p)

            @pl.when(t < 3)
            def _():
                form(pick(t, (z, inward, z)), pick(t, (y, y, 1 - y)))

            return carry

        lax.fori_loop(0, count, second, 0)

        def third(t, carry):
            h, p = part_at(t // PIECES), lax.rem(t, PIECES)
            q = index(far_mid, 1 - y, core)

            @pl.when(t < count - 1)
            def _():
                arrive(q, h, p)
                send_core(q, h, p)

            @pl.when(t == count - 1)
            def _():
                await_bytes(rows.at[q, h, p, head], row_recv.at[slot_of(q, me), h, p])
                send_core_span(q, h, p, head)
                await_bytes(rows.at[q, h, p, rest], code_sem.at[4])
                send_core_span(q, h, p, rest)

            @pl.when(t < 2)
            def _():
                form(pick(t, (far_mid, inward)), pick(t, (y, 1 - y)))

            @pl.when(t == 2)
            def _():
                form(far_mid, 1 - y, [part])

            return carry

        lax.fori_loop(0, count, third, 0)
        await_bytes(codes, code_sem.at[1])
        await_bytes(steps, code_sem.at[3])
        arrive_core(index(far_mid, 1 - y, 1 - core), True)
        await_rows(2 * row_count - RAW, line_send.at[0])
        await_rows(2 * row_count - RAW, side_send.at[0])
        await_rows(count * piece_rows, side_send.at[1])
        await_bytes(raw_in.at[pl.ds(0, 2)], raw_sem.at[0])
        await_bytes(rows.at[pl.ds(0, 6)], core_send.at[0])

    @pl.when(jnp.logical_not(is_end))
    def _():
        far = depth - 1 - outward

        def first(t, carry):
            h, p = part_at(t // PIECES), lax.rem(t, PIECES)
            end, near, beside = index(outward, y, core), index(inward, y, core), index(z, 1 - y, core)
            arrive_near(end, h, p)

            @pl.when(p == 0)
            def _():
                send_in(end, h, 0)

            @pl.when(h == other)
            def _():
                send_in(end, jnp.where(p == 0, part, other), 1)

            send_core(end, h, p)
            column_copy(end, h, p).start()
            arrive_near(near, h, p)
            send_out(near, h, p)
            send_core(near, h, p)
            arrive_near(beside, h, p)
            send_core(beside, h, p)
            return carry

        lax.fori_loop(0, count, first, 0)
        for p in range(PIECES):
            send_in(index(z, 1 - y, core), part, p, extra=1)
        for h in range(groups):
            columns[part, h] = rows[index(outward, y, core), h].reshape(tile_rows, snp_count)
        await_panel()

        def code_copy(source, target, n):
            return pltpu.make_async_remote_copy(
                src_ref=source, dst_ref=target, send_sem=code_sem.at[n], recv_sem=code_sem.at[n + 1],
                device_id={"samp": index(outward, y, core)}, device_id_type=MESH)

        def make(side, p, k):
            def per_core(t, carry):
                which = lax.rem(core + t, 2)
                q = index(far, jnp.where(side == 0, y, 1 - y), which)
                term = None
                for h in range(groups):
                    one = lax.dot_general(rows[q, h, p], columns[k, h], (((1,), (1,)), ((), ())),
                                          preferred_element_type=jnp.float32)
                    term = one if term is None else term + one
                term = term * (1.0 / (groups * snp_count))
                top = jnp.max(jnp.abs(term), axis=0, keepdims=True)
                unit = ((side * 2 + which) * PIECES + p) * groups + k
                made[unit] = jnp.round(term * (CODE_TOP / jnp.maximum(top, TINY))).astype(jnp.int32).astype(jnp.int16)
                made_steps[unit] = top * (1.0 / CODE_TOP)
                code_copy(made.at[unit], codes.at[unit], 0).start()
                return carry

            lax.fori_loop(0, 2, per_core, 0)

        def far_core(side, p):
            arrive_core(index(far, jnp.where(side == 0, y, 1 - y), 1 - core), p == 1)

        def make_list(listed):
            def per_entry(i, carry):
                side, p, away = (pick(i, [entry[n] for entry in listed]) for n in range(3))
                make(side, p, lax.rem(part + away, groups))
                return carry

            lax.fori_loop(0, len(listed), per_entry, 0)

        def second(t, carry):
            h, p = part_at(lax.rem(t, groups)), t // groups
            far_q, cross = index(far, y, core), index(outward, 1 - y, core)

            @pl.when(t >= 2)
            def _():
                far_core(t - 2, 0)
                make(t - 2, 0, part)

            arrive(far_q, h, p)
            send_side(far_q, h, p)
            send_core(far_q, h, p)
            ch, cp = part_at(t // PIECES), lax.rem(t, PIECES)
            arrive(cross, ch, cp)
            send_core(cross, ch, cp)

            @pl.when(t > 0)
            def _():
                q = index(far, 1 - y, core)
                h, p = part_at(lax.rem(t - 1, groups)), (t - 1) // groups
                arrive(q, h, p)
                send_core(q, h, p)

            form(pick(t, (z, outward, inward, z)), pick(t, (y, y, y, 1 - y)))
            return carry

        lax.fori_loop(0, count, second, 0)
        for p in range(PIECES):
            send_side(index(inward, y, core), other, p, extra=1)
        far_core(0, 1)
        make_list([(0, 1, 0)])
        await_bytes(columns.at[other], across_recv.at[PIECES + 1])
        make_list([(0, 0, 1), (0, 1, 1), (1, 0, 1)])
        form(outward, 1 - y)
        q = index(far, 1 - y, core)
        arrive(q, other, PIECES - 1)
        send_core(q, other, PIECES - 1)
        cross = index(inward, 1 - y, core)

        def third(t, carry):
            h, p = part_at(t // PIECES), lax.rem(t, PIECES)
            arrive(cross, h, p)
            send_core(cross, h, p)

            @pl.when(t == 1)
            def _():
                far_core(1, 1)
                make_list([(1, 1, 0), (1, 1, 1)])
                code_copy(made_steps, steps, 2).start()

            @pl.when(t < 2)
            def _():
                form(far, pick(t, (y, 1 - y)), wait=False)

            return carry

        lax.fori_loop(0, count, third, 0)
        form(inward, 1 - y)
        await_rows(2 * row_count - RAW, line_send.at[0])
        await_bytes(rows.at[0, 0], line_send.at[1])
        await_rows(2 * row_count - RAW, line_send.at[2])
        await_bytes(raw_in, raw_sem.at[0])
        await_rows(2 * row_count - RAW, side_send.at[0])
        await_bytes(rows.at[0, 0], side_send.at[1])
        await_bytes(rows.at[pl.ds(0, 8)], core_send.at[0])
        await_bytes(rows.at[0], across_send.at[1])
        await_bytes(made, code_sem.at[0])
        await_bytes(made_steps, code_sem.at[2])

    await_counts(0)
    await_bytes(rows.at[0], across_send.at[0])


def folded_body(shards, groups, genotypes, observed):
    row_count, snp_count = genotypes.shape
    tile_rows = row_count // groups
    piece_rows = tile_rows // PIECES
    units = 4 * PIECES * groups
    outs = (
        pltpu.VMEM((groups, row_count, snp_count), jnp.bfloat16),
        pltpu.VMEM((shards, groups, PIECES, piece_rows, snp_count), jnp.bfloat16),
        pltpu.VMEM((shards, tile_rows, row_count), jnp.float32),
        pltpu.VMEM((units, piece_rows, tile_rows), jnp.int16),
        pltpu.VMEM((units, 1, tile_rows), jnp.float32),
    )
    kept = sum(math.prod(o.shape) * jnp.dtype(o.dtype).itemsize for o in outs)
    held = pl.pallas_call(
        functools.partial(folded, shards, groups),
        out_shape=outs,
        in_specs=[pl.BlockSpec(memory_space=pltpu.HBM)] * 2,
        out_specs=[pl.BlockSpec(memory_space=pltpu.VMEM)] * 5,
        scratch_shapes=[
            pltpu.VMEM((row_count, snp_count), jnp.float32),
            pltpu.VMEM((row_count, snp_count), jnp.int32),
            pltpu.VMEM((shards, 1, snp_count), jnp.float32),
            pltpu.VMEM((shards, 2, snp_count // 2), jnp.int16),
            pltpu.VMEM((groups, groups, tile_rows, snp_count), jnp.bfloat16),
            pltpu.VMEM((units, piece_rows, tile_rows), jnp.int16),
            pltpu.VMEM((units, 1, tile_rows), jnp.float32),
            pltpu.VMEM((RAW, snp_count), jnp.float32),
            pltpu.VMEM((3, RAW, snp_count), jnp.float32),
            pltpu.SemaphoreType.DMA((LOADS,)),
            pltpu.SemaphoreType.DMA((4,)),
            pltpu.SemaphoreType.DMA((2,)),
            pltpu.SemaphoreType.DMA((PIECES + 2,)),
            pltpu.SemaphoreType.DMA((3,)),
            pltpu.SemaphoreType.DMA((2,)),
            pltpu.SemaphoreType.DMA((1,)),
            pltpu.SemaphoreType.DMA((shards // 2 - 1, groups, PIECES)),
            pltpu.SemaphoreType.DMA((shards // 2 + 2,)),
            pltpu.SemaphoreType.DMA((5,)),
            pltpu.SemaphoreType.DMA((4,)),
        ],
        compiler_params=pltpu.CompilerParams(
            collective_id=0, has_side_effects=True, vmem_limit_bytes=VMEM_ALL - FOLDED_SPARE - kept),
    )(genotypes, observed)
    panel, rows, tiles, codes, steps = held
    return pl.pallas_call(
        functools.partial(folded_finish, shards, groups),
        out_shape=jax.ShapeDtypeStruct((shards, 1, tile_rows, row_count), jnp.float32),
        in_specs=[pl.BlockSpec(memory_space=pltpu.VMEM)] * 5,
        out_specs=pl.BlockSpec(memory_space=pltpu.HBM),
        scratch_shapes=[
            pltpu.VMEM((6, tile_rows, row_count), jnp.float32),
            pltpu.SemaphoreType.DMA((1,)),
        ],
        compiler_params=pltpu.CompilerParams(vmem_limit_bytes=FOLDED_FINISH),
    )(rows, panel, tiles, codes, steps)


def solution(mesh):
    shards, groups = mesh.shape["samp"], mesh.shape["snp"]

    def body(genotypes, observed):
        if groups == 2 and shards == 16:
            return folded_body(shards, groups, genotypes, observed)
        row_count, snp_count = genotypes.shape
        tile_rows = row_count // groups
        piece_rows = tile_rows // PIECES
        kept = 2 * (groups * row_count * snp_count) * (1 + shards // groups) + 4 * shards * tile_rows * row_count
        panel, rows, tiles = pl.pallas_call(
            functools.partial(kernel, shards, groups),
            out_shape=(
                pltpu.VMEM((groups, row_count, snp_count), jnp.bfloat16),
                pltpu.VMEM((shards, groups, PIECES, piece_rows, snp_count), jnp.bfloat16),
                pltpu.VMEM((shards, tile_rows, row_count), jnp.float32),
            ),
            in_specs=[pl.BlockSpec(memory_space=pltpu.HBM)] * 2,
            out_specs=[pl.BlockSpec(memory_space=pltpu.VMEM)] * 3,
            scratch_shapes=[
                pltpu.VMEM((row_count, snp_count), jnp.float32),
                pltpu.VMEM((row_count, snp_count), jnp.int32),
                pltpu.VMEM((shards, 2, snp_count), jnp.float32),
                pltpu.SemaphoreType.DMA((2, LOADS)),
                pltpu.SemaphoreType.DMA((shards,)),
                pltpu.SemaphoreType.DMA((shards,)),
                pltpu.SemaphoreType.DMA((groups, groups, PIECES)),
                pltpu.SemaphoreType.DMA((groups, groups, PIECES)),
                pltpu.SemaphoreType.DMA((4, shards, groups, PIECES)),
                pltpu.SemaphoreType.DMA((shards, groups, PIECES)),
            ],
            compiler_params=pltpu.CompilerParams(
                collective_id=0, has_side_effects=True, vmem_limit_bytes=VMEM_ALL - VMEM_SPARE - kept),
        )(genotypes, observed)
        return pl.pallas_call(
            functools.partial(finish, shards, groups),
            out_shape=jax.ShapeDtypeStruct((shards, 1, tile_rows, row_count), jnp.float32),
            in_specs=[pl.BlockSpec(memory_space=pltpu.VMEM)] * 3,
            out_specs=pl.BlockSpec(memory_space=pltpu.HBM),
            scratch_shapes=[
                pltpu.VMEM((4, tile_rows, row_count), jnp.float32),
                pltpu.SemaphoreType.DMA((shards,)),
            ],
            compiler_params=pltpu.CompilerParams(vmem_limit_bytes=VMEM_FINISH),
        )(rows, panel, tiles)

    return jax.shard_map(
        body,
        mesh=mesh,
        in_specs=(P("samp", "snp"), P("samp", "snp")),
        out_specs=P(None, "snp", None, "samp"),
        check_vma=False,
    )
```

```python
import functools
import math

import jax
import jax.numpy as jnp
from jax import lax
from jax.experimental import pallas as pl
from jax.experimental.pallas import tpu as pltpu
from jax.sharding import PartitionSpec as P

MESH = pl.DeviceIdType.MESH
var_floor = 0.1
UP, DOWN, SIDE, CORE = 0, 1, 2, 3
STRIP = 64
PIECES = 2
LOADS = 4
VMEM_ALL = 67043328
VMEM_SPARE = 512 * 1024
VMEM_FINISH = 12 * 1024 * 1024
FOLDED_SPARE = 1024 * 1024
FOLDED_FINISH = 8 * 1024 * 1024
CODE_TOP = 32767.0
TINY = 1e-30
RAW = 32


def index(at_z, at_y, at_core):
    return at_z * 4 + at_y * 2 + at_core


def source_at(z, depth, i):
    pairs = jnp.minimum(z, depth - 1 - z)
    side = jnp.where(i % 2 == 1, z - (i + 1) // 2, z + i // 2)
    far = jnp.where(z < depth - 1 - z, z + i - pairs, z - i + pairs)
    return jnp.where(i <= 2 * pairs, side, far)


def turned_at(z, depth):
    return jnp.where(z < depth - 1, z + 1, depth - 2)


def product(rows, panel, q, parts):
    pieces, piece_rows, snp_count = rows.shape[2:]
    total = None
    for h in parts:
        block = rows[q, h].reshape(pieces * piece_rows, snp_count)
        term = lax.dot_general(block, panel[h], (((1,), (1,)), ((), ())), preferred_element_type=jnp.float32)
        total = term if total is None else total + term
    return total * (1.0 / (rows.shape[1] * snp_count))


def finish(shards, groups, rows, panel, tiles, out_ref, late, out_sem):
    depth = shards // 4
    me = lax.axis_index("samp")
    z, y = me // 4, (me // 2) % 2
    turned = turned_at(z, depth)
    final = source_at(z, depth, depth - 1)
    final = jnp.where(final == turned, source_at(z, depth, depth - 2), final)
    last_part = lax.rem(lax.axis_index("snp") + groups - 1, groups)

    def is_late(q):
        return ((q // 4 == turned) | (q // 4 == final)) & ((q // 2) % 2 != y)

    def put(q, carry):
        @pl.when(jnp.logical_not(is_late(q)))
        def _():
            pltpu.make_async_copy(tiles.at[q], out_ref.at[q, 0], out_sem.at[q]).start()

        return carry

    lax.fori_loop(0, shards, put, 0)

    def form(i, carry):
        q = index(jnp.where(i // 2 == 0, final, turned), 1 - y, lax.rem(i, 2))
        late[i] = tiles[q] + product(rows, panel, q, [last_part])
        pltpu.make_async_copy(late.at[i], out_ref.at[q, 0], out_sem.at[q]).start()
        return carry

    lax.fori_loop(0, 4, form, 0)

    def flush(q, carry):
        pltpu.make_async_copy(tiles.at[q], out_ref.at[q, 0], out_sem.at[q]).wait()
        return carry

    lax.fori_loop(0, shards, flush, 0)


def kernel(shards, groups, geno_hbm, obs_hbm, panel, rows, tiles, geno_ref, obs_ref, counts, load_sem,
           count_send, count_recv, panel_send, panel_recv, row_send, row_recv):
    row_count, snp_count = geno_ref.shape
    tile_rows = row_count // groups
    piece_rows = tile_rows // PIECES
    depth = shards // 4
    me = lax.axis_index("samp")
    part = lax.axis_index("snp")
    z, y, core = me // 4, (me // 2) % 2, me % 2

    load_rows = row_count // LOADS

    def load(i):
        block = pl.ds(pl.multiple_of(i * load_rows, load_rows), load_rows)
        return (pltpu.make_async_copy(geno_hbm.at[block], geno_ref.at[block], load_sem.at[0, i]),
                pltpu.make_async_copy(obs_hbm.at[block], obs_ref.at[block], load_sem.at[1, i]))

    for i in range(LOADS):
        for copy in load(i):
            copy.start()

    barrier = pltpu.get_barrier_semaphore()
    for step in range(1, shards):
        pl.semaphore_signal(barrier, inc=1, device_id={"samp": lax.rem(me + step, shards)}, device_id_type=MESH)
    for step in range(1, groups):
        pl.semaphore_signal(barrier, inc=1, device_id={"snp": lax.rem(part + step, groups)}, device_id_type=MESH)

    def add_strip(i, total):
        alt, call = total
        strip = pl.ds(pl.multiple_of(i * STRIP, STRIP), STRIP)
        present = obs_ref[strip, :].astype(jnp.float32)
        held = present * geno_ref[strip, :]
        for r in range(0, STRIP, 8):
            alt = alt + held[r:r + 8]
            call = call + present[r:r + 8]
        return alt, call

    zero = jnp.zeros((8, snp_count), jnp.float32)
    alt, call = zero, zero
    strips = load_rows // STRIP
    for i in range(LOADS):
        for copy in load(i):
            copy.wait()
        alt, call = lax.fori_loop(i * strips, (i + 1) * strips, add_strip, (alt, call))
    counts[me, 0:1, :] = jnp.sum(alt, axis=0, keepdims=True)
    counts[me, 1:2, :] = jnp.sum(call, axis=0, keepdims=True)

    pl.semaphore_wait(barrier, shards + groups - 2)

    def count_copy(owner, to):
        return pltpu.make_async_remote_copy(
            src_ref=counts.at[owner], dst_ref=counts.at[owner], send_sem=count_send.at[to],
            recv_sem=count_recv.at[owner], device_id={"samp": to}, device_id_type=MESH)

    for step in range(1, shards):
        count_copy(me, lax.rem(me + step, shards)).start()
    for step in range(1, shards):
        other = lax.rem(me + step, shards)
        count_copy(other, other).wait_recv()
    sums = counts[0]
    for s in range(1, shards):
        sums = sums + counts[s]
    frequency = sums[0:1] / (2.0 * jnp.maximum(sums[1:2], 1.0))
    shift = 2.0 * frequency
    gain = lax.rsqrt(jnp.maximum(shift * (1.0 - frequency), var_floor))

    def piece_of(k, p):
        return pl.ds(pl.multiple_of(k * tile_rows + p * piece_rows, piece_rows), piece_rows)

    def panel_copy(h, k, to, p):
        block = panel.at[h, piece_of(k, p)]
        return pltpu.make_async_remote_copy(
            src_ref=block, dst_ref=block, send_sem=panel_send.at[to, k, p],
            recv_sem=panel_recv.at[h, k, p], device_id={"snp": to}, device_id_type=MESH)

    strip_rows = min(STRIP, piece_rows)

    def scale_piece(k, p):
        def scale_strip(i, carry):
            start = pl.multiple_of(k * tile_rows + p * piece_rows + i * strip_rows, strip_rows)
            strip = pl.ds(start, strip_rows)
            present = obs_ref[strip, :].astype(jnp.float32)
            panel[part, strip, :] = (present * (geno_ref[strip, :] - shift) * gain).astype(jnp.bfloat16)
            return carry

        lax.fori_loop(0, piece_rows // strip_rows, scale_strip, 0)

    def row_copy(q, h, p, way, src=None):
        to = (index(z + 1, y, core), index(z - 1, y, core), index(z, 1 - y, core), index(z, y, 1 - core))[way]
        return pltpu.make_async_remote_copy(
            src_ref=rows.at[q, h, p] if src is None else src, dst_ref=rows.at[q, h, p],
            send_sem=row_send.at[way, q, h, p], recv_sem=row_recv.at[q, h, p],
            device_id={"samp": to}, device_id_type=MESH)

    def arrive(q, h, p):
        row_copy(q, h, p, CORE).wait_recv()

    last_part = lax.rem(part + groups - 1, groups)
    turned = turned_at(z, depth)

    def part_at(i):
        return lax.rem(part + i, groups)

    def send_own(h, p):
        mine = panel.at[h, piece_of(part, p)]
        row_copy(me, h, p, SIDE, mine).start()

        @pl.when(z < depth - 1)
        def _():
            row_copy(me, h, p, UP, mine).start()

        @pl.when(z > 0)
        def _():
            row_copy(me, h, p, DOWN, mine).start()

        row_copy(me, h, p, CORE, mine).start()
        rows[me, h, p] = panel[h, piece_of(part, p), :]

    for p in range(PIECES):
        for step in range(1, groups):
            other = part_at(step)
            scale_piece(other, p)
            panel_copy(part, other, other, p).start()
        scale_piece(part, p)
        send_own(part, p)
    for step in range(1, groups):
        other = part_at(step)
        for k in range(1, groups):
            for p in range(PIECES):
                panel_copy(part, lax.rem(other + k, groups), other, p).start()
    for step in range(1, groups):
        h = part_at(step)
        for p in range(PIECES):
            panel_copy(h, part, h, p).wait_recv()
            send_own(h, p)

    def column_arrival(at_z, h, p, way):
        q = index(at_z, y, core)
        arrive(q, h, p)

        @pl.when(z < depth - 1 if way == UP else z > 0)
        def _():
            row_copy(q, h, p, way).start()

        @pl.when((at_z != turned) | (h != last_part))
        def _():
            row_copy(q, h, p, SIDE).start()

        row_copy(q, h, p, CORE).start()

    def column_arrivals(i):
        def per_piece(t, carry):
            h, p = part_at(t // PIECES), lax.rem(t, PIECES)

            @pl.when(z - i >= 0)
            def _():
                column_arrival(z - i, h, p, UP)

            @pl.when(z + i < depth)
            def _():
                column_arrival(z + i, h, p, DOWN)

            return carry

        lax.fori_loop(0, groups * PIECES, per_piece, 0)

    def arrive_all(q):
        def per_piece(t, carry):
            arrive(q, t // PIECES, lax.rem(t, PIECES))
            return carry

        lax.fori_loop(0, groups * PIECES, per_piece, 0)

    def products(at_z, at_y):
        def per_core(t, carry):
            q = index(at_z, at_y, lax.rem(core + t, 2))

            @pl.when(t == 1)
            def _():
                arrive_all(q)

            tiles[q] = product(rows, panel, q, range(groups))
            return carry

        lax.fori_loop(0, 2, per_core, 0)

    def side_arrival(at_z, h, p):
        q = index(at_z, 1 - y, core)
        arrive(q, h, p)
        row_copy(q, h, p, CORE).start()

    final = source_at(z, depth, depth - 1)
    final = jnp.where(final == turned, source_at(z, depth, depth - 2), final)

    def begin_late():
        def per_tile(t, carry):
            q = index(jnp.where(t % 2 == 0, turned, final), 1 - y, lax.rem(core + t // 2, 2))

            @pl.when(t >= 2)
            def _():
                for step in range(groups - 1):
                    for p in range(PIECES):
                        arrive(q, part_at(step), p)

            tiles[q] = product(rows, panel, q, [part_at(step) for step in range(groups - 1)])
            return carry

        lax.fori_loop(0, 4, per_tile, 0)

    def round_of(i, carry):
        @pl.when(i < depth)
        def _():
            column_arrivals(i)

        @pl.when(i == 1)
        def _():
            for step in range(1, groups):
                h = part_at(step)
                for k in range(1, groups):
                    for p in range(PIECES):
                        panel_copy(h, part_at(k), h, p).wait_recv()

        @pl.when(i == depth - 1)
        def _():
            q = index(z, 1 - y, core)

            @pl.when(z > 0)
            def _():
                for p in range(PIECES):
                    row_copy(q, last_part, p, DOWN).start()

            @pl.when(z == depth - 2)
            def _():
                for p in range(PIECES):
                    row_copy(q, last_part, p, UP).start()

        at_z = source_at(z, depth, i - 1)
        products(at_z, y)

        def per_piece(t, c):
            @pl.when((i == depth) & (t == (groups - 1) * PIECES))
            def _():
                begin_late()

            @pl.when((at_z != turned) | (t // PIECES != groups - 1))
            def _():
                side_arrival(at_z, part_at(t // PIECES), lax.rem(t, PIECES))

            return c

        lax.fori_loop(0, groups * PIECES, per_piece, 0)

        @pl.when((at_z != turned) & (at_z != final))
        def _():
            products(at_z, 1 - y)

        return carry

    lax.fori_loop(1, depth + 1, round_of, 0)
    for p in range(PIECES):
        side_arrival(turned, last_part, p)
    for p in range(PIECES):
        arrive(index(final, 1 - y, 1 - core), last_part, p)
        arrive(index(turned, 1 - y, 1 - core), last_part, p)

    for step in range(1, shards):
        count_copy(me, lax.rem(me + step, shards)).wait_send()
    for step in range(1, groups):
        for k in range(groups):
            for p in range(PIECES):
                panel_copy(part, k, part_at(step), p).wait_send()

    def drain(i, carry):
        at_z, h, p = i // (groups * PIECES), lax.rem(i // PIECES, groups), lax.rem(i, PIECES)
        q = index(at_z, y, core)
        across = index(at_z, 1 - y, core)

        @pl.when((at_z <= z) & (z < depth - 1))
        def _():
            row_copy(q, h, p, UP).wait_send()

        @pl.when((at_z >= z) & (z > 0))
        def _():
            row_copy(q, h, p, DOWN).wait_send()

        @pl.when((at_z != turned) | (h != last_part))
        def _():
            row_copy(q, h, p, SIDE).wait_send()

        row_copy(q, h, p, CORE).wait_send()
        row_copy(across, h, p, CORE).wait_send()

        @pl.when((at_z == z) & (h == last_part) & (z > 0))
        def _():
            row_copy(across, h, p, DOWN).wait_send()

        @pl.when((at_z == z) & (h == last_part) & (z == depth - 2))
        def _():
            row_copy(across, h, p, UP).wait_send()

        return carry

    lax.fori_loop(0, depth * groups * PIECES, drain, 0)


def shape_of_line(depth):
    z = lax.axis_index("samp") // 4
    low = z < depth // 2
    inward = jnp.where(low, z + 1, z - 1)
    outward = jnp.clip(jnp.where(low, z - 1, z + 1), 0, depth - 1)
    is_end = (z == 0) | (z == depth - 1)
    return z, inward, outward, is_end


def folded_finish(shards, groups, rows, panel, tiles, codes, steps, out_ref, late, out_sem):
    depth = shards // 4
    me = lax.axis_index("samp")
    y = (me // 2) % 2
    z, inward, outward, is_end = shape_of_line(depth)
    far_mid, far_end = depth - 1 - inward, depth - 1 - z
    last_part = lax.rem(lax.axis_index("snp") + groups - 1, groups)
    piece_rows = rows.shape[3]
    tile_rows = PIECES * piece_rows

    def is_late(q):
        return is_end & ((q // 4 == far_end) | ((q // 4 == far_mid) & ((q // 2) % 2 != y)))

    def put(q, carry):
        @pl.when(jnp.logical_not(is_late(q)))
        def _():
            pltpu.make_async_copy(tiles.at[q], out_ref.at[q, 0], out_sem.at[0]).start()

        return carry

    lax.fori_loop(0, shards, put, 0)

    @pl.when(is_end)
    def _():
        def decode(t, carry):
            for p in range(PIECES):
                for k in range(groups):
                    unit = (t * PIECES + p) * groups + k
                    late[t, p * piece_rows:(p + 1) * piece_rows, k * tile_rows:(k + 1) * tile_rows] = (
                        codes[unit].astype(jnp.float32) * steps[unit])
            q = index(far_end, jnp.where(t // 2 == 0, y, 1 - y), lax.rem(t, 2))
            pltpu.make_async_copy(late.at[t], out_ref.at[q, 0], out_sem.at[0]).start()
            return carry

        lax.fori_loop(0, 4, decode, 0)

        def form(i, carry):
            q = index(far_mid, 1 - y, i)
            late[4 + i] = tiles[q] + product(rows, panel, q, [last_part])
            pltpu.make_async_copy(late.at[4 + i], out_ref.at[q, 0], out_sem.at[0]).start()
            return carry

        lax.fori_loop(0, 2, form, 0)

    pltpu.make_async_copy(tiles, out_ref.at[:, 0], out_sem.at[0]).wait()


def folded(shards, groups, geno_hbm, obs_hbm, panel, rows, tiles, codes, steps, geno_ref, obs_ref, alts, calls, columns,
           made, made_steps, raw, raw_in, load_sem, count_sem, across_send, across_recv, line_send, side_send, core_send, row_recv,
           core_recv, code_sem, raw_sem):
    row_count, snp_count = geno_ref.shape
    tile_rows = row_count // groups
    piece_rows = tile_rows // PIECES
    depth = shards // 4
    me = lax.axis_index("samp")
    part = lax.axis_index("snp")
    y, core = (me // 2) % 2, me % 2
    z, inward, outward, is_end = shape_of_line(depth)
    other = lax.rem(part + 1, groups)
    load_rows = row_count // LOADS

    def load(i):
        block = pl.ds(pl.multiple_of(i * load_rows, load_rows), load_rows)
        return (pltpu.make_async_copy(geno_hbm.at[block], geno_ref.at[block], load_sem.at[i]),
                pltpu.make_async_copy(obs_hbm.at[block], obs_ref.at[block], load_sem.at[i]))

    for i in range(LOADS):
        for copy in load(i):
            copy.start()

    barrier = pltpu.get_barrier_semaphore()
    for step in range(1, shards):
        pl.semaphore_signal(barrier, inc=1, device_id={"samp": lax.rem(me + step, shards)}, device_id_type=MESH)
    pl.semaphore_signal(barrier, inc=1, device_id={"snp": other}, device_id_type=MESH)

    def add_strip(i, total):
        alt, call = total
        strip = pl.ds(pl.multiple_of(i * STRIP, STRIP), STRIP)
        present = obs_ref[strip, :].astype(jnp.float32)
        held = present * geno_ref[strip, :]
        for r in range(0, STRIP, 8):
            alt = alt + held[r:r + 8]
            call = call + present[r:r + 8]
        return alt, call

    zero = jnp.zeros((8, snp_count), jnp.float32)
    alt, call = zero, zero
    strips = load_rows // STRIP
    for i in range(LOADS):
        loaded = geno_ref.at[pl.ds(0, 2 * load_rows)]
        pltpu.make_async_copy(loaded, loaded, load_sem.at[i]).wait()
        alt, call = lax.fori_loop(i * strips, (i + 1) * strips, add_strip, (alt, call))
    alts[me] = jnp.sum(alt, axis=0, keepdims=True)
    call = jnp.sum(call, axis=0, keepdims=True).astype(jnp.int32)
    half = snp_count // 2
    calls[me] = jnp.concatenate([call[:, :half], call[:, half:]]).astype(jnp.int16)

    early = pl.ds(pl.multiple_of(part * tile_rows, tile_rows), RAW)
    raw[...] = jnp.where(obs_ref[early, :] > 0, geno_ref[early, :], -1.0)
    pl.semaphore_wait(barrier, shards)

    for step in range(shards):
        to = jnp.where(z < depth // 2, shards - 1 - step, step)

        @pl.when(to != me)
        def _():
            for n, sent in enumerate((alts, calls)):
                pltpu.make_async_remote_copy(
                    src_ref=sent.at[me], dst_ref=sent.at[me], send_sem=count_sem.at[2 * n],
                    recv_sem=count_sem.at[2 * n + 1], device_id={"samp": to}, device_id_type=MESH).start()

    def await_bytes(ref, sem):
        pltpu.make_async_copy(ref, ref, sem).wait()

    def await_rows(count, sem):
        await_bytes(geno_ref.at[pl.ds(0, count // 2)], sem)

    def raw_copy(to, slot):
        return pltpu.make_async_remote_copy(
            src_ref=raw, dst_ref=raw_in.at[slot], send_sem=raw_sem.at[0], recv_sem=raw_sem.at[1 + slot],
            device_id={"samp": to}, device_id_type=MESH)

    raw_copy(index(z, 1 - y, core), 0).start()
    raw_copy(index(inward, y, core), jnp.where(is_end, 2, 1)).start()

    @pl.when(jnp.logical_not(is_end))
    def _():
        raw_copy(index(outward, y, core), 1).start()

    def await_counts(way):
        for n, sent in enumerate((alts, calls)):
            await_bytes(sent.at[pl.ds(0, shards - 1)], count_sem.at[2 * n + way])

    await_counts(1)
    alt, call = alts[0], calls[0].astype(jnp.int32)
    for s in range(1, shards):
        alt, call = alt + alts[s], call + calls[s].astype(jnp.int32)
    call = jnp.concatenate([call[0:1], call[1:2]], axis=1).astype(jnp.float32)
    frequency = alt / (2.0 * jnp.maximum(call, 1.0))
    shift = 2.0 * frequency
    gain = lax.rsqrt(jnp.maximum(shift * (1.0 - frequency), var_floor))

    def piece_of(k, p):
        return pl.ds(pl.multiple_of(k * tile_rows + p * piece_rows, piece_rows), piece_rows)

    strip_rows = min(STRIP, piece_rows)

    def scale_piece(k, p):
        def scale_strip(i, carry):
            start = pl.multiple_of(k * tile_rows + p * piece_rows + i * strip_rows, strip_rows)
            strip = pl.ds(start, strip_rows)
            present = obs_ref[strip, :].astype(jnp.float32)
            panel[part, strip, :] = (present * (geno_ref[strip, :] - shift) * gain).astype(jnp.bfloat16)
            return carry

        lax.fori_loop(0, piece_rows // strip_rows, scale_strip, 0)

    def panel_copy(k, p):
        block = panel.at[part, piece_of(k, p)]
        return pltpu.make_async_remote_copy(
            src_ref=block, dst_ref=block, send_sem=across_send.at[0],
            recv_sem=across_recv.at[jnp.where(k == part, PIECES, p)], device_id={"snp": other}, device_id_type=MESH)

    def column_copy(q, h, p):
        return pltpu.make_async_remote_copy(
            src_ref=rows.at[q, h, p], dst_ref=columns.at[part, h, pl.ds(pl.multiple_of(p * piece_rows, piece_rows), piece_rows)],
            send_sem=across_send.at[1], recv_sem=across_recv.at[PIECES + 1], device_id={"snp": other}, device_id_type=MESH)

    cut = piece_rows * 7 // 8
    head, rest = pl.ds(0, cut), pl.ds(cut, piece_rows - cut)

    def span_copy(q, h, p, span, to, send_sem, recv_sem):
        return pltpu.make_async_remote_copy(
            src_ref=rows.at[q, h, p, span], dst_ref=rows.at[q, h, p, span], send_sem=send_sem, recv_sem=recv_sem,
            device_id={"samp": to}, device_id_type=MESH)

    def slot_of(q, at):
        return lax.rem(q // 2 - at // 2 + shards // 2, shards // 2) - 1

    def own_copy(q, h, p, to, send_sem, src=None, dst=None):
        return pltpu.make_async_remote_copy(
            src_ref=rows.at[q, h, p] if src is None else src, dst_ref=rows.at[q, h, p] if dst is None else dst,
            send_sem=send_sem,
            recv_sem=row_recv.at[slot_of(q, to), h, p], device_id={"samp": to}, device_id_type=MESH)

    def send_in(q, h, p, extra=0):
        own_copy(q, h, p, index(inward, y, core), line_send.at[extra]).start()

    def send_out(q, h, p):
        own_copy(q, h, p, index(outward, y, core), line_send.at[2]).start()

    def send_side(q, h, p, extra=0):
        own_copy(q, h, p, index(z, 1 - y, core), side_send.at[extra]).start()

    def core_slot(q, h, p):
        late = jnp.where(is_end, (q // 2 == (depth - 1 - inward) * 2 + 1 - y) & (h != part),
                         (q // 4 == depth - 1 - outward) & (p == 1))
        return jnp.where(late, late_slot(q), q // 2)

    def late_slot(q):
        return shards // 2 + lax.rem(q // 2, 2)

    def send_core(q, h, p, src=None):
        pltpu.make_async_remote_copy(
            src_ref=rows.at[q, h, p] if src is None else src, dst_ref=rows.at[q, h, p], send_sem=core_send.at[0],
            recv_sem=core_recv.at[core_slot(q, h, p)], device_id={"samp": index(z, y, 1 - core)},
            device_id_type=MESH).start()

    def send_core_span(q, h, p, span):
        span_copy(q, h, p, span, index(z, y, 1 - core), core_send.at[0], core_recv.at[core_slot(q, h, p)]).start()

    def arrive(q, h, p):
        await_bytes(rows.at[q, h, p], row_recv.at[slot_of(q, me), h, p])

    def arrive_core(q, late):
        await_bytes(rows.at[q, 0], core_recv.at[late_slot(q) if late else q // 2])

    def part_at(i):
        return lax.rem(part + i, groups)

    def send_own(h, p, skip=0):
        mine = panel.at[h, piece_of(part, p)]
        kept = panel.at[h, pl.ds(pl.multiple_of(part * tile_rows + p * piece_rows + skip, 16), piece_rows - skip)]
        kept_to = rows.at[me, h, p, pl.ds(skip, piece_rows - skip)]
        own_copy(me, h, p, index(z, 1 - y, core), side_send.at[0], kept, kept_to).start()
        own_copy(me, h, p, index(inward, y, core), line_send.at[0], kept, kept_to).start()

        @pl.when(jnp.logical_not(is_end))
        def _():
            own_copy(me, h, p, index(outward, y, core), line_send.at[2], kept, kept_to).start()

        send_core(me, h, p, mine)
        rows[me, h, p] = panel[h, piece_of(part, p), :]

    def scale_raw(slot, q):
        await_bytes(raw_in.at[slot], raw_sem.at[1 + slot])
        sent = raw_in[slot]
        rows[q, part, 0, 0:RAW, :] = jnp.where(sent >= 0.0, (sent - shift) * gain, 0.0).astype(jnp.bfloat16)

    def arrive_near(q, h, p):
        @pl.when((h == part) & (p == 0))
        def _():
            await_bytes(rows.at[q, h, p, pl.ds(RAW, piece_rows - RAW)], row_recv.at[slot_of(q, me), h, p])

        @pl.when((h != part) | (p != 0))
        def _():
            arrive(q, h, p)

    for p in range(PIECES):
        scale_piece(part, p)
        send_own(part, p, 0 if p else RAW)
        scale_piece(other, p)
        panel_copy(other, p).start()
    for p in range(PIECES):
        panel_copy(part, p).start()
    scale_raw(0, index(z, 1 - y, core))
    scale_raw(1, index(inward, y, core))

    @pl.when(jnp.logical_not(is_end))
    def _():
        scale_raw(2, index(outward, y, core))

    for p in range(PIECES):
        await_bytes(panel.at[other, piece_of(part, p)], across_recv.at[p])
        send_own(other, p)

    def form(at_z, at_y, parts=None, wait=True):
        def per_core(t, carry):
            q = index(at_z, at_y, lax.rem(core + t, 2))
            if wait:
                @pl.when(t == 1)
                def _():
                    if parts is None:
                        await_bytes(rows.at[q], core_recv.at[q // 2])
                    else:
                        arrive_core(q, False)

            tiles[q] = product(rows, panel, q, range(groups) if parts is None else parts)
            return carry

        lax.fori_loop(0, 2, per_core, 0)

    def await_panel():
        await_bytes(panel.at[other, pl.ds(pl.multiple_of(other * tile_rows, tile_rows), tile_rows)], across_recv.at[PIECES])

    def pick(i, values):
        chosen = values[-1]
        for n in range(len(values) - 2, -1, -1):
            chosen = jnp.where(i == n, values[n], chosen)
        return chosen

    count = groups * PIECES

    @pl.when(is_end)
    def _():
        far_mid = depth - 1 - inward

        def first(t, carry):
            h, p = part_at(t // PIECES), lax.rem(t, PIECES)
            near, beside = index(inward, y, core), index(z, 1 - y, core)
            arrive_near(near, h, p)
            send_side(near, h, p)
            send_core(near, h, p)
            arrive_near(beside, h, p)
            send_in(beside, h, p)
            send_core(beside, h, p)
            return carry

        lax.fori_loop(0, count, first, 0)
        await_panel()

        def second(t, carry):
            h, p = part_at(t // PIECES), lax.rem(t, PIECES)
            far, cross = index(far_mid, y, core), index(inward, 1 - y, core)
            arrive(far, h, p)
            to = index(z, 1 - y, core)

            @pl.when(t < count - 1)
            def _():
                send_side(far, h, p, extra=1)

            @pl.when(t == count - 1)
            def _():
                span_copy(far, h, p, head, to, side_send.at[1], row_recv.at[slot_of(far, to), h, p]).start()
                span_copy(far, h, p, rest, to, side_send.at[1], code_sem.at[4]).start()

            send_core(far, h, p)
            arrive(cross, h, p)
            send_core(cross, h, p)

            @pl.when(t < 3)
            def _():
                form(pick(t, (z, inward, z)), pick(t, (y, y, 1 - y)))

            return carry

        lax.fori_loop(0, count, second, 0)

        def third(t, carry):
            h, p = part_at(t // PIECES), lax.rem(t, PIECES)
            q = index(far_mid, 1 - y, core)

            @pl.when(t < count - 1)
            def _():
                arrive(q, h, p)
                send_core(q, h, p)

            @pl.when(t == count - 1)
            def _():
                await_bytes(rows.at[q, h, p, head], row_recv.at[slot_of(q, me), h, p])
                send_core_span(q, h, p, head)
                await_bytes(rows.at[q, h, p, rest], code_sem.at[4])
                send_core_span(q, h, p, rest)

            @pl.when(t < 2)
            def _():
                form(pick(t, (far_mid, inward)), pick(t, (y, 1 - y)))

            @pl.when(t == 2)
            def _():
                form(far_mid, 1 - y, [part])

            return carry

        lax.fori_loop(0, count, third, 0)
        await_bytes(codes, code_sem.at[1])
        await_bytes(steps, code_sem.at[3])
        arrive_core(index(far_mid, 1 - y, 1 - core), True)
        await_rows(2 * row_count - RAW, line_send.at[0])
        await_rows(2 * row_count - RAW, side_send.at[0])
        await_rows(count * piece_rows, side_send.at[1])
        await_bytes(raw_in.at[pl.ds(0, 2)], raw_sem.at[0])
        await_bytes(rows.at[pl.ds(0, 6)], core_send.at[0])

    @pl.when(jnp.logical_not(is_end))
    def _():
        far = depth - 1 - outward

        def first(t, carry):
            h, p = part_at(t // PIECES), lax.rem(t, PIECES)
            end, near, beside = index(outward, y, core), index(inward, y, core), index(z, 1 - y, core)
            arrive_near(end, h, p)

            @pl.when(p == 0)
            def _():
                send_in(end, h, 0)

            @pl.when(h == other)
            def _():
                send_in(end, jnp.where(p == 0, part, other), 1)

            send_core(end, h, p)
            column_copy(end, h, p).start()
            arrive_near(near, h, p)
            send_out(near, h, p)
            send_core(near, h, p)
            arrive_near(beside, h, p)
            send_core(beside, h, p)
            return carry

        lax.fori_loop(0, count, first, 0)
        for p in range(PIECES):
            send_in(index(z, 1 - y, core), part, p, extra=1)
        for h in range(groups):
            columns[part, h] = rows[index(outward, y, core), h].reshape(tile_rows, snp_count)
        await_panel()

        def code_copy(source, target, n):
            return pltpu.make_async_remote_copy(
                src_ref=source, dst_ref=target, send_sem=code_sem.at[n], recv_sem=code_sem.at[n + 1],
                device_id={"samp": index(outward, y, core)}, device_id_type=MESH)

        def make(side, p, k):
            def per_core(t, carry):
                which = lax.rem(core + t, 2)
                q = index(far, jnp.where(side == 0, y, 1 - y), which)
                term = None
                for h in range(groups):
                    one = lax.dot_general(rows[q, h, p], columns[k, h], (((1,), (1,)), ((), ())),
                                          preferred_element_type=jnp.float32)
                    term = one if term is None else term + one
                term = term * (1.0 / (groups * snp_count))
                top = jnp.max(jnp.abs(term), axis=0, keepdims=True)
                unit = ((side * 2 + which) * PIECES + p) * groups + k
                made[unit] = jnp.round(term * (CODE_TOP / jnp.maximum(top, TINY))).astype(jnp.int32).astype(jnp.int16)
                made_steps[unit] = top * (1.0 / CODE_TOP)
                code_copy(made.at[unit], codes.at[unit], 0).start()
                return carry

            lax.fori_loop(0, 2, per_core, 0)

        def far_core(side, p):
            arrive_core(index(far, jnp.where(side == 0, y, 1 - y), 1 - core), p == 1)

        def make_list(listed):
            def per_entry(i, carry):
                side, p, away = (pick(i, [entry[n] for entry in listed]) for n in range(3))
                make(side, p, lax.rem(part + away, groups))
                return carry

            lax.fori_loop(0, len(listed), per_entry, 0)

        def second(t, carry):
            h, p = part_at(lax.rem(t, groups)), t // groups
            far_q, cross = index(far, y, core), index(outward, 1 - y, core)

            @pl.when(t >= 2)
            def _():
                far_core(t - 2, 0)
                make(t - 2, 0, part)

            arrive(far_q, h, p)
            send_side(far_q, h, p)
            send_core(far_q, h, p)
            ch, cp = part_at(t // PIECES), lax.rem(t, PIECES)
            arrive(cross, ch, cp)
            send_core(cross, ch, cp)

            @pl.when(t > 0)
            def _():
                q = index(far, 1 - y, core)
                h, p = part_at(lax.rem(t - 1, groups)), (t - 1) // groups
                arrive(q, h, p)
                send_core(q, h, p)

            form(pick(t, (z, outward, inward, z)), pick(t, (y, y, y, 1 - y)))
            return carry

        lax.fori_loop(0, count, second, 0)
        for p in range(PIECES):
            send_side(index(inward, y, core), other, p, extra=1)
        far_core(0, 1)
        make_list([(0, 1, 0)])
        await_bytes(columns.at[other], across_recv.at[PIECES + 1])
        make_list([(0, 0, 1), (0, 1, 1), (1, 0, 1)])
        form(outward, 1 - y)
        q = index(far, 1 - y, core)
        arrive(q, other, PIECES - 1)
        send_core(q, other, PIECES - 1)
        cross = index(inward, 1 - y, core)

        def third(t, carry):
            h, p = part_at(t // PIECES), lax.rem(t, PIECES)
            arrive(cross, h, p)
            send_core(cross, h, p)

            @pl.when(t == 1)
            def _():
                far_core(1, 1)
                make_list([(1, 1, 0), (1, 1, 1)])
                code_copy(made_steps, steps, 2).start()

            @pl.when(t < 2)
            def _():
                form(far, pick(t, (y, 1 - y)), wait=False)

            return carry

        lax.fori_loop(0, count, third, 0)
        form(inward, 1 - y)
        await_rows(2 * row_count - RAW, line_send.at[0])
        await_bytes(rows.at[0, 0], line_send.at[1])
        await_rows(2 * row_count - RAW, line_send.at[2])
        await_bytes(raw_in, raw_sem.at[0])
        await_rows(2 * row_count - RAW, side_send.at[0])
        await_bytes(rows.at[0, 0], side_send.at[1])
        await_bytes(rows.at[pl.ds(0, 8)], core_send.at[0])
        await_bytes(rows.at[0], across_send.at[1])
        await_bytes(made, code_sem.at[0])
        await_bytes(made_steps, code_sem.at[2])

    await_counts(0)
    await_bytes(rows.at[0], across_send.at[0])


def folded_body(shards, groups, genotypes, observed):
    row_count, snp_count = genotypes.shape
    tile_rows = row_count // groups
    piece_rows = tile_rows // PIECES
    units = 4 * PIECES * groups
    outs = (
        pltpu.VMEM((groups, row_count, snp_count), jnp.bfloat16),
        pltpu.VMEM((shards, groups, PIECES, piece_rows, snp_count), jnp.bfloat16),
        pltpu.VMEM((shards, tile_rows, row_count), jnp.float32),
        pltpu.VMEM((units, piece_rows, tile_rows), jnp.int16),
        pltpu.VMEM((units, 1, tile_rows), jnp.float32),
    )
    kept = sum(math.prod(o.shape) * jnp.dtype(o.dtype).itemsize for o in outs)
    held = pl.pallas_call(
        functools.partial(folded, shards, groups),
        out_shape=outs,
        in_specs=[pl.BlockSpec(memory_space=pltpu.HBM)] * 2,
        out_specs=[pl.BlockSpec(memory_space=pltpu.VMEM)] * 5,
        scratch_shapes=[
            pltpu.VMEM((row_count, snp_count), jnp.float32),
            pltpu.VMEM((row_count, snp_count), jnp.int32),
            pltpu.VMEM((shards, 1, snp_count), jnp.float32),
            pltpu.VMEM((shards, 2, snp_count // 2), jnp.int16),
            pltpu.VMEM((groups, groups, tile_rows, snp_count), jnp.bfloat16),
            pltpu.VMEM((units, piece_rows, tile_rows), jnp.int16),
            pltpu.VMEM((units, 1, tile_rows), jnp.float32),
            pltpu.VMEM((RAW, snp_count), jnp.float32),
            pltpu.VMEM((3, RAW, snp_count), jnp.float32),
            pltpu.SemaphoreType.DMA((LOADS,)),
            pltpu.SemaphoreType.DMA((4,)),
            pltpu.SemaphoreType.DMA((2,)),
            pltpu.SemaphoreType.DMA((PIECES + 2,)),
            pltpu.SemaphoreType.DMA((3,)),
            pltpu.SemaphoreType.DMA((2,)),
            pltpu.SemaphoreType.DMA((1,)),
            pltpu.SemaphoreType.DMA((shards // 2 - 1, groups, PIECES)),
            pltpu.SemaphoreType.DMA((shards // 2 + 2,)),
            pltpu.SemaphoreType.DMA((5,)),
            pltpu.SemaphoreType.DMA((4,)),
        ],
        compiler_params=pltpu.CompilerParams(
            collective_id=0, has_side_effects=True, vmem_limit_bytes=VMEM_ALL - FOLDED_SPARE - kept),
    )(genotypes, observed)
    panel, rows, tiles, codes, steps = held
    return pl.pallas_call(
        functools.partial(folded_finish, shards, groups),
        out_shape=jax.ShapeDtypeStruct((shards, 1, tile_rows, row_count), jnp.float32),
        in_specs=[pl.BlockSpec(memory_space=pltpu.VMEM)] * 5,
        out_specs=pl.BlockSpec(memory_space=pltpu.HBM),
        scratch_shapes=[
            pltpu.VMEM((6, tile_rows, row_count), jnp.float32),
            pltpu.SemaphoreType.DMA((1,)),
        ],
        compiler_params=pltpu.CompilerParams(vmem_limit_bytes=FOLDED_FINISH),
    )(rows, panel, tiles, codes, steps)


def solution(mesh):
    shards, groups = mesh.shape["samp"], mesh.shape["snp"]

    def body(genotypes, observed):
        if groups == 2 and shards == 16:
            return folded_body(shards, groups, genotypes, observed)
        row_count, snp_count = genotypes.shape
        tile_rows = row_count // groups
        piece_rows = tile_rows // PIECES
        kept = 2 * (groups * row_count * snp_count) * (1 + shards // groups) + 4 * shards * tile_rows * row_count
        panel, rows, tiles = pl.pallas_call(
            functools.partial(kernel, shards, groups),
            out_shape=(
                pltpu.VMEM((groups, row_count, snp_count), jnp.bfloat16),
                pltpu.VMEM((shards, groups, PIECES, piece_rows, snp_count), jnp.bfloat16),
                pltpu.VMEM((shards, tile_rows, row_count), jnp.float32),
            ),
            in_specs=[pl.BlockSpec(memory_space=pltpu.HBM)] * 2,
            out_specs=[pl.BlockSpec(memory_space=pltpu.VMEM)] * 3,
            scratch_shapes=[
                pltpu.VMEM((row_count, snp_count), jnp.float32),
                pltpu.VMEM((row_count, snp_count), jnp.int32),
                pltpu.VMEM((shards, 2, snp_count), jnp.float32),
                pltpu.SemaphoreType.DMA((2, LOADS)),
                pltpu.SemaphoreType.DMA((shards,)),
                pltpu.SemaphoreType.DMA((shards,)),
                pltpu.SemaphoreType.DMA((groups, groups, PIECES)),
                pltpu.SemaphoreType.DMA((groups, groups, PIECES)),
                pltpu.SemaphoreType.DMA((4, shards, groups, PIECES)),
                pltpu.SemaphoreType.DMA((shards, groups, PIECES)),
            ],
            compiler_params=pltpu.CompilerParams(
                collective_id=0, has_side_effects=True, vmem_limit_bytes=VMEM_ALL - VMEM_SPARE - kept),
        )(genotypes, observed)
        return pl.pallas_call(
            functools.partial(finish, shards, groups),
            out_shape=jax.ShapeDtypeStruct((shards, 1, tile_rows, row_count), jnp.float32),
            in_specs=[pl.BlockSpec(memory_space=pltpu.VMEM)] * 3,
            out_specs=pl.BlockSpec(memory_space=pltpu.HBM),
            scratch_shapes=[
                pltpu.VMEM((4, tile_rows, row_count), jnp.float32),
                pltpu.SemaphoreType.DMA((shards,)),
            ],
            compiler_params=pltpu.CompilerParams(vmem_limit_bytes=VMEM_FINISH),
        )(rows, panel, tiles)

    return jax.shard_map(
        body,
        mesh=mesh,
        in_specs=(P("samp", "snp"), P("samp", "snp")),
        out_specs=P(None, "snp", None, "samp"),
        check_vma=False,
    )
```

```python
import functools
import math

import jax
import jax.numpy as jnp
from jax import lax
from jax.experimental import pallas as pl
from jax.experimental.pallas import tpu as pltpu
from jax.sharding import PartitionSpec as P

MESH = pl.DeviceIdType.MESH
var_floor = 0.1
UP, DOWN, SIDE, CORE = 0, 1, 2, 3
STRIP = 64
PIECES = 2
LOADS = 4
VMEM_ALL = 67043328
VMEM_SPARE = 512 * 1024
VMEM_FINISH = 12 * 1024 * 1024
FOLDED_SPARE = 1024 * 1024
FOLDED_FINISH = 8 * 1024 * 1024
CODE_TOP = 32767.0
TINY = 1e-30
RAW = 32


def index(at_z, at_y, at_core):
    return at_z * 4 + at_y * 2 + at_core


def source_at(z, depth, i):
    pairs = jnp.minimum(z, depth - 1 - z)
    side = jnp.where(i % 2 == 1, z - (i + 1) // 2, z + i // 2)
    far = jnp.where(z < depth - 1 - z, z + i - pairs, z - i + pairs)
    return jnp.where(i <= 2 * pairs, side, far)


def turned_at(z, depth):
    return jnp.where(z < depth - 1, z + 1, depth - 2)


def product(rows, panel, q, parts):
    pieces, piece_rows, snp_count = rows.shape[2:]
    total = None
    for h in parts:
        block = rows[q, h].reshape(pieces * piece_rows, snp_count)
        term = lax.dot_general(block, panel[h], (((1,), (1,)), ((), ())), preferred_element_type=jnp.float32)
        total = term if total is None else total + term
    return total * (1.0 / (rows.shape[1] * snp_count))


def finish(shards, groups, rows, panel, tiles, out_ref, late, out_sem):
    depth = shards // 4
    me = lax.axis_index("samp")
    z, y = me // 4, (me // 2) % 2
    turned = turned_at(z, depth)
    final = source_at(z, depth, depth - 1)
    final = jnp.where(final == turned, source_at(z, depth, depth - 2), final)
    last_part = lax.rem(lax.axis_index("snp") + groups - 1, groups)

    def is_late(q):
        return ((q // 4 == turned) | (q // 4 == final)) & ((q // 2) % 2 != y)

    def put(q, carry):
        @pl.when(jnp.logical_not(is_late(q)))
        def _():
            pltpu.make_async_copy(tiles.at[q], out_ref.at[q, 0], out_sem.at[q]).start()

        return carry

    lax.fori_loop(0, shards, put, 0)

    def form(i, carry):
        q = index(jnp.where(i // 2 == 0, final, turned), 1 - y, lax.rem(i, 2))
        late[i] = tiles[q] + product(rows, panel, q, [last_part])
        pltpu.make_async_copy(late.at[i], out_ref.at[q, 0], out_sem.at[q]).start()
        return carry

    lax.fori_loop(0, 4, form, 0)

    def flush(q, carry):
        pltpu.make_async_copy(tiles.at[q], out_ref.at[q, 0], out_sem.at[q]).wait()
        return carry

    lax.fori_loop(0, shards, flush, 0)


def kernel(shards, groups, geno_hbm, obs_hbm, panel, rows, tiles, geno_ref, obs_ref, counts, load_sem,
           count_send, count_recv, panel_send, panel_recv, row_send, row_recv):
    row_count, snp_count = geno_ref.shape
    tile_rows = row_count // groups
    piece_rows = tile_rows // PIECES
    depth = shards // 4
    me = lax.axis_index("samp")
    part = lax.axis_index("snp")
    z, y, core = me // 4, (me // 2) % 2, me % 2

    load_rows = row_count // LOADS

    def load(i):
        block = pl.ds(pl.multiple_of(i * load_rows, load_rows), load_rows)
        return (pltpu.make_async_copy(geno_hbm.at[block], geno_ref.at[block], load_sem.at[0, i]),
                pltpu.make_async_copy(obs_hbm.at[block], obs_ref.at[block], load_sem.at[1, i]))

    for i in range(LOADS):
        for copy in load(i):
            copy.start()

    barrier = pltpu.get_barrier_semaphore()
    for step in range(1, shards):
        pl.semaphore_signal(barrier, inc=1, device_id={"samp": lax.rem(me + step, shards)}, device_id_type=MESH)
    for step in range(1, groups):
        pl.semaphore_signal(barrier, inc=1, device_id={"snp": lax.rem(part + step, groups)}, device_id_type=MESH)

    def add_strip(i, total):
        alt, call = total
        strip = pl.ds(pl.multiple_of(i * STRIP, STRIP), STRIP)
        present = obs_ref[strip, :].astype(jnp.float32)
        held = present * geno_ref[strip, :]
        for r in range(0, STRIP, 8):
            alt = alt + held[r:r + 8]
            call = call + present[r:r + 8]
        return alt, call

    zero = jnp.zeros((8, snp_count), jnp.float32)
    alt, call = zero, zero
    strips = load_rows // STRIP
    for i in range(LOADS):
        for copy in load(i):
            copy.wait()
        alt, call = lax.fori_loop(i * strips, (i + 1) * strips, add_strip, (alt, call))
    counts[me, 0:1, :] = jnp.sum(alt, axis=0, keepdims=True)
    counts[me, 1:2, :] = jnp.sum(call, axis=0, keepdims=True)

    pl.semaphore_wait(barrier, shards + groups - 2)

    def count_copy(owner, to):
        return pltpu.make_async_remote_copy(
            src_ref=counts.at[owner], dst_ref=counts.at[owner], send_sem=count_send.at[to],
            recv_sem=count_recv.at[owner], device_id={"samp": to}, device_id_type=MESH)

    for step in range(1, shards):
        count_copy(me, lax.rem(me + step, shards)).start()
    for step in range(1, shards):
        other = lax.rem(me + step, shards)
        count_copy(other, other).wait_recv()
    sums = counts[0]
    for s in range(1, shards):
        sums = sums + counts[s]
    frequency = sums[0:1] / (2.0 * jnp.maximum(sums[1:2], 1.0))
    shift = 2.0 * frequency
    gain = lax.rsqrt(jnp.maximum(shift * (1.0 - frequency), var_floor))

    def piece_of(k, p):
        return pl.ds(pl.multiple_of(k * tile_rows + p * piece_rows, piece_rows), piece_rows)

    def panel_copy(h, k, to, p):
        block = panel.at[h, piece_of(k, p)]
        return pltpu.make_async_remote_copy(
            src_ref=block, dst_ref=block, send_sem=panel_send.at[to, k, p],
            recv_sem=panel_recv.at[h, k, p], device_id={"snp": to}, device_id_type=MESH)

    strip_rows = min(STRIP, piece_rows)

    def scale_piece(k, p):
        def scale_strip(i, carry):
            start = pl.multiple_of(k * tile_rows + p * piece_rows + i * strip_rows, strip_rows)
            strip = pl.ds(start, strip_rows)
            present = obs_ref[strip, :].astype(jnp.float32)
            panel[part, strip, :] = (present * (geno_ref[strip, :] - shift) * gain).astype(jnp.bfloat16)
            return carry

        lax.fori_loop(0, piece_rows // strip_rows, scale_strip, 0)

    def row_copy(q, h, p, way, src=None):
        to = (index(z + 1, y, core), index(z - 1, y, core), index(z, 1 - y, core), index(z, y, 1 - core))[way]
        return pltpu.make_async_remote_copy(
            src_ref=rows.at[q, h, p] if src is None else src, dst_ref=rows.at[q, h, p],
            send_sem=row_send.at[way, q, h, p], recv_sem=row_recv.at[q, h, p],
            device_id={"samp": to}, device_id_type=MESH)

    def arrive(q, h, p):
        row_copy(q, h, p, CORE).wait_recv()

    last_part = lax.rem(part + groups - 1, groups)
    turned = turned_at(z, depth)

    def part_at(i):
        return lax.rem(part + i, groups)

    def send_own(h, p):
        mine = panel.at[h, piece_of(part, p)]
        row_copy(me, h, p, SIDE, mine).start()

        @pl.when(z < depth - 1)
        def _():
            row_copy(me, h, p, UP, mine).start()

        @pl.when(z > 0)
        def _():
            row_copy(me, h, p, DOWN, mine).start()

        row_copy(me, h, p, CORE, mine).start()
        rows[me, h, p] = panel[h, piece_of(part, p), :]

    for p in range(PIECES):
        for step in range(1, groups):
            other = part_at(step)
            scale_piece(other, p)
            panel_copy(part, other, other, p).start()
        scale_piece(part, p)
        send_own(part, p)
    for step in range(1, groups):
        other = part_at(step)
        for k in range(1, groups):
            for p in range(PIECES):
                panel_copy(part, lax.rem(other + k, groups), other, p).start()
    for step in range(1, groups):
        h = part_at(step)
        for p in range(PIECES):
            panel_copy(h, part, h, p).wait_recv()
            send_own(h, p)

    def column_arrival(at_z, h, p, way):
        q = index(at_z, y, core)
        arrive(q, h, p)

        @pl.when(z < depth - 1 if way == UP else z > 0)
        def _():
            row_copy(q, h, p, way).start()

        @pl.when((at_z != turned) | (h != last_part))
        def _():
            row_copy(q, h, p, SIDE).start()

        row_copy(q, h, p, CORE).start()

    def column_arrivals(i):
        def per_piece(t, carry):
            h, p = part_at(t // PIECES), lax.rem(t, PIECES)

            @pl.when(z - i >= 0)
            def _():
                column_arrival(z - i, h, p, UP)

            @pl.when(z + i < depth)
            def _():
                column_arrival(z + i, h, p, DOWN)

            return carry

        lax.fori_loop(0, groups * PIECES, per_piece, 0)

    def arrive_all(q):
        def per_piece(t, carry):
            arrive(q, t // PIECES, lax.rem(t, PIECES))
            return carry

        lax.fori_loop(0, groups * PIECES, per_piece, 0)

    def products(at_z, at_y):
        def per_core(t, carry):
            q = index(at_z, at_y, lax.rem(core + t, 2))

            @pl.when(t == 1)
            def _():
                arrive_all(q)

            tiles[q] = product(rows, panel, q, range(groups))
            return carry

        lax.fori_loop(0, 2, per_core, 0)

    def side_arrival(at_z, h, p):
        q = index(at_z, 1 - y, core)
        arrive(q, h, p)
        row_copy(q, h, p, CORE).start()

    final = source_at(z, depth, depth - 1)
    final = jnp.where(final == turned, source_at(z, depth, depth - 2), final)

    def begin_late():
        def per_tile(t, carry):
            q = index(jnp.where(t % 2 == 0, turned, final), 1 - y, lax.rem(core + t // 2, 2))

            @pl.when(t >= 2)
            def _():
                for step in range(groups - 1):
                    for p in range(PIECES):
                        arrive(q, part_at(step), p)

            tiles[q] = product(rows, panel, q, [part_at(step) for step in range(groups - 1)])
            return carry

        lax.fori_loop(0, 4, per_tile, 0)

    def round_of(i, carry):
        @pl.when(i < depth)
        def _():
            column_arrivals(i)

        @pl.when(i == 1)
        def _():
            for step in range(1, groups):
                h = part_at(step)
                for k in range(1, groups):
                    for p in range(PIECES):
                        panel_copy(h, part_at(k), h, p).wait_recv()

        @pl.when(i == depth - 1)
        def _():
            q = index(z, 1 - y, core)

            @pl.when(z > 0)
            def _():
                for p in range(PIECES):
                    row_copy(q, last_part, p, DOWN).start()

            @pl.when(z == depth - 2)
            def _():
                for p in range(PIECES):
                    row_copy(q, last_part, p, UP).start()

        at_z = source_at(z, depth, i - 1)
        products(at_z, y)

        def per_piece(t, c):
            @pl.when((i == depth) & (t == (groups - 1) * PIECES))
            def _():
                begin_late()

            @pl.when((at_z != turned) | (t // PIECES != groups - 1))
            def _():
                side_arrival(at_z, part_at(t // PIECES), lax.rem(t, PIECES))

            return c

        lax.fori_loop(0, groups * PIECES, per_piece, 0)

        @pl.when((at_z != turned) & (at_z != final))
        def _():
            products(at_z, 1 - y)

        return carry

    lax.fori_loop(1, depth + 1, round_of, 0)
    for p in range(PIECES):
        side_arrival(turned, last_part, p)
    for p in range(PIECES):
        arrive(index(final, 1 - y, 1 - core), last_part, p)
        arrive(index(turned, 1 - y, 1 - core), last_part, p)

    for step in range(1, shards):
        count_copy(me, lax.rem(me + step, shards)).wait_send()
    for step in range(1, groups):
        for k in range(groups):
            for p in range(PIECES):
                panel_copy(part, k, part_at(step), p).wait_send()

    def drain(i, carry):
        at_z, h, p = i // (groups * PIECES), lax.rem(i // PIECES, groups), lax.rem(i, PIECES)
        q = index(at_z, y, core)
        across = index(at_z, 1 - y, core)

        @pl.when((at_z <= z) & (z < depth - 1))
        def _():
            row_copy(q, h, p, UP).wait_send()

        @pl.when((at_z >= z) & (z > 0))
        def _():
            row_copy(q, h, p, DOWN).wait_send()

        @pl.when((at_z != turned) | (h != last_part))
        def _():
            row_copy(q, h, p, SIDE).wait_send()

        row_copy(q, h, p, CORE).wait_send()
        row_copy(across, h, p, CORE).wait_send()

        @pl.when((at_z == z) & (h == last_part) & (z > 0))
        def _():
            row_copy(across, h, p, DOWN).wait_send()

        @pl.when((at_z == z) & (h == last_part) & (z == depth - 2))
        def _():
            row_copy(across, h, p, UP).wait_send()

        return carry

    lax.fori_loop(0, depth * groups * PIECES, drain, 0)


def shape_of_line(depth):
    z = lax.axis_index("samp") // 4
    low = z < depth // 2
    inward = jnp.where(low, z + 1, z - 1)
    outward = jnp.clip(jnp.where(low, z - 1, z + 1), 0, depth - 1)
    is_end = (z == 0) | (z == depth - 1)
    return z, inward, outward, is_end


def folded_finish(shards, groups, rows, panel, tiles, codes, steps, out_ref, late, out_sem):
    depth = shards // 4
    me = lax.axis_index("samp")
    y = (me // 2) % 2
    z, inward, outward, is_end = shape_of_line(depth)
    far_mid, far_end = depth - 1 - inward, depth - 1 - z
    last_part = lax.rem(lax.axis_index("snp") + groups - 1, groups)
    piece_rows = rows.shape[3]
    tile_rows = PIECES * piece_rows

    def is_late(q):
        return is_end & ((q // 4 == far_end) | ((q // 4 == far_mid) & ((q // 2) % 2 != y)))

    def put(q, carry):
        @pl.when(jnp.logical_not(is_late(q)))
        def _():
            pltpu.make_async_copy(tiles.at[q], out_ref.at[q, 0], out_sem.at[0]).start()

        return carry

    lax.fori_loop(0, shards, put, 0)

    @pl.when(is_end)
    def _():
        def decode(t, carry):
            for p in range(PIECES):
                for k in range(groups):
                    unit = (t * PIECES + p) * groups + k
                    late[t, p * piece_rows:(p + 1) * piece_rows, k * tile_rows:(k + 1) * tile_rows] = (
                        codes[unit].astype(jnp.float32) * steps[unit])
            q = index(far_end, jnp.where(t // 2 == 0, y, 1 - y), lax.rem(t, 2))
            pltpu.make_async_copy(late.at[t], out_ref.at[q, 0], out_sem.at[0]).start()
            return carry

        lax.fori_loop(0, 4, decode, 0)

        def form(i, carry):
            q = index(far_mid, 1 - y, i)
            late[4 + i] = tiles[q] + product(rows, panel, q, [last_part])
            pltpu.make_async_copy(late.at[4 + i], out_ref.at[q, 0], out_sem.at[0]).start()
            return carry

        lax.fori_loop(0, 2, form, 0)

    pltpu.make_async_copy(tiles, out_ref.at[:, 0], out_sem.at[0]).wait()


def folded(shards, groups, geno_hbm, obs_hbm, panel, rows, tiles, codes, steps, geno_ref, obs_ref, alts, calls, columns,
           made, made_steps, raw, raw_in, load_sem, count_sem, across_send, across_recv, line_send, side_send, core_send, row_recv,
           core_recv, code_sem, raw_sem):
    row_count, snp_count = geno_ref.shape
    tile_rows = row_count // groups
    piece_rows = tile_rows // PIECES
    depth = shards // 4
    me = lax.axis_index("samp")
    part = lax.axis_index("snp")
    y, core = (me // 2) % 2, me % 2
    z, inward, outward, is_end = shape_of_line(depth)
    other = lax.rem(part + 1, groups)
    load_rows = row_count // LOADS

    def load(i):
        block = pl.ds(pl.multiple_of(i * load_rows, load_rows), load_rows)
        return (pltpu.make_async_copy(geno_hbm.at[block], geno_ref.at[block], load_sem.at[i]),
                pltpu.make_async_copy(obs_hbm.at[block], obs_ref.at[block], load_sem.at[i]))

    for i in range(LOADS):
        for copy in load(i):
            copy.start()

    barrier = pltpu.get_barrier_semaphore()
    for step in range(1, shards):
        pl.semaphore_signal(barrier, inc=1, device_id={"samp": lax.rem(me + step, shards)}, device_id_type=MESH)
    pl.semaphore_signal(barrier, inc=1, device_id={"snp": other}, device_id_type=MESH)

    def add_strip(i, total):
        alt, call = total
        strip = pl.ds(pl.multiple_of(i * STRIP, STRIP), STRIP)
        present = obs_ref[strip, :].astype(jnp.float32)
        held = present * geno_ref[strip, :]
        for r in range(0, STRIP, 8):
            alt = alt + held[r:r + 8]
            call = call + present[r:r + 8]
        return alt, call

    zero = jnp.zeros((8, snp_count), jnp.float32)
    alt, call = zero, zero
    strips = load_rows // STRIP
    for i in range(LOADS):
        loaded = geno_ref.at[pl.ds(0, 2 * load_rows)]
        pltpu.make_async_copy(loaded, loaded, load_sem.at[i]).wait()
        alt, call = lax.fori_loop(i * strips, (i + 1) * strips, add_strip, (alt, call))
    alts[me] = jnp.sum(alt, axis=0, keepdims=True)
    call = jnp.sum(call, axis=0, keepdims=True).astype(jnp.int32)
    half = snp_count // 2
    calls[me] = jnp.concatenate([call[:, :half], call[:, half:]]).astype(jnp.int16)

    early = pl.ds(pl.multiple_of(part * tile_rows, tile_rows), RAW)
    raw[...] = jnp.where(obs_ref[early, :] > 0, geno_ref[early, :], -1.0)
    pl.semaphore_wait(barrier, shards)

    for step in range(shards):
        to = jnp.where(z < depth // 2, shards - 1 - step, step)

        @pl.when(to != me)
        def _():
            for n, sent in enumerate((alts, calls)):
                pltpu.make_async_remote_copy(
                    src_ref=sent.at[me], dst_ref=sent.at[me], send_sem=count_sem.at[2 * n],
                    recv_sem=count_sem.at[2 * n + 1], device_id={"samp": to}, device_id_type=MESH).start()

    def await_bytes(ref, sem):
        pltpu.make_async_copy(ref, ref, sem).wait()

    def await_rows(count, sem):
        await_bytes(geno_ref.at[pl.ds(0, count // 2)], sem)

    def raw_copy(to, slot):
        return pltpu.make_async_remote_copy(
            src_ref=raw, dst_ref=raw_in.at[slot], send_sem=raw_sem.at[0], recv_sem=raw_sem.at[1],
            device_id={"samp": to}, device_id_type=MESH)

    raw_copy(index(z, 1 - y, core), 0).start()
    raw_copy(index(inward, y, core), jnp.where(is_end, 2, 1)).start()

    @pl.when(jnp.logical_not(is_end))
    def _():
        raw_copy(index(outward, y, core), 1).start()

    def await_counts(way):
        for n, sent in enumerate((alts, calls)):
            await_bytes(sent.at[pl.ds(0, shards - 1)], count_sem.at[2 * n + way])

    await_counts(1)
    alt, call = alts[0], calls[0].astype(jnp.int32)
    for s in range(1, shards):
        alt, call = alt + alts[s], call + calls[s].astype(jnp.int32)
    call = jnp.concatenate([call[0:1], call[1:2]], axis=1).astype(jnp.float32)
    frequency = alt / (2.0 * jnp.maximum(call, 1.0))
    shift = 2.0 * frequency
    gain = lax.rsqrt(jnp.maximum(shift * (1.0 - frequency), var_floor))

    def piece_of(k, p):
        return pl.ds(pl.multiple_of(k * tile_rows + p * piece_rows, piece_rows), piece_rows)

    strip_rows = min(STRIP, piece_rows)

    def scale_piece(k, p):
        def scale_strip(i, carry):
            start = pl.multiple_of(k * tile_rows + p * piece_rows + i * strip_rows, strip_rows)
            strip = pl.ds(start, strip_rows)
            present = obs_ref[strip, :].astype(jnp.float32)
            panel[part, strip, :] = (present * (geno_ref[strip, :] - shift) * gain).astype(jnp.bfloat16)
            return carry

        lax.fori_loop(0, piece_rows // strip_rows, scale_strip, 0)

    def panel_copy(k, p):
        block = panel.at[part, piece_of(k, p)]
        return pltpu.make_async_remote_copy(
            src_ref=block, dst_ref=block, send_sem=across_send.at[0],
            recv_sem=across_recv.at[jnp.where(k == part, PIECES, p)], device_id={"snp": other}, device_id_type=MESH)

    def column_copy(q, h, p):
        return pltpu.make_async_remote_copy(
            src_ref=rows.at[q, h, p], dst_ref=columns.at[part, h, pl.ds(pl.multiple_of(p * piece_rows, piece_rows), piece_rows)],
            send_sem=across_send.at[1], recv_sem=across_recv.at[PIECES + 1], device_id={"snp": other}, device_id_type=MESH)

    cut = piece_rows * 7 // 8
    head, rest = pl.ds(0, cut), pl.ds(cut, piece_rows - cut)

    def span_copy(q, h, p, span, to, send_sem, recv_sem):
        return pltpu.make_async_remote_copy(
            src_ref=rows.at[q, h, p, span], dst_ref=rows.at[q, h, p, span], send_sem=send_sem, recv_sem=recv_sem,
            device_id={"samp": to}, device_id_type=MESH)

    def slot_of(q, at):
        return lax.rem(q // 2 - at // 2 + shards // 2, shards // 2) - 1

    def own_copy(q, h, p, to, send_sem, src=None, dst=None):
        return pltpu.make_async_remote_copy(
            src_ref=rows.at[q, h, p] if src is None else src, dst_ref=rows.at[q, h, p] if dst is None else dst,
            send_sem=send_sem,
            recv_sem=row_recv.at[slot_of(q, to), h, p], device_id={"samp": to}, device_id_type=MESH)

    def send_in(q, h, p, extra=0):
        own_copy(q, h, p, index(inward, y, core), line_send.at[extra]).start()

    def send_out(q, h, p):
        own_copy(q, h, p, index(outward, y, core), line_send.at[2]).start()

    def send_side(q, h, p, extra=0):
        own_copy(q, h, p, index(z, 1 - y, core), side_send.at[extra]).start()

    def core_slot(q, h, p):
        late = jnp.where(is_end, (q // 2 == (depth - 1 - inward) * 2 + 1 - y) & (h != part),
                         (q // 4 == depth - 1 - outward) & (p == 1))
        return jnp.where(late, late_slot(q), q // 2)

    def late_slot(q):
        return shards // 2 + lax.rem(q // 2, 2)

    def send_core(q, h, p, src=None):
        pltpu.make_async_remote_copy(
            src_ref=rows.at[q, h, p] if src is None else src, dst_ref=rows.at[q, h, p], send_sem=core_send.at[0],
            recv_sem=core_recv.at[core_slot(q, h, p)], device_id={"samp": index(z, y, 1 - core)},
            device_id_type=MESH).start()

    def send_core_span(q, h, p, span):
        span_copy(q, h, p, span, index(z, y, 1 - core), core_send.at[0], core_recv.at[core_slot(q, h, p)]).start()

    def arrive(q, h, p):
        await_bytes(rows.at[q, h, p], row_recv.at[slot_of(q, me), h, p])

    def arrive_core(q, late):
        await_bytes(rows.at[q, 0], core_recv.at[late_slot(q) if late else q // 2])

    def part_at(i):
        return lax.rem(part + i, groups)

    def send_own(h, p, skip=0):
        mine = panel.at[h, piece_of(part, p)]
        kept = panel.at[h, pl.ds(pl.multiple_of(part * tile_rows + p * piece_rows + skip, 16), piece_rows - skip)]
        kept_to = rows.at[me, h, p, pl.ds(skip, piece_rows - skip)]
        own_copy(me, h, p, index(z, 1 - y, core), side_send.at[0], kept, kept_to).start()
        own_copy(me, h, p, index(inward, y, core), line_send.at[0], kept, kept_to).start()

        @pl.when(jnp.logical_not(is_end))
        def _():
            own_copy(me, h, p, index(outward, y, core), line_send.at[2], kept, kept_to).start()

        send_core(me, h, p, mine)
        rows[me, h, p] = panel[h, piece_of(part, p), :]

    def scale_raw(slot, q):
        sent = raw_in[slot]
        rows[q, part, 0, 0:RAW, :] = jnp.where(sent >= 0.0, (sent - shift) * gain, 0.0).astype(jnp.bfloat16)

    def arrive_near(q, h, p):
        @pl.when((h == part) & (p == 0))
        def _():
            await_bytes(rows.at[q, h, p, pl.ds(RAW, piece_rows - RAW)], row_recv.at[slot_of(q, me), h, p])

        @pl.when((h != part) | (p != 0))
        def _():
            arrive(q, h, p)

    for p in range(PIECES):
        scale_piece(part, p)
        send_own(part, p, 0 if p else RAW)
        scale_piece(other, p)
        panel_copy(other, p).start()
    for p in range(PIECES):
        panel_copy(part, p).start()

    @pl.when(is_end)
    def _():
        await_bytes(raw_in.at[pl.ds(0, 2)], raw_sem.at[1])

    @pl.when(jnp.logical_not(is_end))
    def _():
        await_bytes(raw_in, raw_sem.at[1])

    scale_raw(0, index(z, 1 - y, core))
    scale_raw(1, index(inward, y, core))

    @pl.when(jnp.logical_not(is_end))
    def _():
        scale_raw(2, index(outward, y, core))

    for p in range(PIECES):
        await_bytes(panel.at[other, piece_of(part, p)], across_recv.at[p])
        send_own(other, p)

    def form(at_z, at_y, parts=None, wait=True):
        def per_core(t, carry):
            q = index(at_z, at_y, lax.rem(core + t, 2))
            if wait:
                @pl.when(t == 1)
                def _():
                    if parts is None:
                        await_bytes(rows.at[q], core_recv.at[q // 2])
                    else:
                        arrive_core(q, False)

            tiles[q] = product(rows, panel, q, range(groups) if parts is None else parts)
            return carry

        lax.fori_loop(0, 2, per_core, 0)

    def await_panel():
        await_bytes(panel.at[other, pl.ds(pl.multiple_of(other * tile_rows, tile_rows), tile_rows)], across_recv.at[PIECES])

    def pick(i, values):
        chosen = values[-1]
        for n in range(len(values) - 2, -1, -1):
            chosen = jnp.where(i == n, values[n], chosen)
        return chosen

    count = groups * PIECES

    @pl.when(is_end)
    def _():
        far_mid = depth - 1 - inward

        def first(t, carry):
            h, p = part_at(t // PIECES), lax.rem(t, PIECES)
            near, beside = index(inward, y, core), index(z, 1 - y, core)
            arrive_near(near, h, p)
            send_side(near, h, p)
            send_core(near, h, p)
            arrive_near(beside, h, p)
            send_in(beside, h, p)
            send_core(beside, h, p)
            return carry

        lax.fori_loop(0, count, first, 0)
        await_panel()

        def second(t, carry):
            h, p = part_at(t // PIECES), lax.rem(t, PIECES)
            far, cross = index(far_mid, y, core), index(inward, 1 - y, core)
            arrive(far, h, p)
            to = index(z, 1 - y, core)

            @pl.when(t < count - 1)
            def _():
                send_side(far, h, p, extra=1)

            @pl.when(t == count - 1)
            def _():
                span_copy(far, h, p, head, to, side_send.at[1], row_recv.at[slot_of(far, to), h, p]).start()
                span_copy(far, h, p, rest, to, side_send.at[1], code_sem.at[4]).start()

            send_core(far, h, p)
            arrive(cross, h, p)
            send_core(cross, h, p)

            @pl.when(t < 3)
            def _():
                form(pick(t, (z, inward, z)), pick(t, (y, y, 1 - y)))

            return carry

        lax.fori_loop(0, count, second, 0)

        def third(t, carry):
            h, p = part_at(t // PIECES), lax.rem(t, PIECES)
            q = index(far_mid, 1 - y, core)

            @pl.when(t < count - 1)
            def _():
                arrive(q, h, p)
                send_core(q, h, p)

            @pl.when(t == count - 1)
            def _():
                await_bytes(rows.at[q, h, p, head], row_recv.at[slot_of(q, me), h, p])
                send_core_span(q, h, p, head)
                await_bytes(rows.at[q, h, p, rest], code_sem.at[4])
                send_core_span(q, h, p, rest)

            @pl.when(t < 2)
            def _():
                form(pick(t, (far_mid, inward)), pick(t, (y, 1 - y)))

            @pl.when(t == 2)
            def _():
                form(far_mid, 1 - y, [part])

            return carry

        lax.fori_loop(0, count, third, 0)
        await_bytes(codes, code_sem.at[1])
        await_bytes(steps, code_sem.at[3])
        arrive_core(index(far_mid, 1 - y, 1 - core), True)
        await_rows(2 * row_count - RAW, line_send.at[0])
        await_rows(2 * row_count - RAW, side_send.at[0])
        await_rows(count * piece_rows, side_send.at[1])
        await_bytes(raw_in.at[pl.ds(0, 2)], raw_sem.at[0])
        await_bytes(rows.at[pl.ds(0, 6)], core_send.at[0])

    @pl.when(jnp.logical_not(is_end))
    def _():
        far = depth - 1 - outward

        def first(t, carry):
            h, p = part_at(t // PIECES), lax.rem(t, PIECES)
            end, near, beside = index(outward, y, core), index(inward, y, core), index(z, 1 - y, core)
            arrive_near(end, h, p)

            @pl.when(p == 0)
            def _():
                send_in(end, h, 0)

            @pl.when(h == other)
            def _():
                send_in(end, jnp.where(p == 0, part, other), 1)

            send_core(end, h, p)
            column_copy(end, h, p).start()
            arrive_near(near, h, p)
            send_out(near, h, p)
            send_core(near, h, p)
            arrive_near(beside, h, p)
            send_core(beside, h, p)
            return carry

        lax.fori_loop(0, count, first, 0)
        for p in range(PIECES):
            send_in(index(z, 1 - y, core), part, p, extra=1)
        for h in range(groups):
            columns[part, h] = rows[index(outward, y, core), h].reshape(tile_rows, snp_count)
        await_panel()

        def code_copy(source, target, n):
            return pltpu.make_async_remote_copy(
                src_ref=source, dst_ref=target, send_sem=code_sem.at[n], recv_sem=code_sem.at[n + 1],
                device_id={"samp": index(outward, y, core)}, device_id_type=MESH)

        def make(side, p, k):
            def per_core(t, carry):
                which = lax.rem(core + t, 2)
                q = index(far, jnp.where(side == 0, y, 1 - y), which)
                term = None
                for h in range(groups):
                    one = lax.dot_general(rows[q, h, p], columns[k, h], (((1,), (1,)), ((), ())),
                                          preferred_element_type=jnp.float32)
                    term = one if term is None else term + one
                term = term * (1.0 / (groups * snp_count))
                top = jnp.max(jnp.abs(term), axis=0, keepdims=True)
                unit = ((side * 2 + which) * PIECES + p) * groups + k
                made[unit] = jnp.round(term * (CODE_TOP / jnp.maximum(top, TINY))).astype(jnp.int32).astype(jnp.int16)
                made_steps[unit] = top * (1.0 / CODE_TOP)
                code_copy(made.at[unit], codes.at[unit], 0).start()
                return carry

            lax.fori_loop(0, 2, per_core, 0)

        def far_core(side, p):
            arrive_core(index(far, jnp.where(side == 0, y, 1 - y), 1 - core), p == 1)

        def make_list(listed):
            def per_entry(i, carry):
                side, p, away = (pick(i, [entry[n] for entry in listed]) for n in range(3))
                make(side, p, lax.rem(part + away, groups))
                return carry

            lax.fori_loop(0, len(listed), per_entry, 0)

        def second(t, carry):
            h, p = part_at(lax.rem(t, groups)), t // groups
            far_q, cross = index(far, y, core), index(outward, 1 - y, core)

            @pl.when(t >= 2)
            def _():
                far_core(t - 2, 0)
                make(t - 2, 0, part)

            arrive(far_q, h, p)
            send_side(far_q, h, p)
            send_core(far_q, h, p)
            ch, cp = part_at(t // PIECES), lax.rem(t, PIECES)
            arrive(cross, ch, cp)
            send_core(cross, ch, cp)

            @pl.when(t > 0)
            def _():
                q = index(far, 1 - y, core)
                h, p = part_at(lax.rem(t - 1, groups)), (t - 1) // groups
                arrive(q, h, p)
                send_core(q, h, p)

            form(pick(t, (z, outward, inward, z)), pick(t, (y, y, y, 1 - y)))
            return carry

        lax.fori_loop(0, count, second, 0)
        for p in range(PIECES):
            send_side(index(inward, y, core), other, p, extra=1)
        far_core(0, 1)
        make_list([(0, 1, 0)])
        await_bytes(columns.at[other], across_recv.at[PIECES + 1])
        make_list([(0, 0, 1), (0, 1, 1), (1, 0, 1)])
        form(outward, 1 - y)
        q = index(far, 1 - y, core)
        arrive(q, other, PIECES - 1)
        send_core(q, other, PIECES - 1)
        cross = index(inward, 1 - y, core)

        def third(t, carry):
            h, p = part_at(t // PIECES), lax.rem(t, PIECES)
            arrive(cross, h, p)
            send_core(cross, h, p)

            @pl.when(t == 1)
            def _():
                far_core(1, 1)
                make_list([(1, 1, 0), (1, 1, 1)])
                code_copy(made_steps, steps, 2).start()

            @pl.when(t < 2)
            def _():
                form(far, pick(t, (y, 1 - y)), wait=False)

            return carry

        lax.fori_loop(0, count, third, 0)
        form(inward, 1 - y)
        await_rows(2 * row_count - RAW, line_send.at[0])
        await_bytes(rows.at[0, 0], line_send.at[1])
        await_rows(2 * row_count - RAW, line_send.at[2])
        await_bytes(raw_in, raw_sem.at[0])
        await_rows(2 * row_count - RAW, side_send.at[0])
        await_bytes(rows.at[0, 0], side_send.at[1])
        await_bytes(rows.at[pl.ds(0, 8)], core_send.at[0])
        await_bytes(rows.at[0], across_send.at[1])
        await_bytes(made, code_sem.at[0])
        await_bytes(made_steps, code_sem.at[2])

    await_counts(0)
    await_bytes(rows.at[0], across_send.at[0])


def folded_body(shards, groups, genotypes, observed):
    row_count, snp_count = genotypes.shape
    tile_rows = row_count // groups
    piece_rows = tile_rows // PIECES
    units = 4 * PIECES * groups
    outs = (
        pltpu.VMEM((groups, row_count, snp_count), jnp.bfloat16),
        pltpu.VMEM((shards, groups, PIECES, piece_rows, snp_count), jnp.bfloat16),
        pltpu.VMEM((shards, tile_rows, row_count), jnp.float32),
        pltpu.VMEM((units, piece_rows, tile_rows), jnp.int16),
        pltpu.VMEM((units, 1, tile_rows), jnp.float32),
    )
    kept = sum(math.prod(o.shape) * jnp.dtype(o.dtype).itemsize for o in outs)
    held = pl.pallas_call(
        functools.partial(folded, shards, groups),
        out_shape=outs,
        in_specs=[pl.BlockSpec(memory_space=pltpu.HBM)] * 2,
        out_specs=[pl.BlockSpec(memory_space=pltpu.VMEM)] * 5,
        scratch_shapes=[
            pltpu.VMEM((row_count, snp_count), jnp.float32),
            pltpu.VMEM((row_count, snp_count), jnp.int32),
            pltpu.VMEM((shards, 1, snp_count), jnp.float32),
            pltpu.VMEM((shards, 2, snp_count // 2), jnp.int16),
            pltpu.VMEM((groups, groups, tile_rows, snp_count), jnp.bfloat16),
            pltpu.VMEM((units, piece_rows, tile_rows), jnp.int16),
            pltpu.VMEM((units, 1, tile_rows), jnp.float32),
            pltpu.VMEM((RAW, snp_count), jnp.float32),
            pltpu.VMEM((3, RAW, snp_count), jnp.float32),
            pltpu.SemaphoreType.DMA((LOADS,)),
            pltpu.SemaphoreType.DMA((4,)),
            pltpu.SemaphoreType.DMA((2,)),
            pltpu.SemaphoreType.DMA((PIECES + 2,)),
            pltpu.SemaphoreType.DMA((3,)),
            pltpu.SemaphoreType.DMA((2,)),
            pltpu.SemaphoreType.DMA((1,)),
            pltpu.SemaphoreType.DMA((shards // 2 - 1, groups, PIECES)),
            pltpu.SemaphoreType.DMA((shards // 2 + 2,)),
            pltpu.SemaphoreType.DMA((5,)),
            pltpu.SemaphoreType.DMA((2,)),
        ],
        compiler_params=pltpu.CompilerParams(
            collective_id=0, has_side_effects=True, vmem_limit_bytes=VMEM_ALL - FOLDED_SPARE - kept),
    )(genotypes, observed)
    panel, rows, tiles, codes, steps = held
    return pl.pallas_call(
        functools.partial(folded_finish, shards, groups),
        out_shape=jax.ShapeDtypeStruct((shards, 1, tile_rows, row_count), jnp.float32),
        in_specs=[pl.BlockSpec(memory_space=pltpu.VMEM)] * 5,
        out_specs=pl.BlockSpec(memory_space=pltpu.HBM),
        scratch_shapes=[
            pltpu.VMEM((6, tile_rows, row_count), jnp.float32),
            pltpu.SemaphoreType.DMA((1,)),
        ],
        compiler_params=pltpu.CompilerParams(vmem_limit_bytes=FOLDED_FINISH),
    )(rows, panel, tiles, codes, steps)


def solution(mesh):
    shards, groups = mesh.shape["samp"], mesh.shape["snp"]

    def body(genotypes, observed):
        if groups == 2 and shards == 16:
            return folded_body(shards, groups, genotypes, observed)
        row_count, snp_count = genotypes.shape
        tile_rows = row_count // groups
        piece_rows = tile_rows // PIECES
        kept = 2 * (groups * row_count * snp_count) * (1 + shards // groups) + 4 * shards * tile_rows * row_count
        panel, rows, tiles = pl.pallas_call(
            functools.partial(kernel, shards, groups),
            out_shape=(
                pltpu.VMEM((groups, row_count, snp_count), jnp.bfloat16),
                pltpu.VMEM((shards, groups, PIECES, piece_rows, snp_count), jnp.bfloat16),
                pltpu.VMEM((shards, tile_rows, row_count), jnp.float32),
            ),
            in_specs=[pl.BlockSpec(memory_space=pltpu.HBM)] * 2,
            out_specs=[pl.BlockSpec(memory_space=pltpu.VMEM)] * 3,
            scratch_shapes=[
                pltpu.VMEM((row_count, snp_count), jnp.float32),
                pltpu.VMEM((row_count, snp_count), jnp.int32),
                pltpu.VMEM((shards, 2, snp_count), jnp.float32),
                pltpu.SemaphoreType.DMA((2, LOADS)),
                pltpu.SemaphoreType.DMA((shards,)),
                pltpu.SemaphoreType.DMA((shards,)),
                pltpu.SemaphoreType.DMA((groups, groups, PIECES)),
                pltpu.SemaphoreType.DMA((groups, groups, PIECES)),
                pltpu.SemaphoreType.DMA((4, shards, groups, PIECES)),
                pltpu.SemaphoreType.DMA((shards, groups, PIECES)),
            ],
            compiler_params=pltpu.CompilerParams(
                collective_id=0, has_side_effects=True, vmem_limit_bytes=VMEM_ALL - VMEM_SPARE - kept),
        )(genotypes, observed)
        return pl.pallas_call(
            functools.partial(finish, shards, groups),
            out_shape=jax.ShapeDtypeStruct((shards, 1, tile_rows, row_count), jnp.float32),
            in_specs=[pl.BlockSpec(memory_space=pltpu.VMEM)] * 3,
            out_specs=pl.BlockSpec(memory_space=pltpu.HBM),
            scratch_shapes=[
                pltpu.VMEM((4, tile_rows, row_count), jnp.float32),
                pltpu.SemaphoreType.DMA((shards,)),
            ],
            compiler_params=pltpu.CompilerParams(vmem_limit_bytes=VMEM_FINISH),
        )(rows, panel, tiles)

    return jax.shard_map(
        body,
        mesh=mesh,
        in_specs=(P("samp", "snp"), P("samp", "snp")),
        out_specs=P(None, "snp", None, "samp"),
        check_vma=False,
    )
```
